32 devices in a mesh: fsdp: 4 (over z), ctx: 4 (over x, core), tp: 2 (over y).
Axes of the slice: x: 2, y: 2, z: 4, core: 2. Of those that a mesh axis runs over, the one named last changes fastest.
Arguments:
- tokens: bfloat16 [16, 1024, 1024], P('fsdp', 'ctx'), may hold values from -12 to 12
- condition: bfloat16 [16, 1024], P('fsdp'), may hold values from -6 to 6
- mod_weight: bfloat16 [1024, 6144], P(None, ('fsdp', 'tp')), may hold values from -0.1875 to 0.1875
- mod_bias: bfloat16 [6144], P(('fsdp', 'tp')), may hold values from -3 to 3
- qkv_weight: bfloat16 [3, 1024, 1024], P(None, 'fsdp', 'tp'), may hold values from -0.125 to 0.125
- qv_bias: bfloat16 [2, 8, 128], P(None, 'tp', 'fsdp'), may hold values from -3 to 3
- attn_weight: bfloat16 [1024, 1024], P('tp', 'fsdp'), may hold values from -3 to 3
- attn_bias: bfloat16 [1024], P('fsdp'), may hold values from -3 to 3
- up_weight: bfloat16 [1024, 4096], P('fsdp', 'tp'), may hold values from -0.1875 to 0.1875
- up_bias: bfloat16 [32, 128], P('tp', 'fsdp'), may hold values from -3 to 3
- down_weight: bfloat16 [4096, 1024], P('tp', 'fsdp'), may hold values from -0.09375 to 0.09375
- down_bias: bfloat16 [1024], P('fsdp'), may hold values from -3 to 3
- cotangent: bfloat16 [16, 1024, 1024], P('fsdp', 'ctx'), may hold values from -6 to 6
Outputs:
- layer_out: bfloat16 [16, 1024, 1024], P('fsdp', 'ctx')
- tokens_grad: float32 [16, 1024, 1024], P('fsdp', 'ctx')
- condition_grad: float32 [16, 1024], P(('fsdp', 'tp'))
- mod_wgrad: float32 [1024, 6144], P(None, ('fsdp', 'tp'))
- mod_bgrad: float32 [6144], P(('fsdp', 'tp'))
- qkv_wgrad: float32 [3, 1024, 1024], P(None, 'fsdp', 'tp')
- qv_bgrad: float32 [2, 8, 128], P(None, 'tp', 'fsdp')
- attn_wgrad: float32 [1024, 1024], P('tp', 'fsdp')
- attn_bgrad: float32 [1024], P('fsdp')
- up_wgrad: float32 [1024, 4096], P('fsdp', 'tp')
- up_bgrad: float32 [32, 128], P('tp', 'fsdp')
- down_wgrad: float32 [4096, 1024], P('tp', 'fsdp')
- down_bgrad: float32 [1024], P('fsdp')
The draws below stay inside these ranges and needn't reach their ends.
All inputs are finite; a program needn't handle non-finite values.
Results may differ from the reference program's by a relative error of at most 0.0109.
The reference program's roundings to bfloat16 on the way count: a program that leaves them out, or rounds other values in their place, can miss the bound.
Values may be sent and summed in bfloat16 or wider, within the bound.
A program may use at most 320 MiB of HBM per device.

```python
import math
import jax
import jax.numpy as jnp
from jax import lax

D = 1024
HEADS = 16
HEAD_DIM = 64
FF = 4096
LATENTS = 16
SEQ = 1024


def draw_tokens(key, part):
    base_key = jax.random.fold_in(key, 0)
    shape = (LATENTS, SEQ, D)
    values = jnp.clip(jax.random.normal(base_key, shape, jnp.float32), -6.0, 6.0)
    return values.astype(jnp.bfloat16)


def draw_qkv_weight(key, part):
    base_key = jax.random.fold_in(key, 0)
    base = jnp.clip(jax.random.normal(base_key, (3, D, D), jnp.float32), -4.0, 4.0) * D ** (-0.5)
    return base.astype(jnp.bfloat16)


def levels(stream_key, extent, cuts, smallest, largest):
    gain, own = 1.0, jax.random.fold_in(stream_key, 6)
    for dim, blocks in cuts:
        steps = jnp.exp(jax.random.uniform(jax.random.fold_in(own, dim), (blocks,), jnp.float32, smallest / len(cuts), largest / len(cuts)))
        gain = gain * jnp.repeat(steps, extent[dim] // blocks).reshape([-1 if axis == dim else 1 for axis in range(len(extent))])
    return gain


def scatter_about(key, shape, deviation, most, pieces=(), held_as=jnp.bfloat16):
    factor_of = levels(key, shape, pieces, -0.22, 0.18) if pieces else 1.0
    drawn = jax.random.normal(key, shape, jnp.float32) * deviation * factor_of
    return jnp.minimum(jnp.maximum(drawn, -most), most).astype(held_as)


def setup_inputs(seed: int = 0) -> dict:
    splits = jax.random.split(jax.random.key(seed), 14)
    tokens = draw_tokens(jax.random.fold_in(splits[13], 71), 0)
    condition = scatter_about(splits[1], (LATENTS, D), 1.0, 6.0, ((0, 4),))
    mod_weight = scatter_about(splits[2], (D, 6 * D), D ** -0.5, 0.1875, ((1, 8),))
    mod_bias = scatter_about(splits[3], (6 * D,), 0.5, 3.0, ((0, 8),))
    qkv_weight = draw_qkv_weight(jax.random.fold_in(splits[13], 71), 0)
    qv_bias = scatter_about(splits[5], (2, D // 128, 128), 0.5, 3.0, ((1, 2), (2, 4)))
    attn_weight = scatter_about(splits[6], (D, D), 0.5, 3.0, ((0, 2), (1, 4)))
    attn_bias = scatter_about(splits[7], (D,), 0.5, 3.0, ((0, 4),))
    up_weight = scatter_about(splits[8], (D, FF), D ** -0.5, 0.1875, ((0, 4), (1, 2)))
    up_bias = scatter_about(splits[9], (FF // 128, 128), 0.5, 3.0, ((0, 2), (1, 4)))
    down_weight = scatter_about(splits[10], (FF, D), FF ** -0.5, 0.09375, ((0, 2), (1, 4)))
    down_bias = scatter_about(splits[11], (D,), 0.5, 3.0, ((0, 4),))
    cotangent = scatter_about(splits[12], (LATENTS, SEQ, D), 1.0, 6.0, ((0, 4), (1, 4)))
    return dict(tokens=tokens, condition=condition, mod_weight=mod_weight, mod_bias=mod_bias, qkv_weight=qkv_weight, qv_bias=qv_bias, attn_weight=attn_weight, attn_bias=attn_bias, up_weight=up_weight, up_bias=up_bias, down_weight=down_weight, down_bias=down_bias, cotangent=cotangent)


@jax.custom_vjp
def low(v):
    return lax.optimization_barrier(v.astype(jnp.bfloat16)).astype(jnp.float32)

@jax.custom_vjp
def low_back(v):
    return v

def low_keep(v):
    return (low(v), None)

def low_pass(kept, grad):
    return (grad,)

def back_keep(v):
    return (v, None)

def back_low(kept, grad):
    return (low(grad),)
low.defvjp(low_keep, low_pass)
low_back.defvjp(back_keep, back_low)

def matmul(left, right):
    return jnp.dot(left, right, precision=lax.Precision.HIGHEST, preferred_element_type=jnp.float32)

def modulate(tok_rows, shift_row, scale_row):
    centre = tok_rows - lax.optimization_barrier(jnp.mean(tok_rows, axis=-1, keepdims=True))
    spread = lax.optimization_barrier(jnp.mean(centre * centre, axis=-1, keepdims=True))
    normed = centre * lax.rsqrt(spread + 1e-06)
    return normed * (1.0 + scale_row) + shift_row

def attention(queries, keys_all, values_all):
    block_rows = math.gcd(SEQ, 512)

    def per_block(query_block):
        scores = low_back(jnp.einsum('qhd,khd->hqk', query_block, keys_all, precision=lax.Precision.HIGHEST) * 0.125)
        row_max = lax.optimization_barrier(jnp.max(scores, axis=-1, keepdims=True))
        weights = jnp.exp(scores - row_max)
        probs = low(weights / lax.optimization_barrier(jnp.sum(weights, axis=-1, keepdims=True)))
        return jnp.einsum('hqk,khd->qhd', probs, values_all, precision=lax.Precision.HIGHEST)
    blocks = queries.reshape(SEQ // block_rows, block_rows, HEADS, HEAD_DIM)
    return lax.map(jax.checkpoint(per_block), blocks).reshape(SEQ, D)

def layer(params, tok_rows, cond_row):
    mod_weight, mod_bias, qkv_weight, qv_bias, attn_weight, attn_bias, up_weight, up_bias, down_weight, down_bias = params
    act_cond = low(jax.nn.silu(cond_row))
    modulation = low_back(matmul(act_cond[None, :], mod_weight)[0] + mod_bias).reshape(6, D)
    attn_input = low(modulate(tok_rows, modulation[0], modulation[1]))
    q_bias = qv_bias[0].reshape(D)
    v_bias = qv_bias[1].reshape(D)
    queries = low_back(low(matmul(attn_input, qkv_weight[0]) + q_bias)).reshape(SEQ, HEADS, HEAD_DIM)
    keys_all = low_back(low(matmul(attn_input, qkv_weight[1]))).reshape(SEQ, HEADS, HEAD_DIM)
    values_all = low_back(low(matmul(attn_input, qkv_weight[2]) + v_bias)).reshape(SEQ, HEADS, HEAD_DIM)
    attended = low_back(low(attention(queries, keys_all, values_all)))
    attn_out = low_back(matmul(attended, attn_weight) + attn_bias)
    middle = tok_rows + modulation[2] * attn_out
    mlp_input = low(modulate(middle, modulation[3], modulation[4]))
    up_pre = low_back(matmul(mlp_input, up_weight) + up_bias.reshape(FF))
    up_act = low(jax.nn.gelu(up_pre, approximate=True))
    mlp_out = low_back(matmul(up_act, down_weight) + down_bias)
    return middle + modulation[5] * mlp_out

def reference(tokens, condition, mod_weight, mod_bias, qkv_weight, qv_bias, attn_weight, attn_bias, up_weight, up_bias, down_weight, down_bias, cotangent):
    params = tuple((weight_in.astype(jnp.float32) for weight_in in (mod_weight, mod_bias, qkv_weight, qv_bias, attn_weight, attn_bias, up_weight, up_bias, down_weight, down_bias)))

    def per_latent(running, inputs):
        tok_rows, cond_row, grad_rows = inputs
        layer_y, pullback = jax.vjp(layer, params, tok_rows.astype(jnp.float32), cond_row.astype(jnp.float32))
        param_grads, tok_grad, cond_grad = pullback(grad_rows.astype(jnp.float32))
        running = jax.tree.map(jnp.add, running, param_grads)
        return (running, (layer_y.astype(jnp.bfloat16), tok_grad, cond_grad))
    zeros = jax.tree.map(jnp.zeros_like, params)
    totals, outputs = lax.scan(per_latent, zeros, (tokens, condition, cotangent))
    return (outputs[0], outputs[1], outputs[2], totals[0], totals[1], totals[2], totals[3], totals[4], totals[5], totals[6], totals[7], totals[8], totals[9])
```

```python
import jax
import jax.numpy as jnp
from jax import lax
from jax.sharding import PartitionSpec as P


def modulate(tok_rows, shift_row, scale_row):
    centre = tok_rows - jnp.mean(tok_rows, axis=-1, keepdims=True)
    spread = jnp.mean(centre * centre, axis=-1, keepdims=True)
    normed = centre * lax.rsqrt(spread + 1e-06)
    return normed * (1.0 + scale_row[:, None, :]) + shift_row[:, None, :]


def gelu_tanh(pre_act):
    return jax.nn.gelu(pre_act, approximate=True)


def flat_dot(left, right):
    return jnp.dot(left, right, preferred_element_type=jnp.float32)


def head_slice(source, latent, head_pair):
    row_count = source.shape[1]
    picked = lax.dynamic_slice(source, (latent, 0, head_pair * 128), (1, row_count, 128))
    return picked[0].reshape(row_count, 2, 64)


def tokens_major(stacked, latents, head_pairs):
    row_count = stacked.shape[-2]
    grouped = stacked.reshape(latents, head_pairs, row_count, 128)
    return jnp.transpose(grouped, (0, 2, 1, 3)).reshape(latents, row_count, head_pairs * 128)


def attend(queries, keys_all, values_all, head_pairs):

    def attend_per_block(block_index):
        latent = block_index // head_pairs
        head_pair = block_index % head_pairs
        query_h = head_slice(queries, latent, head_pair)
        key_h = head_slice(keys_all, latent, head_pair)
        value_h = head_slice(values_all, latent, head_pair)
        scores = (
            jnp.einsum("qhd,khd->hqk", query_h, key_h, preferred_element_type=jnp.float32) * 0.125
        )
        row_max = jnp.max(scores, axis=-1, keepdims=True)
        weights = jnp.exp(scores - row_max)
        row_total = jnp.sum(weights, axis=-1, keepdims=True)
        probs_low = (weights / row_total).astype(jnp.bfloat16)
        attended = jnp.einsum(
            "hqk,khd->qhd", probs_low, value_h, preferred_element_type=jnp.float32
        )
        return (attended.reshape(query_h.shape[0], 128), (row_max + jnp.log(row_total))[..., 0])

    return lax.map(attend_per_block, jnp.arange(queries.shape[0] * head_pairs))


def query_side(queries, keys_all, values_all, grad_rows, log_norm, head_pairs):

    def query_per_block(packed):
        block_index, norm_block = packed
        latent = block_index // head_pairs
        head_pair = block_index % head_pairs
        query_h = head_slice(queries, latent, head_pair)
        key_h = head_slice(keys_all, latent, head_pair)
        value_h = head_slice(values_all, latent, head_pair)
        grad_h = head_slice(grad_rows, latent, head_pair)
        scores = (
            jnp.einsum("qhd,khd->hqk", query_h, key_h, preferred_element_type=jnp.float32) * 0.125
        )
        probs = jnp.exp(scores - norm_block[..., None])
        dprobs = jnp.einsum("qhd,khd->hqk", grad_h, value_h, preferred_element_type=jnp.float32)
        row_delta = jnp.sum(probs * dprobs, axis=-1, keepdims=True)
        score_grad = (probs * (dprobs - row_delta)).astype(jnp.bfloat16)
        query_grad = (
            jnp.einsum("hqk,khd->qhd", score_grad, key_h, preferred_element_type=jnp.float32)
            * 0.125
        )
        query_count = query_h.shape[0]
        key_grad = (
            jnp.einsum("hqk,qhd->khd", score_grad, query_h, preferred_element_type=jnp.float32)
            * 0.125
        )
        value_grad = jnp.einsum(
            "hqk,qhd->khd", probs.astype(jnp.bfloat16), grad_h, preferred_element_type=jnp.float32
        )
        return (
            query_grad.reshape(query_count, 128),
            key_grad.reshape(-1, 128),
            value_grad.reshape(-1, 128),
        )

    return lax.map(query_per_block, (jnp.arange(queries.shape[0] * head_pairs), log_norm))


def body(
    tokens,
    condition,
    mod_weight,
    mod_bias,
    qkv_weight,
    qv_bias,
    attn_weight,
    attn_bias,
    up_weight,
    up_bias,
    down_weight,
    down_bias,
    cotangent,
):
    latents, tok_count, width = tokens.shape
    gathered = (
        lax.all_gather(condition, "fsdp", axis=0, tiled=True),
        lax.all_gather(qkv_weight, "fsdp", axis=1, tiled=True),
        lax.all_gather(qv_bias, "fsdp", axis=2, tiled=True),
        lax.all_gather(attn_weight, "fsdp", axis=1, tiled=True),
        lax.all_gather(attn_bias, "fsdp", axis=0, tiled=True),
        lax.all_gather(up_weight, "fsdp", axis=0, tiled=True),
        lax.all_gather(up_bias, "fsdp", axis=1, tiled=True),
        lax.all_gather(down_weight, "fsdp", axis=1, tiled=True),
        lax.all_gather(down_bias, "fsdp", axis=0, tiled=True),
    )
    (
        cond_all,
        qkv_full,
        qv_full,
        attn_full,
        attn_bias_full,
        up_full,
        up_bias_full,
        down_full,
        down_bias_full,
    ) = gathered
    q_bias = qv_full[0].reshape(-1).astype(jnp.float32)
    v_bias = qv_full[1].reshape(-1).astype(jnp.float32)
    hidden_bias = up_bias_full.reshape(-1).astype(jnp.float32)
    act_all = jax.nn.silu(cond_all.astype(jnp.float32)).astype(jnp.bfloat16)
    mod_piece = flat_dot(act_all, mod_weight) + mod_bias.astype(jnp.float32)
    mod_full = lax.all_gather(mod_piece, ("fsdp", "tp"), axis=1, tiled=True)
    first_latent = lax.axis_index("fsdp") * latents
    modulation = lax.dynamic_slice_in_dim(mod_full, first_latent, latents, 0).reshape(
        latents, 6, width
    )
    shift_attn, scale_attn, gate_attn = (modulation[:, 0], modulation[:, 1], modulation[:, 2])
    shift_mlp, scale_mlp, gate_mlp = (modulation[:, 3], modulation[:, 4], modulation[:, 5])
    tok_float = tokens.astype(jnp.float32)
    attn_input_f, norm_pull_attn = jax.vjp(modulate, tok_float, shift_attn, scale_attn)
    attn_input = attn_input_f.astype(jnp.bfloat16).reshape(-1, width)
    queries = (
        (flat_dot(attn_input, qkv_full[0]) + q_bias)
        .astype(jnp.bfloat16)
        .reshape(latents, tok_count, -1)
    )
    keys_own = (
        flat_dot(attn_input, qkv_full[1]).astype(jnp.bfloat16).reshape(latents, tok_count, -1)
    )
    values_own = (
        (flat_dot(attn_input, qkv_full[2]) + v_bias)
        .astype(jnp.bfloat16)
        .reshape(latents, tok_count, -1)
    )
    keys_all, values_all = (
        lax.all_gather(keys_own, "ctx", axis=1, tiled=True),
        lax.all_gather(values_own, "ctx", axis=1, tiled=True),
    )
    head_width = queries.shape[-1]
    head_pairs = head_width // 128
    attended_st, log_norm = attend(queries, keys_all, values_all, head_pairs)
    attended = (
        tokens_major(attended_st, latents, head_pairs).astype(jnp.bfloat16).reshape(-1, head_width)
    )
    attn_out = lax.psum(flat_dot(attended, attn_full), "tp") + attn_bias_full.astype(jnp.float32)
    attn_out = attn_out.reshape(latents, tok_count, width)
    middle = tok_float + gate_attn[:, None, :] * attn_out
    mlp_input_f, norm_pull_mlp = jax.vjp(modulate, middle, shift_mlp, scale_mlp)
    mlp_input = mlp_input_f.astype(jnp.bfloat16).reshape(-1, width)
    up_pre = flat_dot(mlp_input, up_full) + hidden_bias
    up_act_f, gelu_pull = jax.vjp(gelu_tanh, up_pre)
    up_act = up_act_f.astype(jnp.bfloat16)
    mlp_out = lax.psum(flat_dot(up_act, down_full), "tp") + down_bias_full.astype(jnp.float32)
    mlp_out = mlp_out.reshape(latents, tok_count, width)
    layer_out = (middle + gate_mlp[:, None, :] * mlp_out).astype(jnp.bfloat16)
    out_grad = cotangent.astype(jnp.float32)
    gate_mlp_grad = jnp.sum(out_grad * mlp_out, axis=1)
    mlp_grad = (out_grad * gate_mlp[:, None, :]).astype(jnp.bfloat16).reshape(-1, width)
    down_bgrad_part = jnp.sum(mlp_grad.astype(jnp.float32), axis=0)
    down_wgrad_part = flat_dot(up_act.T, mlp_grad)
    up_grad = gelu_pull(flat_dot(mlp_grad, down_full.T))[0].astype(jnp.bfloat16)
    up_bgrad_part = jnp.sum(up_grad.astype(jnp.float32), axis=0)
    up_wgrad_part = flat_dot(mlp_input.T, up_grad)
    mlp_input_grad = lax.psum(flat_dot(up_grad, up_full.T), "tp").reshape(latents, tok_count, width)
    middle_part, shift_mlp_grad, scale_mlp_grad = norm_pull_mlp(mlp_input_grad)
    middle_grad = out_grad + middle_part
    gate_attn_grad = jnp.sum(middle_grad * attn_out, axis=1)
    attn_grad = (middle_grad * gate_attn[:, None, :]).astype(jnp.bfloat16).reshape(-1, width)
    attn_bgrad_part = jnp.sum(attn_grad.astype(jnp.float32), axis=0)
    attn_wgrad_part = flat_dot(attended.T, attn_grad)
    attended_grad = (
        flat_dot(attn_grad, attn_full.T)
        .astype(jnp.bfloat16)
        .reshape(latents, tok_count, head_width)
    )
    query_st, key_st, value_st = query_side(
        queries, keys_all, values_all, attended_grad, log_norm, head_pairs
    )
    key_parts = key_st.reshape(latents, head_pairs, -1, 128)
    value_parts = value_st.reshape(latents, head_pairs, -1, 128)
    key_sum, value_sum = (
        lax.psum_scatter(key_parts, "ctx", scatter_dimension=2, tiled=True),
        lax.psum_scatter(value_parts, "ctx", scatter_dimension=2, tiled=True),
    )
    key_grad = tokens_major(
        key_sum.reshape(latents * head_pairs, tok_count, 128), latents, head_pairs
    )
    value_grad = tokens_major(
        value_sum.reshape(latents * head_pairs, tok_count, 128), latents, head_pairs
    )
    query_flat = (
        tokens_major(query_st, latents, head_pairs).astype(jnp.bfloat16).reshape(-1, head_width)
    )
    key_flat = key_grad.astype(jnp.bfloat16).reshape(-1, head_width)
    value_flat = value_grad.astype(jnp.bfloat16).reshape(-1, head_width)
    input_terms = (
        flat_dot(query_flat, qkv_full[0].T)
        + flat_dot(key_flat, qkv_full[1].T)
        + flat_dot(value_flat, qkv_full[2].T)
    )
    attn_input_grad = lax.psum(input_terms, "tp").reshape(latents, tok_count, width)
    qkv_wgrad_part = jnp.stack(
        [
            flat_dot(attn_input.T, query_flat),
            flat_dot(attn_input.T, key_flat),
            flat_dot(attn_input.T, value_flat),
        ]
    )
    qv_bgrad_part = jnp.stack(
        [
            jnp.sum(query_flat.astype(jnp.float32), axis=0),
            jnp.sum(value_flat.astype(jnp.float32), axis=0),
        ]
    ).reshape(2, -1, 128)
    token_part, shift_attn_grad, scale_attn_grad = norm_pull_attn(attn_input_grad)
    tokens_grad = middle_grad + token_part
    mod_grad_own = jnp.stack(
        [
            shift_attn_grad,
            scale_attn_grad,
            gate_attn_grad,
            shift_mlp_grad,
            scale_mlp_grad,
            gate_mlp_grad,
        ],
        axis=1,
    ).reshape(latents, -1)
    mod_grad_slab = lax.dynamic_update_slice_in_dim(
        jnp.zeros(mod_full.shape, jnp.float32), mod_grad_own, first_latent, 0
    )
    mod_grad_all = lax.psum(mod_grad_slab, ("fsdp", "ctx")).astype(jnp.bfloat16)
    piece = lax.axis_index("fsdp") * lax.axis_size("tp") + lax.axis_index("tp")
    piece_width = mod_weight.shape[1]
    mod_grad_piece = lax.dynamic_slice_in_dim(mod_grad_all, piece * piece_width, piece_width, 1)
    mod_wgrad = flat_dot(act_all.T, mod_grad_piece)
    mod_bgrad = jnp.sum(mod_grad_piece.astype(jnp.float32), axis=0)
    own_rows = mod_full.shape[0] // (lax.axis_size("fsdp") * lax.axis_size("tp"))
    act_grad = lax.psum_scatter(
        flat_dot(mod_grad_piece, mod_weight.T), ("fsdp", "tp"), scatter_dimension=0, tiled=True
    )
    cond_rows = lax.dynamic_slice_in_dim(cond_all, piece * own_rows, own_rows, 0).astype(
        jnp.float32
    )
    condition_grad = jax.vjp(jax.nn.silu, cond_rows)[1](act_grad)[0]
    partials = (
        qkv_wgrad_part,
        qv_bgrad_part,
        attn_wgrad_part,
        attn_bgrad_part,
        up_wgrad_part,
        up_bgrad_part.reshape(-1, 128),
        down_wgrad_part,
        down_bgrad_part,
    )
    shards = (
        lax.psum_scatter(partials[0], "fsdp", scatter_dimension=1, tiled=True),
        lax.psum_scatter(partials[1], "fsdp", scatter_dimension=2, tiled=True),
        lax.psum_scatter(partials[2], "fsdp", scatter_dimension=1, tiled=True),
        lax.psum_scatter(partials[3], "fsdp", scatter_dimension=0, tiled=True),
        lax.psum_scatter(partials[4], "fsdp", scatter_dimension=0, tiled=True),
        lax.psum_scatter(partials[5], "fsdp", scatter_dimension=1, tiled=True),
        lax.psum_scatter(partials[6], "fsdp", scatter_dimension=1, tiled=True),
        lax.psum_scatter(partials[7], "fsdp", scatter_dimension=0, tiled=True),
    )
    reduced = lax.psum(
        (shards[0], shards[1], shards[2], shards[3], shards[4], shards[5], shards[6], shards[7]),
        "ctx",
    )
    qkv_wgrad, qv_bgrad, attn_wgrad, attn_bgrad, up_wgrad, up_bgrad, down_wgrad, down_bgrad = (
        reduced
    )
    return (
        layer_out,
        tokens_grad,
        condition_grad,
        mod_wgrad,
        mod_bgrad,
        qkv_wgrad,
        qv_bgrad,
        attn_wgrad,
        attn_bgrad,
        up_wgrad,
        up_bgrad,
        down_wgrad,
        down_bgrad,
    )


X_SWAP = [(0, 2), (2, 0), (1, 3), (3, 1)]
CORE_SWAP = [(0, 1), (1, 0), (2, 3), (3, 2)]
Y_SWAP = [(0, 1), (1, 0)]


def to_x(value):
    return lax.ppermute(value, "ctx", X_SWAP)


def to_core(value):
    return lax.ppermute(value, "ctx", CORE_SWAP)


def to_y(value):
    return lax.ppermute(value, "tp", Y_SWAP)


def to_z(value, step):
    count = lax.axis_size("fsdp")
    return lax.ppermute(value, "fsdp", [(src, (src + step) % count) for src in range(count)])


def z_order(relative, z):
    count = len(relative)
    back = list(relative[::-1])
    doubled = jnp.stack(back + back[:-1])
    return lax.dynamic_slice_in_dim(doubled, count - 1 - z, count, 0)


def pick(stacked, index):
    return lax.dynamic_index_in_dim(stacked, index, 0, keepdims=False)


def gather_z(value):
    count = lax.axis_size("fsdp")
    return [value] + [to_z(value, step) for step in range(1, count)]


def normalize(rows):
    centre = rows - jnp.mean(rows, axis=-1, keepdims=True)
    spread = jnp.mean(centre * centre, axis=-1, keepdims=True)
    inverse = lax.rsqrt(spread + 1e-06)
    return centre * inverse, inverse


def normalize_back(grad, normed, inverse, scale):
    e = grad * (1.0 + scale)
    mean_e = jnp.mean(e, axis=-1, keepdims=True)
    mean_en = jnp.mean(e * normed, axis=-1, keepdims=True)
    return (e - mean_e - normed * mean_en) * inverse


def dot_nt(left, right):
    return lax.dot_general(left, right, (((1,), (1,)), ((), ())), preferred_element_type=jnp.float32)


def dot_tn(left, right):
    return lax.dot_general(left, right, (((0,), (0,)), ((), ())), preferred_element_type=jnp.float32)


def attn_forward(x_own, x_oth, nat, oth, q_bias, v_bias):
    z = lax.axis_index("fsdp")
    x_all = jnp.concatenate([x_own, x_oth])
    planes = [z_order(nat, z), z_order(oth, z)]
    weights = []
    for part in range(3):
        weights.append(jnp.concatenate([p[:, part].reshape(-1, p.shape[-1]) for p in planes], axis=1))
    out_w = jnp.concatenate([jnp.transpose(p[:, 3], (1, 0, 2)).reshape(p.shape[2], -1) for p in planes], axis=0)
    q = (flat_dot(x_all, weights[0]) + q_bias).astype(jnp.bfloat16)
    k = flat_dot(x_all, weights[1]).astype(jnp.bfloat16)
    v = (flat_dot(x_all, weights[2]) + v_bias).astype(jnp.bfloat16)
    heads = lambda a: a.reshape(a.shape[0], -1, 64)
    scores = jnp.einsum("qhd,khd->hqk", heads(q), heads(k), preferred_element_type=jnp.float32) * 0.125
    row_max = jnp.max(scores, axis=-1, keepdims=True)
    w = jnp.exp(scores - row_max)
    total = jnp.sum(w, axis=-1, keepdims=True)
    probs = (w / total).astype(jnp.bfloat16)
    attended = jnp.einsum("hqk,khd->qhd", probs, heads(v), preferred_element_type=jnp.float32)
    attended = attended.reshape(q.shape).astype(jnp.bfloat16)
    log_norm = (row_max + jnp.log(total))[..., 0]
    out = flat_dot(attended, out_w)
    half = x_own.shape[0]
    return q, k, v, attended, log_norm, out[:half], out[half:]


def attn_backward(g_own, g_oth, x_own, x_oth, nat, oth, q, k, v, attended, log_norm):
    z = lax.axis_index("fsdp")
    x_all = jnp.concatenate([x_own, x_oth])
    g_all = jnp.concatenate([g_own, g_oth])
    planes = [z_order(nat, z), z_order(oth, z)]
    weights = []
    for part in range(3):
        weights.append(jnp.concatenate([p[:, part].reshape(-1, p.shape[-1]) for p in planes], axis=1))
    out_w = jnp.concatenate([jnp.transpose(p[:, 3], (1, 0, 2)).reshape(p.shape[2], -1) for p in planes], axis=0)
    att_w = dot_tn(attended, g_all)
    d_att = dot_nt(g_all, out_w).astype(jnp.bfloat16)
    heads = lambda a: a.reshape(a.shape[0], -1, 64)
    scores = jnp.einsum("qhd,khd->hqk", heads(q), heads(k), preferred_element_type=jnp.float32) * 0.125
    probs = jnp.exp(scores - log_norm[..., None])
    dprobs = jnp.einsum("qhd,khd->hqk", heads(d_att), heads(v), preferred_element_type=jnp.float32)
    delta = jnp.sum(probs * dprobs, axis=-1, keepdims=True)
    ds = (probs * (dprobs - delta)).astype(jnp.bfloat16)
    dq = jnp.einsum("hqk,khd->qhd", ds, heads(k), preferred_element_type=jnp.float32) * 0.125
    dk = jnp.einsum("hqk,qhd->khd", ds, heads(q), preferred_element_type=jnp.float32) * 0.125
    dv = jnp.einsum("hqk,qhd->khd", probs.astype(jnp.bfloat16), heads(d_att), preferred_element_type=jnp.float32)
    dq, dk, dv = [a.reshape(q.shape).astype(jnp.bfloat16) for a in (dq, dk, dv)]
    back = dot_nt(dq, weights[0]) + dot_nt(dk, weights[1]) + dot_nt(dv, weights[2])
    bias = jnp.stack([jnp.sum(dq.astype(jnp.float32), axis=0), jnp.sum(dv.astype(jnp.float32), axis=0)])
    half = x_own.shape[0]
    count = len(nat)
    pieces = []
    w_rows = [dot_tn(x_all, a).astype(jnp.bfloat16) for a in (dq, dk, dv)]
    att_w = att_w.astype(jnp.bfloat16)
    wide = nat[0].shape[-1]
    depth = x_all.shape[1] // count
    for plane in range(2):
        cut = slice(plane * wide, (plane + 1) * wide)
        qkv = jnp.stack([a[:, cut].reshape(count, depth, wide) for a in w_rows], axis=1)
        att = jnp.transpose(att_w[cut].reshape(wide, count, depth), (1, 0, 2))[:, None]
        pieces.append(jnp.concatenate([qkv, att], axis=1))
    rel = [[pick(p, (z + step) % count) for step in range(count)] for p in pieces]
    return back[:half], back[half:], rel[0], rel[1], bias


def mlp(m_own, m_oth, g_own, g_oth, up_nat, up_oth, down_nat, down_oth, bias):
    z = lax.axis_index("fsdp")
    count = len(up_nat)
    m_all = jnp.concatenate([m_own, m_oth])
    g_all = jnp.concatenate([g_own, g_oth])
    half = m_own.shape[0]
    up_w = jnp.concatenate([z_order(p, z).reshape(-1, p[0].shape[-1]) for p in (up_nat, up_oth)], axis=1)
    down_w = jnp.concatenate(
        [jnp.transpose(z_order(p, z), (1, 0, 2)).reshape(p[0].shape[0], -1) for p in (down_nat, down_oth)], axis=0
    )
    pre = flat_dot(m_all, up_w) + bias
    act_f, pull = jax.vjp(gelu_tanh, pre)
    act = act_f.astype(jnp.bfloat16)
    out = flat_dot(act, down_w)
    up_grad = pull(dot_nt(g_all, down_w))[0].astype(jnp.bfloat16)
    back = dot_nt(up_grad, up_w)
    up_bgrad = jnp.sum(up_grad.astype(jnp.float32), axis=0)
    up_wg = dot_tn(m_all, up_grad).astype(jnp.bfloat16)
    down_wg = dot_tn(act, g_all).astype(jnp.bfloat16)
    wide = up_nat[0].shape[-1]
    depth = m_all.shape[1] // count
    ups, downs = [], []
    for plane in range(2):
        cut = slice(plane * wide, (plane + 1) * wide)
        up_p = up_wg[:, cut].reshape(count, depth, wide)
        down_p = jnp.transpose(down_wg[cut].reshape(wide, count, depth), (1, 0, 2))
        ups.append([pick(up_p, (z + step) % count) for step in range(count)])
        downs.append([pick(down_p, (z + step) % count) for step in range(count)])
    return (
        out[:half], out[half:], back[:half], back[half:],
        ups[0], ups[1], downs[0], downs[1], up_bgrad,
    )


def reduce_pieces(nat, oth):
    f32 = jnp.float32
    got = [to_y(piece) for piece in oth]
    summed = [(a.astype(f32) + b.astype(f32)) for a, b in zip(nat, got)]
    total = summed[0]
    for step in range(1, len(summed)):
        total = total + to_z(summed[step].astype(jnp.bfloat16), step).astype(f32)
    low = total.astype(jnp.bfloat16)
    return low.astype(f32) + to_x(low).astype(f32)


def hyper_sum(value):
    value = value + to_core(value)
    value = value + to_x(value)
    value = value + to_y(value)
    count = lax.axis_size("fsdp")
    reach = 1
    while reach < count:
        value = value + lax.ppermute(value, "fsdp", [(src, src ^ reach) for src in range(count)])
        reach *= 2
    return value


def fast_body(
    tokens, condition, mod_weight, mod_bias, qkv_weight, qv_bias, attn_weight, attn_bias,
    up_weight, up_bias, down_weight, down_bias, cotangent,
):
    f32, bf16 = jnp.float32, jnp.bfloat16
    latents, tok_count, width = tokens.shape
    count = lax.axis_size("fsdp")
    z, y = lax.axis_index("fsdp"), lax.axis_index("tp")
    place = lax.axis_index("ctx")
    x, core = place // 2, place % 2
    mine, theirs = 2 * x + y, 2 * (1 - x) + y

    small_parts = (condition, qv_bias, attn_bias, up_bias, down_bias)
    small = jnp.concatenate([a.reshape(-1) for a in small_parts])
    small_all = z_order(gather_z(small), z)
    cond_size = condition.size
    cond_all = small_all[:, :cond_size].reshape(count * latents, width)
    bias_all = small_all[:, cond_size:]
    bias_oth = to_y(bias_all)
    marks = [qv_bias.size, qv_bias.size + attn_bias.size, qv_bias.size + attn_bias.size + up_bias.size]

    def qv_plane(b):
        rows = jnp.transpose(b[:, : marks[0]].reshape((count,) + qv_bias.shape), (1, 2, 0, 3)).reshape(2, -1)
        return lax.dynamic_slice_in_dim(rows, core * (rows.shape[1] // 2), rows.shape[1] // 2, 1)

    def up_plane(b):
        rows = jnp.transpose(b[:, marks[1] : marks[2]].reshape((count,) + up_bias.shape), (1, 0, 2)).reshape(-1)
        return lax.dynamic_slice_in_dim(rows, core * (rows.shape[0] // 2), rows.shape[0] // 2, 0)

    qv = jnp.concatenate([qv_plane(bias_all), qv_plane(bias_oth)], axis=1).astype(f32)
    hidden_bias = jnp.concatenate([up_plane(bias_all), up_plane(bias_oth)]).astype(f32)
    attn_bias_full = bias_all[:, marks[0] : marks[1]].reshape(-1).astype(f32)
    down_bias_full = bias_all[:, marks[2] :].reshape(-1).astype(f32)

    act_all = jax.nn.silu(cond_all.astype(f32)).astype(bf16)
    mod_piece = flat_dot(act_all, mod_weight) + mod_bias.astype(f32)
    mod_pair = jnp.stack([mod_piece, to_y(mod_piece)], axis=1)
    mod_pair = jnp.where(y == 0, mod_pair, mod_pair[:, ::-1])
    rows_for = lambda step: lax.dynamic_slice_in_dim(mod_pair, ((z + step) % count) * latents, latents, 0)
    mod_rel = [pick(rows_for(0), mine)] + [pick(to_z(rows_for(step), step), mine) for step in range(1, count)]
    modulation = z_order(mod_rel, z).reshape(6, width)
    shift_attn, scale_attn, gate_attn, shift_mlp, scale_mlp, gate_mlp = [modulation[r] for r in range(6)]

    def enter(source):
        return jnp.concatenate([pick(source, mine), to_x(pick(source, theirs))])

    tok = enter(tokens).astype(f32)
    cot = enter(cotangent).astype(f32)

    half_of = lambda a, axis: lax.dynamic_slice_in_dim(a, core * (a.shape[axis] // 2), a.shape[axis] // 2, axis)
    own_a = jnp.concatenate([half_of(qkv_weight, 2), half_of(attn_weight, 0)[None]])
    a_nat = gather_z(own_a)
    a_oth = [to_y(p) for p in a_nat]
    up_nat = gather_z(half_of(up_weight, 1))
    up_oth = [to_y(p) for p in up_nat]
    down_nat = gather_z(half_of(down_weight, 0))
    down_oth = [to_y(p) for p in down_nat]

    norm_a, inv_a = normalize(tok)
    x_own = (norm_a * (1.0 + scale_attn) + shift_attn).astype(bf16)
    x_oth = to_core(x_own)
    q, k, v, attended, log_norm, ao_own, ao_send = attn_forward(x_own, x_oth, a_nat, a_oth, qv[0], qv[1])
    attn_out = ao_own + to_core(ao_send).astype(f32) + attn_bias_full
    middle = tok + gate_attn * attn_out
    norm_m, inv_m = normalize(middle)
    m_own = (norm_m * (1.0 + scale_mlp) + shift_mlp).astype(bf16)
    m_oth = to_core(m_own)
    g_own = (cot * gate_mlp).astype(bf16)
    g_oth = to_core(g_own)
    (
        mo_own, mo_send, mig_own, mig_send, upg_nat, upg_oth, downg_nat, downg_oth, up_bpart,
    ) = mlp(m_own, m_oth, g_own, g_oth, up_nat, up_oth, down_nat, down_oth, hidden_bias)
    up_half = reduce_pieces(upg_nat, upg_oth)
    down_half = reduce_pieces(downg_nat, downg_oth)
    mlp_out = mo_own + to_core(mo_send).astype(f32) + down_bias_full
    out_rows = (middle + gate_mlp * mlp_out).astype(bf16)
    gate_mlp_grad = jnp.sum(cot * mlp_out, axis=0)
    down_bpart = jnp.sum(g_own.astype(f32), axis=0)
    mig = mig_own + to_core(mig_send).astype(f32)
    middle_grad = cot + normalize_back(mig, norm_m, inv_m, scale_mlp)
    shift_mlp_grad = jnp.sum(mig, axis=0)
    scale_mlp_grad = jnp.sum(mig * norm_m, axis=0)
    gate_attn_grad = jnp.sum(middle_grad * attn_out, axis=0)
    ag_own = (middle_grad * gate_attn).astype(bf16)
    attn_bpart = jnp.sum(ag_own.astype(f32), axis=0)
    ag_oth = to_core(ag_own)
    aig_own, aig_send, ag_nat, ag_othp, qv_bpart = attn_backward(
        ag_own, ag_oth, x_own, x_oth, a_nat, a_oth, q, k, v, attended, log_norm
    )
    a_half = reduce_pieces(ag_nat, ag_othp)
    aig = aig_own + to_core(aig_send).astype(f32)
    tok_grad = middle_grad + normalize_back(aig, norm_a, inv_a, scale_attn)
    shift_attn_grad = jnp.sum(aig, axis=0)
    scale_attn_grad = jnp.sum(aig * norm_a, axis=0)

    def leave(rows):
        own, other = rows[:tok_count], to_x(rows[tok_count:])
        own_y, other_y = to_y(own), to_y(other)
        result = jnp.zeros((latents, tok_count, width), rows.dtype)
        for value, where_x, where_y in ((own, x, y), (other, 1 - x, y), (own_y, x, 1 - y), (other_y, 1 - x, 1 - y)):
            result = lax.dynamic_update_slice(result, value[None], (2 * where_x + where_y, 0, 0))
        return result

    layer_out = leave(out_rows)
    tokens_grad = leave(tok_grad.astype(bf16)).astype(f32)

    mod_own = jnp.stack(
        [shift_attn_grad, scale_attn_grad, gate_attn_grad, shift_mlp_grad, scale_mlp_grad, gate_mlp_grad]
    ).reshape(-1)
    mod_own = (mod_own + to_core(mod_own)).astype(bf16)
    by_x = jnp.stack([mod_own, to_x(mod_own)])
    by_x = jnp.where(x == 0, by_x, by_x[::-1])
    by_y = jnp.stack([by_x, to_y(by_x)], axis=1)
    by_y = jnp.where(y == 0, by_y, by_y[:, ::-1]).reshape(latents, -1)
    mod_grad_all = z_order(gather_z(by_y), z).reshape(count * latents, -1)
    piece = z * 2 + y
    piece_width = mod_weight.shape[1]
    mod_grad_piece = lax.dynamic_slice_in_dim(mod_grad_all, piece * piece_width, piece_width, 1)
    mod_wgrad = dot_tn(act_all, mod_grad_piece)
    mod_bgrad = jnp.sum(mod_grad_piece.astype(f32), axis=0)
    act_part = dot_nt(mod_grad_piece, mod_weight)
    part_for = lambda step: lax.dynamic_slice_in_dim(act_part, ((z + step) % count) * latents, latents, 0)
    act_z = part_for(0)
    for step in range(1, count):
        act_z = act_z + to_z(part_for(step), step)
    own_rows = latents // 2
    act_grad = lax.dynamic_slice_in_dim(act_z, y * own_rows, own_rows, 0) + to_y(
        lax.dynamic_slice_in_dim(act_z, (1 - y) * own_rows, own_rows, 0)
    )
    cond_rows = lax.dynamic_slice_in_dim(cond_all, piece * own_rows, own_rows, 0).astype(f32)
    condition_grad = jax.vjp(jax.nn.silu, cond_rows)[1](act_grad)[0]

    def spread(part, full):
        quarter = part.shape[-1] // 2
        zero = jnp.zeros(part.shape[:-1] + (full,), f32)
        plane = full // 2
        at = [0] * (part.ndim - 1)
        zero = lax.dynamic_update_slice(zero, part[..., :quarter], (*at, y * plane + core * quarter))
        return lax.dynamic_update_slice(zero, part[..., quarter:], (*at, (1 - y) * plane + core * quarter))

    qv_spread = spread(qv_bpart, width)
    up_spread = spread(up_bpart, up_bpart.shape[0] * 2)
    packed = hyper_sum(jnp.concatenate([qv_spread.reshape(-1), up_spread, attn_bpart, down_bpart]))
    qv_sum = packed[: 2 * width].reshape(2, width // 128, 128)
    up_sum = packed[2 * width : 2 * width + up_spread.shape[0]].reshape(-1, 128)
    rest = packed[2 * width + up_spread.shape[0] :].reshape(2, width)
    lanes = 128 // count
    qv_bgrad = lax.dynamic_slice(qv_sum, (0, y * qv_bias.shape[1], z * lanes), qv_bias.shape)
    up_bgrad = lax.dynamic_slice(up_sum, (y * up_bias.shape[0], z * lanes), up_bias.shape)
    attn_bgrad = lax.dynamic_slice_in_dim(rest[0], z * (width // count), width // count, 0)
    down_bgrad = lax.dynamic_slice_in_dim(rest[1], z * (width // count), width // count, 0)

    def both(part, axis):
        other = to_core(part)
        first = jnp.where(core == 0, part, other)
        second = jnp.where(core == 0, other, part)
        return jnp.concatenate([first, second], axis=axis)

    qkv_wgrad = both(a_half[:3], 2)
    attn_wgrad = both(a_half[3], 0)
    up_wgrad = both(up_half, 1)
    down_wgrad = both(down_half, 0)
    return (
        layer_out, tokens_grad, condition_grad, mod_wgrad, mod_bgrad, qkv_wgrad, qv_bgrad,
        attn_wgrad, attn_bgrad, up_wgrad, up_bgrad, down_wgrad, down_bgrad,
    )


def solution(mesh):
    placed = (
        P("fsdp", "ctx", None),
        P("fsdp", None),
        P(None, ("fsdp", "tp")),
        P(("fsdp", "tp")),
        P(None, "fsdp", "tp"),
        P(None, "tp", "fsdp"),
        P("tp", "fsdp"),
        P("fsdp"),
        P("fsdp", "tp"),
        P("tp", "fsdp"),
        P("tp", "fsdp"),
        P("fsdp"),
        P("fsdp", "ctx", None),
    )
    shape = dict(mesh.shape)
    chip_per_latent = shape["ctx"] == 4 and shape["tp"] == 2 and shape["fsdp"] == 4
    return jax.shard_map(
        fast_body if chip_per_latent else body,
        mesh=mesh,
        in_specs=placed,
        out_specs=(
            P("fsdp", "ctx", None),
            P("fsdp", "ctx", None),
            P(("fsdp", "tp"), None),
            P(None, ("fsdp", "tp")),
            P(("fsdp", "tp")),
            P(None, "fsdp", "tp"),
            P(None, "tp", "fsdp"),
            P("tp", "fsdp"),
            P("fsdp"),
            P("fsdp", "tp"),
            P("tp", "fsdp"),
            P("tp", "fsdp"),
            P("fsdp"),
        ),
        check_vma=False,
    )
```

```python
import functools
import math

import jax
import jax.numpy as jnp
from jax import lax
from jax.experimental import pallas as pl
from jax.experimental.pallas import tpu as pltpu
from jax.sharding import PartitionSpec as P


def modulate(tok_rows, shift_row, scale_row):
    centre = tok_rows - jnp.mean(tok_rows, axis=-1, keepdims=True)
    spread = jnp.mean(centre * centre, axis=-1, keepdims=True)
    normed = centre * lax.rsqrt(spread + 1e-06)
    return normed * (1.0 + scale_row[:, None, :]) + shift_row[:, None, :]


def gelu_tanh(pre_act):
    return jax.nn.gelu(pre_act, approximate=True)


def flat_dot(left, right):
    return jnp.dot(left, right, preferred_element_type=jnp.float32)


def head_slice(source, latent, head_pair):
    row_count = source.shape[1]
    picked = lax.dynamic_slice(source, (latent, 0, head_pair * 128), (1, row_count, 128))
    return picked[0].reshape(row_count, 2, 64)


def tokens_major(stacked, latents, head_pairs):
    row_count = stacked.shape[-2]
    grouped = stacked.reshape(latents, head_pairs, row_count, 128)
    return jnp.transpose(grouped, (0, 2, 1, 3)).reshape(latents, row_count, head_pairs * 128)


def attend(queries, keys_all, values_all, head_pairs):

    def attend_per_block(block_index):
        latent = block_index // head_pairs
        head_pair = block_index % head_pairs
        query_h = head_slice(queries, latent, head_pair)
        key_h = head_slice(keys_all, latent, head_pair)
        value_h = head_slice(values_all, latent, head_pair)
        scores = (
            jnp.einsum("qhd,khd->hqk", query_h, key_h, preferred_element_type=jnp.float32) * 0.125
        )
        row_max = jnp.max(scores, axis=-1, keepdims=True)
        weights = jnp.exp(scores - row_max)
        row_total = jnp.sum(weights, axis=-1, keepdims=True)
        probs_low = (weights / row_total).astype(jnp.bfloat16)
        attended = jnp.einsum(
            "hqk,khd->qhd", probs_low, value_h, preferred_element_type=jnp.float32
        )
        return (attended.reshape(query_h.shape[0], 128), (row_max + jnp.log(row_total))[..., 0])

    return lax.map(attend_per_block, jnp.arange(queries.shape[0] * head_pairs))


def query_side(queries, keys_all, values_all, grad_rows, log_norm, head_pairs):

    def query_per_block(packed):
        block_index, norm_block = packed
        latent = block_index // head_pairs
        head_pair = block_index % head_pairs
        query_h = head_slice(queries, latent, head_pair)
        key_h = head_slice(keys_all, latent, head_pair)
        value_h = head_slice(values_all, latent, head_pair)
        grad_h = head_slice(grad_rows, latent, head_pair)
        scores = (
            jnp.einsum("qhd,khd->hqk", query_h, key_h, preferred_element_type=jnp.float32) * 0.125
        )
        probs = jnp.exp(scores - norm_block[..., None])
        dprobs = jnp.einsum("qhd,khd->hqk", grad_h, value_h, preferred_element_type=jnp.float32)
        row_delta = jnp.sum(probs * dprobs, axis=-1, keepdims=True)
        score_grad = (probs * (dprobs - row_delta)).astype(jnp.bfloat16)
        query_grad = (
            jnp.einsum("hqk,khd->qhd", score_grad, key_h, preferred_element_type=jnp.float32)
            * 0.125
        )
        query_count = query_h.shape[0]
        key_grad = (
            jnp.einsum("hqk,qhd->khd", score_grad, query_h, preferred_element_type=jnp.float32)
            * 0.125
        )
        value_grad = jnp.einsum(
            "hqk,qhd->khd", probs.astype(jnp.bfloat16), grad_h, preferred_element_type=jnp.float32
        )
        return (
            query_grad.reshape(query_count, 128),
            key_grad.reshape(-1, 128),
            value_grad.reshape(-1, 128),
        )

    return lax.map(query_per_block, (jnp.arange(queries.shape[0] * head_pairs), log_norm))


def body(
    tokens,
    condition,
    mod_weight,
    mod_bias,
    qkv_weight,
    qv_bias,
    attn_weight,
    attn_bias,
    up_weight,
    up_bias,
    down_weight,
    down_bias,
    cotangent,
):
    latents, tok_count, width = tokens.shape
    gathered = (
        lax.all_gather(condition, "fsdp", axis=0, tiled=True),
        lax.all_gather(qkv_weight, "fsdp", axis=1, tiled=True),
        lax.all_gather(qv_bias, "fsdp", axis=2, tiled=True),
        lax.all_gather(attn_weight, "fsdp", axis=1, tiled=True),
        lax.all_gather(attn_bias, "fsdp", axis=0, tiled=True),
        lax.all_gather(up_weight, "fsdp", axis=0, tiled=True),
        lax.all_gather(up_bias, "fsdp", axis=1, tiled=True),
        lax.all_gather(down_weight, "fsdp", axis=1, tiled=True),
        lax.all_gather(down_bias, "fsdp", axis=0, tiled=True),
    )
    (
        cond_all,
        qkv_full,
        qv_full,
        attn_full,
        attn_bias_full,
        up_full,
        up_bias_full,
        down_full,
        down_bias_full,
    ) = gathered
    q_bias = qv_full[0].reshape(-1).astype(jnp.float32)
    v_bias = qv_full[1].reshape(-1).astype(jnp.float32)
    hidden_bias = up_bias_full.reshape(-1).astype(jnp.float32)
    act_all = jax.nn.silu(cond_all.astype(jnp.float32)).astype(jnp.bfloat16)
    mod_piece = flat_dot(act_all, mod_weight) + mod_bias.astype(jnp.float32)
    mod_full = lax.all_gather(mod_piece, ("fsdp", "tp"), axis=1, tiled=True)
    first_latent = lax.axis_index("fsdp") * latents
    modulation = lax.dynamic_slice_in_dim(mod_full, first_latent, latents, 0).reshape(
        latents, 6, width
    )
    shift_attn, scale_attn, gate_attn = (modulation[:, 0], modulation[:, 1], modulation[:, 2])
    shift_mlp, scale_mlp, gate_mlp = (modulation[:, 3], modulation[:, 4], modulation[:, 5])
    tok_float = tokens.astype(jnp.float32)
    attn_input_f, norm_pull_attn = jax.vjp(modulate, tok_float, shift_attn, scale_attn)
    attn_input = attn_input_f.astype(jnp.bfloat16).reshape(-1, width)
    queries = (
        (flat_dot(attn_input, qkv_full[0]) + q_bias)
        .astype(jnp.bfloat16)
        .reshape(latents, tok_count, -1)
    )
    keys_own = (
        flat_dot(attn_input, qkv_full[1]).astype(jnp.bfloat16).reshape(latents, tok_count, -1)
    )
    values_own = (
        (flat_dot(attn_input, qkv_full[2]) + v_bias)
        .astype(jnp.bfloat16)
        .reshape(latents, tok_count, -1)
    )
    keys_all, values_all = (
        lax.all_gather(keys_own, "ctx", axis=1, tiled=True),
        lax.all_gather(values_own, "ctx", axis=1, tiled=True),
    )
    head_width = queries.shape[-1]
    head_pairs = head_width // 128
    attended_st, log_norm = attend(queries, keys_all, values_all, head_pairs)
    attended = (
        tokens_major(attended_st, latents, head_pairs).astype(jnp.bfloat16).reshape(-1, head_width)
    )
    attn_out = lax.psum(flat_dot(attended, attn_full), "tp") + attn_bias_full.astype(jnp.float32)
    attn_out = attn_out.reshape(latents, tok_count, width)
    middle = tok_float + gate_attn[:, None, :] * attn_out
    mlp_input_f, norm_pull_mlp = jax.vjp(modulate, middle, shift_mlp, scale_mlp)
    mlp_input = mlp_input_f.astype(jnp.bfloat16).reshape(-1, width)
    up_pre = flat_dot(mlp_input, up_full) + hidden_bias
    up_act_f, gelu_pull = jax.vjp(gelu_tanh, up_pre)
    up_act = up_act_f.astype(jnp.bfloat16)
    mlp_out = lax.psum(flat_dot(up_act, down_full), "tp") + down_bias_full.astype(jnp.float32)
    mlp_out = mlp_out.reshape(latents, tok_count, width)
    layer_out = (middle + gate_mlp[:, None, :] * mlp_out).astype(jnp.bfloat16)
    out_grad = cotangent.astype(jnp.float32)
    gate_mlp_grad = jnp.sum(out_grad * mlp_out, axis=1)
    mlp_grad = (out_grad * gate_mlp[:, None, :]).astype(jnp.bfloat16).reshape(-1, width)
    down_bgrad_part = jnp.sum(mlp_grad.astype(jnp.float32), axis=0)
    down_wgrad_part = flat_dot(up_act.T, mlp_grad)
    up_grad = gelu_pull(flat_dot(mlp_grad, down_full.T))[0].astype(jnp.bfloat16)
    up_bgrad_part = jnp.sum(up_grad.astype(jnp.float32), axis=0)
    up_wgrad_part = flat_dot(mlp_input.T, up_grad)
    mlp_input_grad = lax.psum(flat_dot(up_grad, up_full.T), "tp").reshape(latents, tok_count, width)
    middle_part, shift_mlp_grad, scale_mlp_grad = norm_pull_mlp(mlp_input_grad)
    middle_grad = out_grad + middle_part
    gate_attn_grad = jnp.sum(middle_grad * attn_out, axis=1)
    attn_grad = (middle_grad * gate_attn[:, None, :]).astype(jnp.bfloat16).reshape(-1, width)
    attn_bgrad_part = jnp.sum(attn_grad.astype(jnp.float32), axis=0)
    attn_wgrad_part = flat_dot(attended.T, attn_grad)
    attended_grad = (
        flat_dot(attn_grad, attn_full.T)
        .astype(jnp.bfloat16)
        .reshape(latents, tok_count, head_width)
    )
    query_st, key_st, value_st = query_side(
        queries, keys_all, values_all, attended_grad, log_norm, head_pairs
    )
    key_parts = key_st.reshape(latents, head_pairs, -1, 128)
    value_parts = value_st.reshape(latents, head_pairs, -1, 128)
    key_sum, value_sum = (
        lax.psum_scatter(key_parts, "ctx", scatter_dimension=2, tiled=True),
        lax.psum_scatter(value_parts, "ctx", scatter_dimension=2, tiled=True),
    )
    key_grad = tokens_major(
        key_sum.reshape(latents * head_pairs, tok_count, 128), latents, head_pairs
    )
    value_grad = tokens_major(
        value_sum.reshape(latents * head_pairs, tok_count, 128), latents, head_pairs
    )
    query_flat = (
        tokens_major(query_st, latents, head_pairs).astype(jnp.bfloat16).reshape(-1, head_width)
    )
    key_flat = key_grad.astype(jnp.bfloat16).reshape(-1, head_width)
    value_flat = value_grad.astype(jnp.bfloat16).reshape(-1, head_width)
    input_terms = (
        flat_dot(query_flat, qkv_full[0].T)
        + flat_dot(key_flat, qkv_full[1].T)
        + flat_dot(value_flat, qkv_full[2].T)
    )
    attn_input_grad = lax.psum(input_terms, "tp").reshape(latents, tok_count, width)
    qkv_wgrad_part = jnp.stack(
        [
            flat_dot(attn_input.T, query_flat),
            flat_dot(attn_input.T, key_flat),
            flat_dot(attn_input.T, value_flat),
        ]
    )
    qv_bgrad_part = jnp.stack(
        [
            jnp.sum(query_flat.astype(jnp.float32), axis=0),
            jnp.sum(value_flat.astype(jnp.float32), axis=0),
        ]
    ).reshape(2, -1, 128)
    token_part, shift_attn_grad, scale_attn_grad = norm_pull_attn(attn_input_grad)
    tokens_grad = middle_grad + token_part
    mod_grad_own = jnp.stack(
        [
            shift_attn_grad,
            scale_attn_grad,
            gate_attn_grad,
            shift_mlp_grad,
            scale_mlp_grad,
            gate_mlp_grad,
        ],
        axis=1,
    ).reshape(latents, -1)
    mod_grad_slab = lax.dynamic_update_slice_in_dim(
        jnp.zeros(mod_full.shape, jnp.float32), mod_grad_own, first_latent, 0
    )
    mod_grad_all = lax.psum(mod_grad_slab, ("fsdp", "ctx")).astype(jnp.bfloat16)
    piece = lax.axis_index("fsdp") * lax.axis_size("tp") + lax.axis_index("tp")
    piece_width = mod_weight.shape[1]
    mod_grad_piece = lax.dynamic_slice_in_dim(mod_grad_all, piece * piece_width, piece_width, 1)
    mod_wgrad = flat_dot(act_all.T, mod_grad_piece)
    mod_bgrad = jnp.sum(mod_grad_piece.astype(jnp.float32), axis=0)
    own_rows = mod_full.shape[0] // (lax.axis_size("fsdp") * lax.axis_size("tp"))
    act_grad = lax.psum_scatter(
        flat_dot(mod_grad_piece, mod_weight.T), ("fsdp", "tp"), scatter_dimension=0, tiled=True
    )
    cond_rows = lax.dynamic_slice_in_dim(cond_all, piece * own_rows, own_rows, 0).astype(
        jnp.float32
    )
    condition_grad = jax.vjp(jax.nn.silu, cond_rows)[1](act_grad)[0]
    partials = (
        qkv_wgrad_part,
        qv_bgrad_part,
        attn_wgrad_part,
        attn_bgrad_part,
        up_wgrad_part,
        up_bgrad_part.reshape(-1, 128),
        down_wgrad_part,
        down_bgrad_part,
    )
    shards = (
        lax.psum_scatter(partials[0], "fsdp", scatter_dimension=1, tiled=True),
        lax.psum_scatter(partials[1], "fsdp", scatter_dimension=2, tiled=True),
        lax.psum_scatter(partials[2], "fsdp", scatter_dimension=1, tiled=True),
        lax.psum_scatter(partials[3], "fsdp", scatter_dimension=0, tiled=True),
        lax.psum_scatter(partials[4], "fsdp", scatter_dimension=0, tiled=True),
        lax.psum_scatter(partials[5], "fsdp", scatter_dimension=1, tiled=True),
        lax.psum_scatter(partials[6], "fsdp", scatter_dimension=1, tiled=True),
        lax.psum_scatter(partials[7], "fsdp", scatter_dimension=0, tiled=True),
    )
    reduced = lax.psum(
        (shards[0], shards[1], shards[2], shards[3], shards[4], shards[5], shards[6], shards[7]),
        "ctx",
    )
    qkv_wgrad, qv_bgrad, attn_wgrad, attn_bgrad, up_wgrad, up_bgrad, down_wgrad, down_bgrad = (
        reduced
    )
    return (
        layer_out,
        tokens_grad,
        condition_grad,
        mod_wgrad,
        mod_bgrad,
        qkv_wgrad,
        qv_bgrad,
        attn_wgrad,
        attn_bgrad,
        up_wgrad,
        up_bgrad,
        down_wgrad,
        down_bgrad,
    )


X_SWAP = [(0, 2), (2, 0), (1, 3), (3, 1)]
CORE_SWAP = [(0, 1), (1, 0), (2, 3), (3, 2)]
Y_SWAP = [(0, 1), (1, 0)]


def to_x(value):
    return lax.ppermute(value, "ctx", X_SWAP)


def to_core(value):
    return lax.ppermute(value, "ctx", CORE_SWAP)


def to_y(value):
    return lax.ppermute(value, "tp", Y_SWAP)


def to_z(value, step):
    count = lax.axis_size("fsdp")
    return lax.ppermute(value, "fsdp", [(src, (src + step) % count) for src in range(count)])


def z_order(relative, z):
    count = len(relative)
    back = list(relative[::-1])
    doubled = jnp.stack(back + back[:-1])
    return lax.dynamic_slice_in_dim(doubled, count - 1 - z, count, 0)


def pick(stacked, index):
    return lax.dynamic_index_in_dim(stacked, index, 0, keepdims=False)


def gather_z(value):
    count = lax.axis_size("fsdp")
    return [value] + [to_z(value, step) for step in range(1, count)]


def normalize(rows):
    centre = rows - jnp.mean(rows, axis=-1, keepdims=True)
    spread = jnp.mean(centre * centre, axis=-1, keepdims=True)
    inverse = lax.rsqrt(spread + 1e-06)
    return centre * inverse, inverse


def normalize_back(grad, normed, inverse, scale):
    e = grad * (1.0 + scale)
    mean_e = jnp.mean(e, axis=-1, keepdims=True)
    mean_en = jnp.mean(e * normed, axis=-1, keepdims=True)
    return (e - mean_e - normed * mean_en) * inverse


def dot_nt(left, right):
    return lax.dot_general(left, right, (((1,), (1,)), ((), ())), preferred_element_type=jnp.float32)


def dot_tn(left, right):
    return lax.dot_general(left, right, (((0,), (0,)), ((), ())), preferred_element_type=jnp.float32)


ANYWHERE = pl.BlockSpec(memory_space=pl.ANY)
VMEM_BYTES = 64 * 1024 * 1024 - 4 * 65536


def nt(left, right):
    return lax.dot_general(left, right, (((1,), (1,)), ((), ())), preferred_element_type=jnp.float32)


def nn(left, right):
    return lax.dot_general(left, right, (((1,), (0,)), ((), ())), preferred_element_type=jnp.float32)


def block_of(index, size):
    return pl.ds(pl.multiple_of(index * size, size), size)


def shard_of(z, step, count):
    return lax.rem(z - step + count, count)


def shard_for(z, step, count):
    return lax.rem(z + step, count)


def attn_copies(plane, pieces, wqkv, wout, sems):
    count = len(pieces)
    z = lax.axis_index("fsdp")
    result = []
    for step, piece in enumerate(pieces):
        rows = piece.shape[1]
        at = block_of(shard_of(z, step, count), rows)
        result.append(pltpu.make_async_copy(piece.at[pl.ds(0, 3)], wqkv.at[plane, :, at, :], sems.at[plane, step, 0]))
        result.append(pltpu.make_async_copy(piece.at[3], wout.at[plane, :, at], sems.at[plane, step, 1]))
    return result


def row_copies(refs, target, sems):
    half = refs[0].shape[0]
    return [
        pltpu.make_async_copy(ref, target.at[pl.ds(i * half, half)], sems.at[i]) for i, ref in enumerate(refs)
    ]


def head_mask(rows, head):
    lane = lax.broadcasted_iota(jnp.int32, (rows, 128), 1)
    return (lane >= 64 * head) & (lane < 64 * head + 64)


def attn_forward_kernel(count, block, *refs):
    x_own, x_oth = refs[:2]
    pieces = (refs[2 : 2 + count], refs[2 + count : 2 + 2 * count])
    qb, vb, q_ref, k_ref, v_ref, att_ref, lse_ref, out_own, out_send = refs[2 + 2 * count : 11 + 2 * count]
    xs, wqkv, wout, vt, acc, w_sem, x_sem, o_sem = refs[11 + 2 * count :]
    plane = pl.program_id(0)
    rows = xs.shape[0]
    half = rows // 2
    f32, bf16 = jnp.float32, jnp.bfloat16

    @pl.when(plane == 0)
    def _():
        for copy in row_copies((x_own, x_oth), xs, x_sem):
            copy.start()
        for p in range(2):
            for copy in attn_copies(p, pieces[p], wqkv, wout, w_sem):
                copy.start()
        for copy in row_copies((x_own, x_oth), xs, x_sem):
            copy.wait()

    for p in range(2):

        @pl.when(plane == p)
        def _():
            for copy in attn_copies(p, pieces[p], wqkv, wout, w_sem):
                copy.wait()

    def project(b, _):
        at = block_of(b, block)
        xb = xs[at, :]
        q_ref[0, at, :] = (nn(xb, wqkv[plane, 0]) + qb[...]).astype(bf16)
        k_ref[0, at, :] = nn(xb, wqkv[plane, 1]).astype(bf16)
        value = (nn(xb, wqkv[plane, 2]) + vb[...]).astype(bf16)
        v_ref[0, at, :] = value
        vt[:, at] = value.T
        return 0

    lax.fori_loop(0, rows // block, project, 0)

    for pair in range(2):
        lanes = slice(128 * pair, 128 * pair + 128)

        def attend(b, _):
            at = block_of(b, block)
            qp = q_ref[0, at, lanes] * jnp.bfloat16(0.125)
            keys = k_ref[0, :, lanes]
            tops = []
            for head in range(2):
                scores = nt(keys, jnp.where(head_mask(block, head), qp, jnp.bfloat16(0)))
                top = jnp.max(scores, axis=0, keepdims=True)
                weights = jnp.exp(scores - top)
                total = jnp.sum(weights, axis=0, keepdims=True)
                probs = (weights * (1.0 / total)).astype(bf16)
                low = 128 * pair + 64 * head
                tops.append(nn(vt[low : low + 64, :], probs))
                lse_ref[0, 2 * pair + head : 2 * pair + head + 1, at] = top + jnp.log(total)
            att_ref[0, at, lanes] = jnp.concatenate(tops, axis=0).T.astype(bf16)
            return 0

        lax.fori_loop(0, rows // block, attend, 0)

    def finish(b, _):
        at = block_of(b, block)
        term = nn(att_ref[0, at, :], wout[plane])

        @pl.when(plane == 0)
        def _():
            acc[at, :] = term

        @pl.when(plane == 1)
        def _():
            acc[at, :] = acc[at, :] + term

        return 0

    lax.fori_loop(0, rows // block, finish, 0)

    @pl.when(plane == 1)
    def _():
        for i, ref in enumerate((out_own, out_send)):
            pltpu.make_async_copy(acc.at[pl.ds(i * half, half)], ref, o_sem.at[i]).start()
        for i, ref in enumerate((out_own, out_send)):
            pltpu.make_async_copy(acc.at[pl.ds(i * half, half)], ref, o_sem.at[i]).wait()


def attn_forward(x_own, x_oth, nat, oth, q_bias, v_bias):
    count = len(nat)
    half, width = x_own.shape
    rows = 2 * half
    wide = nat[0].shape[2]
    bf16, f32 = jnp.bfloat16, jnp.float32
    by_plane = lambda *shape: pl.BlockSpec((1,) + shape, lambda p: (p,) + (0,) * len(shape))
    biases = [b.reshape(2, 1, wide) for b in (q_bias, v_bias)]
    squeezed = pl.BlockSpec((None, 1, wide), lambda p: (p, 0, 0))
    shape = lambda s, d: jax.ShapeDtypeStruct(s, d)
    flops = 2 * rows * width * wide * 2 * 4 + 8 * 2 * rows * rows * 64 * 2
    return pl.pallas_call(
        functools.partial(attn_forward_kernel, count, min(256, half)),
        grid=(2,),
        in_specs=[ANYWHERE] * (2 + 2 * count) + [squeezed] * 2,
        out_specs=[by_plane(rows, wide)] * 4 + [by_plane(4, rows), ANYWHERE, ANYWHERE],
        out_shape=[shape((2, rows, wide), bf16)] * 4 + [shape((2, 4, rows), f32)] + [shape((half, width), f32)] * 2,
        scratch_shapes=[
            pltpu.VMEM((rows, width), bf16),
            pltpu.VMEM((2, 3, width, wide), bf16),
            pltpu.VMEM((2, wide, width), bf16),
            pltpu.VMEM((wide, rows), bf16),
            pltpu.VMEM((rows, width), f32),
            pltpu.SemaphoreType.DMA((2, count, 2)),
            pltpu.SemaphoreType.DMA((2,)),
            pltpu.SemaphoreType.DMA((2,)),
        ],
        compiler_params=pltpu.CompilerParams(dimension_semantics=("arbitrary",), vmem_limit_bytes=VMEM_BYTES),
        cost_estimate=pl.CostEstimate(flops=flops, bytes_accessed=18 << 20, transcendentals=8 * rows * rows),
        name="attn_forward",
    )(x_own, x_oth, *nat, *oth, *biases)


def attn_backward_kernel(count, block, *refs):
    g_own, g_oth, x_own, x_oth = refs[:4]
    pieces = (refs[4 : 4 + count], refs[4 + count : 4 + 2 * count])
    refs = refs[4 + 2 * count :]
    q_ref, k_ref, v_ref, att_ref, lse_ref = refs[:5]
    back_own, back_send = refs[5:7]
    grads = (refs[7 : 7 + count], refs[7 + count : 7 + 2 * count])
    bias_ref = refs[7 + 2 * count]
    (gs, xs, xt, attt, wqkv, wout, d_att, dq, dk, dv, kt, dk_acc, dv_acc, acc, wg, awg, w_sem, x_sem, o_sem, g_sem) = refs[
        8 + 2 * count :
    ]
    plane = pl.program_id(0)
    rows = xs.shape[0]
    half = rows // 2
    f32, bf16 = jnp.float32, jnp.bfloat16
    z = lax.axis_index("fsdp")
    blocks = rows // block

    @pl.when(plane == 0)
    def _():
        inputs = row_copies((g_own, g_oth), gs, x_sem.at[0]) + row_copies((x_own, x_oth), xs, x_sem.at[1])
        for copy in inputs:
            copy.start()
        for p in range(2):
            for copy in attn_copies(p, pieces[p], wqkv, wout, w_sem):
                copy.start()
        for copy in inputs:
            copy.wait()

        def flip(b, _):
            at = block_of(b, block)
            xt[:, at] = xs[at, :].T
            return 0

        lax.fori_loop(0, blocks, flip, 0)

    for p in range(2):

        @pl.when(plane == p)
        def _():
            for copy in attn_copies(p, pieces[p], wqkv, wout, w_sem):
                copy.wait()

    def enter(b, _):
        at = block_of(b, block)
        d_att[at, :] = nt(gs[at, :], wout[plane]).astype(bf16)
        attt[:, at] = att_ref[0, at, :].T
        kt[:, at] = k_ref[0, at, :].T
        return 0

    lax.fori_loop(0, blocks, enter, 0)

    for pair in range(2):
        lanes = slice(128 * pair, 128 * pair + 128)
        dk_acc[...] = jnp.zeros_like(dk_acc)
        dv_acc[...] = jnp.zeros_like(dv_acc)

        def step(b, _):
            at = block_of(b, block)
            qp = q_ref[0, at, lanes] * jnp.bfloat16(0.125)
            dp = d_att[at, lanes]
            keys = k_ref[0, :, lanes]
            values = v_ref[0, :, lanes]
            tops, p_all, s_all, q_all, d_all = [], [], [], [], []
            for head in range(2):
                mask = head_mask(block, head)
                qm = jnp.where(mask, qp, jnp.bfloat16(0))
                dm = jnp.where(mask, dp, jnp.bfloat16(0))
                r = 2 * pair + head
                probs = jnp.exp(nt(keys, qm) - lse_ref[0, r : r + 1, at])
                dprobs = nt(values, dm)
                delta = jnp.sum(probs * dprobs, axis=0, keepdims=True)
                ds = (probs * (dprobs - delta)).astype(bf16)
                low = 128 * pair + 64 * head
                tops.append(nn(kt[low : low + 64, :], ds))
                dv_acc[...] = dv_acc[...] + nn(probs.astype(bf16), dm)
                dk_acc[...] = dk_acc[...] + nn(ds, qm)
            dq[at, lanes] = (jnp.concatenate(tops, axis=0).T * 0.125).astype(bf16)
            return 0

        lax.fori_loop(0, blocks, step, 0)
        dk[:, lanes] = dk_acc[...].astype(bf16)
        dv[:, lanes] = dv_acc[...].astype(bf16)

    bias_ref[0, 0:1, :] = jnp.sum(dq[...].astype(f32), axis=0, keepdims=True)
    bias_ref[0, 1:2, :] = jnp.sum(dv[...].astype(f32), axis=0, keepdims=True)

    def leave(b, _):
        at = block_of(b, block)
        term = nt(dq[at, :], wqkv[plane, 0]) + nt(dk[at, :], wqkv[plane, 1]) + nt(dv[at, :], wqkv[plane, 2])

        @pl.when(plane == 0)
        def _():
            acc[at, :] = term

        @pl.when(plane == 1)
        def _():
            acc[at, :] = acc[at, :] + term

        return 0

    lax.fori_loop(0, blocks, leave, 0)

    outs = ((back_own, 0), (back_send, 1))

    @pl.when(plane == 1)
    def _():
        for ref, i in outs:
            pltpu.make_async_copy(acc.at[pl.ds(i * half, half)], ref, o_sem.at[i]).start()

    def weigh(b, _):
        at = block_of(b, block)
        xb = xt[at, :]
        for part, ref in enumerate((dq, dk, dv)):
            wg[plane, part, at, :] = nn(xb, ref[...]).astype(bf16)
        return 0

    lax.fori_loop(0, xt.shape[0] // block, weigh, 0)
    awg[plane] = nn(attt[...], gs[...]).astype(bf16)

    def sends(p):
        result = []
        for step_, ref in enumerate(grads[p]):
            depth = ref.shape[1]
            at = block_of(shard_for(z, step_, count), depth)
            result.append(pltpu.make_async_copy(wg.at[p, :, at, :], ref.at[pl.ds(0, 3)], g_sem.at[p, step_, 0]))
            result.append(pltpu.make_async_copy(awg.at[p, :, at], ref.at[3], g_sem.at[p, step_, 1]))
        return result

    for p in range(2):

        @pl.when(plane == p)
        def _():
            for copy in sends(p):
                copy.start()

    @pl.when(plane == 1)
    def _():
        for ref, i in outs:
            pltpu.make_async_copy(acc.at[pl.ds(i * half, half)], ref, o_sem.at[i]).wait()
        for p in range(2):
            for copy in sends(p):
                copy.wait()


def attn_backward(g_own, g_oth, x_own, x_oth, nat, oth, q, k, v, attended, log_norm):
    count = len(nat)
    half, width = x_own.shape
    rows = 2 * half
    wide = nat[0].shape[2]
    bf16, f32 = jnp.bfloat16, jnp.float32
    by_plane = lambda *shape: pl.BlockSpec((1,) + shape, lambda p: (p,) + (0,) * len(shape))
    shape = lambda s, d: jax.ShapeDtypeStruct(s, d)
    flops = 2 * rows * width * wide * 2 * 8 + 8 * 5 * rows * rows * 64 * 2
    block = min(256, half)
    results = pl.pallas_call(
        functools.partial(attn_backward_kernel, count, block),
        grid=(2,),
        in_specs=[ANYWHERE] * (4 + 2 * count) + [by_plane(rows, wide)] * 4 + [by_plane(4, rows)],
        out_specs=[ANYWHERE] * (2 + 2 * count) + [by_plane(2, wide)],
        out_shape=[shape((half, width), f32)] * 2
        + [shape(nat[0].shape, bf16)] * (2 * count)
        + [shape((2, 2, wide), f32)],
        scratch_shapes=[
            pltpu.VMEM((rows, width), bf16),
            pltpu.VMEM((rows, width), bf16),
            pltpu.VMEM((width, rows), bf16),
            pltpu.VMEM((wide, rows), bf16),
            pltpu.VMEM((2, 3, width, wide), bf16),
            pltpu.VMEM((2, wide, width), bf16),
            pltpu.VMEM((rows, wide), bf16),
            pltpu.VMEM((rows, wide), bf16),
            pltpu.VMEM((rows, wide), bf16),
            pltpu.VMEM((rows, wide), bf16),
            pltpu.VMEM((wide, rows), bf16),
            pltpu.VMEM((rows, 128), f32),
            pltpu.VMEM((rows, 128), f32),
            pltpu.VMEM((rows, width), f32),
            pltpu.VMEM((2, 3, width, wide), bf16),
            pltpu.VMEM((2, wide, width), bf16),
            pltpu.SemaphoreType.DMA((2, count, 2)),
            pltpu.SemaphoreType.DMA((2, 2)),
            pltpu.SemaphoreType.DMA((2,)),
            pltpu.SemaphoreType.DMA((2, count, 2)),
        ],
        compiler_params=pltpu.CompilerParams(dimension_semantics=("arbitrary",), vmem_limit_bytes=VMEM_BYTES),
        cost_estimate=pl.CostEstimate(flops=flops, bytes_accessed=24 << 20, transcendentals=8 * rows * rows),
        name="attn_backward",
    )(g_own, g_oth, x_own, x_oth, *nat, *oth, q, k, v, attended, log_norm)
    back_own, back_send = results[:2]
    bias = jnp.transpose(results[-1], (1, 0, 2)).reshape(2, -1)
    return back_own, back_send, results[2 : 2 + count], results[2 + count : 2 + 2 * count], bias


GELU_A = math.sqrt(2.0 / math.pi)
GELU_B = 0.044715


def mlp_copies(plane, ups, downs, upw, downw, sems):
    count = len(ups)
    z = lax.axis_index("fsdp")
    result = []
    for step in range(count):
        at = block_of(shard_of(z, step, count), ups[step].shape[0])
        result.append(pltpu.make_async_copy(ups[step], upw.at[plane, at, :], sems.at[plane, step, 0]))
        result.append(pltpu.make_async_copy(downs[step], downw.at[plane, :, at], sems.at[plane, step, 1]))
    return result


def mlp_kernel(count, block, tile, *refs):
    m_own, m_oth, g_own, g_oth = refs[:4]
    refs = refs[4:]
    ups, downs = (refs[:count], refs[count : 2 * count]), (refs[2 * count : 3 * count], refs[3 * count : 4 * count])
    bias_ref = refs[4 * count]
    refs = refs[4 * count + 1 :]
    out_own, out_send, back_own, back_send = refs[:4]
    refs = refs[4:]
    up_out, down_out = (refs[:count], refs[count : 2 * count]), (refs[2 * count : 3 * count], refs[3 * count : 4 * count])
    bgrad_ref = refs[4 * count]
    (ms, mt, gs, upw, downw, out_acc, back_acc, ugs, actt, upg, downg, w_sem, x_sem, o_sem, g_sem) = refs[4 * count + 1 :]
    plane, part = pl.program_id(0), pl.program_id(1)
    parts = pl.num_programs(1)
    rows, width = ms.shape
    half = rows // 2
    f32, bf16 = jnp.float32, jnp.bfloat16
    z = lax.axis_index("fsdp")
    first = (plane == 0) & (part == 0)
    final = (plane == 1) & (part == parts - 1)

    @pl.when(first)
    def _():
        inputs = row_copies((m_own, m_oth), ms, x_sem.at[0]) + row_copies((g_own, g_oth), gs, x_sem.at[1])
        for copy in inputs:
            copy.start()
        for p in range(2):
            for copy in mlp_copies(p, ups[p], downs[p], upw, downw, w_sem):
                copy.start()
        for copy in inputs:
            copy.wait()

        def flip(b, _):
            at = block_of(b, block)
            mt[:, at] = ms[at, :].T
            return 0

        lax.fori_loop(0, rows // block, flip, 0)

    for p in range(2):

        @pl.when((plane == p) & (part == 0))
        def _():
            for copy in mlp_copies(p, ups[p], downs[p], upw, downw, w_sem):
                copy.wait()

    hidden = block_of(part, tile)

    def work(b, total):
        at = block_of(b, block)
        pre = nn(ms[at, :], upw[plane, :, hidden]) + bias_ref[...]
        dact = nt(gs[at, :], downw[plane, hidden, :])
        square = pre * pre
        inner = jnp.tanh(GELU_A * (pre + GELU_B * (square * pre)))
        half_plus = 0.5 + 0.5 * inner
        act = (pre * half_plus).astype(bf16)
        slope = half_plus + (0.5 * GELU_A) * pre * (1.0 - inner * inner) * (1.0 + (3.0 * GELU_B) * square)
        ug = (dact * slope).astype(bf16)
        out_term = nn(act, downw[plane, hidden, :])
        back_term = nt(ug, upw[plane, :, hidden])

        @pl.when(first)
        def _():
            out_acc[at, :] = out_term
            back_acc[at, :] = back_term

        @pl.when(jnp.logical_not(first))
        def _():
            out_acc[at, :] = out_acc[at, :] + out_term
            back_acc[at, :] = back_acc[at, :] + back_term

        ugs[at, :] = ug
        actt[:, at] = act.T
        return total + jnp.sum(ug.astype(f32), axis=0, keepdims=True)

    bgrad_ref[...] = lax.fori_loop(0, rows // block, work, jnp.zeros((1, tile), f32))

    ends = ((out_acc, 0, out_own), (out_acc, 1, out_send), (back_acc, 0, back_own), (back_acc, 1, back_send))

    def results():
        return [
            pltpu.make_async_copy(a.at[pl.ds(i * half, half)], ref, o_sem.at[j]) for j, (a, i, ref) in enumerate(ends)
        ]

    @pl.when(final)
    def _():
        for copy in results():
            copy.start()

    def weigh_up(b, _):
        at = block_of(b, block)
        upg[plane, at, hidden] = nn(mt[at, :], ugs[...]).astype(bf16)
        return 0

    lax.fori_loop(0, width // block, weigh_up, 0)

    def weigh_down(b, _):
        at = block_of(b, block)
        to = pl.ds(pl.multiple_of(part * tile + b * block, block), block)
        downg[plane, to, :] = nn(actt[at, :], gs[...]).astype(bf16)
        return 0

    lax.fori_loop(0, tile // block, weigh_down, 0)

    def sends(p):
        result = []
        for step in range(count):
            at = block_of(shard_for(z, step, count), up_out[p][step].shape[0])
            result.append(pltpu.make_async_copy(upg.at[p, at, :], up_out[p][step], g_sem.at[p, step, 0]))
            result.append(pltpu.make_async_copy(downg.at[p, :, at], down_out[p][step], g_sem.at[p, step, 1]))
        return result

    for p in range(2):

        @pl.when((plane == p) & (part == parts - 1))
        def _():
            for copy in sends(p):
                copy.start()

    @pl.when(final)
    def _():
        for copy in results():
            copy.wait()
        for p in range(2):
            for copy in sends(p):
                copy.wait()


def mlp(m_own, m_oth, g_own, g_oth, up_nat, up_oth, down_nat, down_oth, bias):
    count = len(up_nat)
    half, width = m_own.shape
    rows = 2 * half
    wide = up_nat[0].shape[1]
    tile = min(512, wide)
    parts = wide // tile
    block = min(256, half)
    bf16, f32 = jnp.bfloat16, jnp.float32
    shape = lambda s, d: jax.ShapeDtypeStruct(s, d)
    hidden_spec = pl.BlockSpec((None, None, 1, tile), lambda p, h: (p, h, 0, 0))
    results = pl.pallas_call(
        functools.partial(mlp_kernel, count, block, tile),
        grid=(2, parts),
        in_specs=[ANYWHERE] * (4 + 4 * count) + [hidden_spec],
        out_specs=[ANYWHERE] * (4 + 4 * count) + [hidden_spec],
        out_shape=[shape((half, width), f32)] * 4
        + [shape(up_nat[0].shape, bf16)] * (2 * count)
        + [shape(down_nat[0].shape, bf16)] * (2 * count)
        + [shape((2, parts, 1, tile), f32)],
        scratch_shapes=[
            pltpu.VMEM((rows, width), bf16),
            pltpu.VMEM((width, rows), bf16),
            pltpu.VMEM((rows, width), bf16),
            pltpu.VMEM((2, width, wide), bf16),
            pltpu.VMEM((2, wide, width), bf16),
            pltpu.VMEM((rows, width), f32),
            pltpu.VMEM((rows, width), f32),
            pltpu.VMEM((rows, tile), bf16),
            pltpu.VMEM((tile, rows), bf16),
            pltpu.VMEM((2, width, wide), bf16),
            pltpu.VMEM((2, wide, width), bf16),
            pltpu.SemaphoreType.DMA((2, count, 2)),
            pltpu.SemaphoreType.DMA((2, 2)),
            pltpu.SemaphoreType.DMA((4,)),
            pltpu.SemaphoreType.DMA((2, count, 2)),
        ],
        compiler_params=pltpu.CompilerParams(
            dimension_semantics=("arbitrary", "arbitrary"), vmem_limit_bytes=VMEM_BYTES
        ),
        cost_estimate=pl.CostEstimate(
            flops=6 * 2 * rows * width * 2 * wide, bytes_accessed=40 << 20, transcendentals=rows * 2 * wide
        ),
        name="mlp",
    )(m_own, m_oth, g_own, g_oth, *up_nat, *up_oth, *down_nat, *down_oth, bias.reshape(2, parts, 1, tile))
    grads = results[4:-1]
    return (*results[:4], *[grads[i * count : (i + 1) * count] for i in range(4)], results[-1].reshape(-1))


def reduce_pieces(nat, oth):
    f32 = jnp.float32
    got = [to_y(piece) for piece in oth]
    summed = [(a.astype(f32) + b.astype(f32)) for a, b in zip(nat, got)]
    total = summed[0]
    for step in range(1, len(summed)):
        total = total + to_z(summed[step].astype(jnp.bfloat16), step).astype(f32)
    low = total.astype(jnp.bfloat16)
    return low.astype(f32) + to_x(low).astype(f32)


def hyper_sum(value):
    value = value + to_core(value)
    value = value + to_x(value)
    value = value + to_y(value)
    count = lax.axis_size("fsdp")
    reach = 1
    while reach < count:
        value = value + lax.ppermute(value, "fsdp", [(src, src ^ reach) for src in range(count)])
        reach *= 2
    return value


def fast_body(
    tokens, condition, mod_weight, mod_bias, qkv_weight, qv_bias, attn_weight, attn_bias,
    up_weight, up_bias, down_weight, down_bias, cotangent,
):
    f32, bf16 = jnp.float32, jnp.bfloat16
    latents, tok_count, width = tokens.shape
    count = lax.axis_size("fsdp")
    z, y = lax.axis_index("fsdp"), lax.axis_index("tp")
    place = lax.axis_index("ctx")
    x, core = place // 2, place % 2
    mine, theirs = 2 * x + y, 2 * (1 - x) + y

    small_parts = (condition, qv_bias, attn_bias, up_bias, down_bias)
    small = jnp.concatenate([a.reshape(-1) for a in small_parts])
    small_all = z_order(gather_z(small), z)
    cond_size = condition.size
    cond_all = small_all[:, :cond_size].reshape(count * latents, width)
    bias_all = small_all[:, cond_size:]
    bias_oth = to_y(bias_all)
    marks = [qv_bias.size, qv_bias.size + attn_bias.size, qv_bias.size + attn_bias.size + up_bias.size]

    def qv_plane(b):
        rows = jnp.transpose(b[:, : marks[0]].reshape((count,) + qv_bias.shape), (1, 2, 0, 3)).reshape(2, -1)
        return lax.dynamic_slice_in_dim(rows, core * (rows.shape[1] // 2), rows.shape[1] // 2, 1)

    def up_plane(b):
        rows = jnp.transpose(b[:, marks[1] : marks[2]].reshape((count,) + up_bias.shape), (1, 0, 2)).reshape(-1)
        return lax.dynamic_slice_in_dim(rows, core * (rows.shape[0] // 2), rows.shape[0] // 2, 0)

    qv = jnp.concatenate([qv_plane(bias_all), qv_plane(bias_oth)], axis=1).astype(f32)
    hidden_bias = jnp.concatenate([up_plane(bias_all), up_plane(bias_oth)]).astype(f32)
    attn_bias_full = bias_all[:, marks[0] : marks[1]].reshape(-1).astype(f32)
    down_bias_full = bias_all[:, marks[2] :].reshape(-1).astype(f32)

    act_all = jax.nn.silu(cond_all.astype(f32)).astype(bf16)
    mod_piece = flat_dot(act_all, mod_weight) + mod_bias.astype(f32)
    mod_pair = jnp.stack([mod_piece, to_y(mod_piece)], axis=1)
    mod_pair = jnp.where(y == 0, mod_pair, mod_pair[:, ::-1])
    rows_for = lambda step: lax.dynamic_slice_in_dim(mod_pair, ((z + step) % count) * latents, latents, 0)
    mod_rel = [pick(rows_for(0), mine)] + [pick(to_z(rows_for(step), step), mine) for step in range(1, count)]
    modulation = z_order(mod_rel, z).reshape(6, width)
    shift_attn, scale_attn, gate_attn, shift_mlp, scale_mlp, gate_mlp = [modulation[r] for r in range(6)]

    def enter(source):
        return jnp.concatenate([pick(source, mine), to_x(pick(source, theirs))])

    tok = enter(tokens).astype(f32)
    cot = enter(cotangent).astype(f32)

    half_of = lambda a, axis: lax.dynamic_slice_in_dim(a, core * (a.shape[axis] // 2), a.shape[axis] // 2, axis)
    own_a = jnp.concatenate([half_of(qkv_weight, 2), half_of(attn_weight, 0)[None]])
    a_nat = gather_z(own_a)
    a_oth = [to_y(p) for p in a_nat]
    up_nat = gather_z(half_of(up_weight, 1))
    up_oth = [to_y(p) for p in up_nat]
    down_nat = gather_z(half_of(down_weight, 0))
    down_oth = [to_y(p) for p in down_nat]

    norm_a, inv_a = normalize(tok)
    x_own = (norm_a * (1.0 + scale_attn) + shift_attn).astype(bf16)
    x_oth = to_core(x_own)
    q, k, v, attended, log_norm, ao_own, ao_send = attn_forward(x_own, x_oth, a_nat, a_oth, qv[0], qv[1])
    attn_out = ao_own + to_core(ao_send).astype(f32) + attn_bias_full
    middle = tok + gate_attn * attn_out
    norm_m, inv_m = normalize(middle)
    m_own = (norm_m * (1.0 + scale_mlp) + shift_mlp).astype(bf16)
    m_oth = to_core(m_own)
    g_own = (cot * gate_mlp).astype(bf16)
    g_oth = to_core(g_own)
    (
        mo_own, mo_send, mig_own, mig_send, upg_nat, upg_oth, downg_nat, downg_oth, up_bpart,
    ) = mlp(m_own, m_oth, g_own, g_oth, up_nat, up_oth, down_nat, down_oth, hidden_bias)
    up_half = reduce_pieces(upg_nat, upg_oth)
    down_half = reduce_pieces(downg_nat, downg_oth)
    mlp_out = mo_own + to_core(mo_send).astype(f32) + down_bias_full
    out_rows = (middle + gate_mlp * mlp_out).astype(bf16)
    gate_mlp_grad = jnp.sum(cot * mlp_out, axis=0)
    down_bpart = jnp.sum(g_own.astype(f32), axis=0)
    mig = mig_own + to_core(mig_send).astype(f32)
    middle_grad = cot + normalize_back(mig, norm_m, inv_m, scale_mlp)
    shift_mlp_grad = jnp.sum(mig, axis=0)
    scale_mlp_grad = jnp.sum(mig * norm_m, axis=0)
    gate_attn_grad = jnp.sum(middle_grad * attn_out, axis=0)
    ag_own = (middle_grad * gate_attn).astype(bf16)
    attn_bpart = jnp.sum(ag_own.astype(f32), axis=0)
    ag_oth = to_core(ag_own)
    aig_own, aig_send, ag_nat, ag_othp, qv_bpart = attn_backward(
        ag_own, ag_oth, x_own, x_oth, a_nat, a_oth, q, k, v, attended, log_norm
    )
    a_half = reduce_pieces(ag_nat, ag_othp)
    aig = aig_own + to_core(aig_send).astype(f32)
    tok_grad = middle_grad + normalize_back(aig, norm_a, inv_a, scale_attn)
    shift_attn_grad = jnp.sum(aig, axis=0)
    scale_attn_grad = jnp.sum(aig * norm_a, axis=0)

    def leave(rows):
        own, other = rows[:tok_count], to_x(rows[tok_count:])
        own_y, other_y = to_y(own), to_y(other)
        result = jnp.zeros((latents, tok_count, width), rows.dtype)
        for value, where_x, where_y in ((own, x, y), (other, 1 - x, y), (own_y, x, 1 - y), (other_y, 1 - x, 1 - y)):
            result = lax.dynamic_update_slice(result, value[None], (2 * where_x + where_y, 0, 0))
        return result

    layer_out = leave(out_rows)
    tokens_grad = leave(tok_grad.astype(bf16)).astype(f32)

    mod_own = jnp.stack(
        [shift_attn_grad, scale_attn_grad, gate_attn_grad, shift_mlp_grad, scale_mlp_grad, gate_mlp_grad]
    ).reshape(-1)
    mod_own = (mod_own + to_core(mod_own)).astype(bf16)
    by_x = jnp.stack([mod_own, to_x(mod_own)])
    by_x = jnp.where(x == 0, by_x, by_x[::-1])
    by_y = jnp.stack([by_x, to_y(by_x)], axis=1)
    by_y = jnp.where(y == 0, by_y, by_y[:, ::-1]).reshape(latents, -1)
    mod_grad_all = z_order(gather_z(by_y), z).reshape(count * latents, -1)
    piece = z * 2 + y
    piece_width = mod_weight.shape[1]
    mod_grad_piece = lax.dynamic_slice_in_dim(mod_grad_all, piece * piece_width, piece_width, 1)
    mod_wgrad = dot_tn(act_all, mod_grad_piece)
    mod_bgrad = jnp.sum(mod_grad_piece.astype(f32), axis=0)
    act_part = dot_nt(mod_grad_piece, mod_weight)
    part_for = lambda step: lax.dynamic_slice_in_dim(act_part, ((z + step) % count) * latents, latents, 0)
    act_z = part_for(0)
    for step in range(1, count):
        act_z = act_z + to_z(part_for(step), step)
    own_rows = latents // 2
    act_grad = lax.dynamic_slice_in_dim(act_z, y * own_rows, own_rows, 0) + to_y(
        lax.dynamic_slice_in_dim(act_z, (1 - y) * own_rows, own_rows, 0)
    )
    cond_rows = lax.dynamic_slice_in_dim(cond_all, piece * own_rows, own_rows, 0).astype(f32)
    condition_grad = jax.vjp(jax.nn.silu, cond_rows)[1](act_grad)[0]

    def spread(part, full):
        quarter = part.shape[-1] // 2
        zero = jnp.zeros(part.shape[:-1] + (full,), f32)
        plane = full // 2
        at = [0] * (part.ndim - 1)
        zero = lax.dynamic_update_slice(zero, part[..., :quarter], (*at, y * plane + core * quarter))
        return lax.dynamic_update_slice(zero, part[..., quarter:], (*at, (1 - y) * plane + core * quarter))

    qv_spread = spread(qv_bpart, width)
    up_spread = spread(up_bpart, up_bpart.shape[0] * 2)
    packed = hyper_sum(jnp.concatenate([qv_spread.reshape(-1), up_spread, attn_bpart, down_bpart]))
    qv_sum = packed[: 2 * width].reshape(2, width // 128, 128)
    up_sum = packed[2 * width : 2 * width + up_spread.shape[0]].reshape(-1, 128)
    rest = packed[2 * width + up_spread.shape[0] :].reshape(2, width)
    lanes = 128 // count
    qv_bgrad = lax.dynamic_slice(qv_sum, (0, y * qv_bias.shape[1], z * lanes), qv_bias.shape)
    up_bgrad = lax.dynamic_slice(up_sum, (y * up_bias.shape[0], z * lanes), up_bias.shape)
    attn_bgrad = lax.dynamic_slice_in_dim(rest[0], z * (width // count), width // count, 0)
    down_bgrad = lax.dynamic_slice_in_dim(rest[1], z * (width // count), width // count, 0)

    def both(part, axis):
        other = to_core(part)
        first = jnp.where(core == 0, part, other)
        second = jnp.where(core == 0, other, part)
        return jnp.concatenate([first, second], axis=axis)

    qkv_wgrad = both(a_half[:3], 2)
    attn_wgrad = both(a_half[3], 0)
    up_wgrad = both(up_half, 1)
    down_wgrad = both(down_half, 0)
    return (
        layer_out, tokens_grad, condition_grad, mod_wgrad, mod_bgrad, qkv_wgrad, qv_bgrad,
        attn_wgrad, attn_bgrad, up_wgrad, up_bgrad, down_wgrad, down_bgrad,
    )


def solution(mesh):
    placed = (
        P("fsdp", "ctx", None),
        P("fsdp", None),
        P(None, ("fsdp", "tp")),
        P(("fsdp", "tp")),
        P(None, "fsdp", "tp"),
        P(None, "tp", "fsdp"),
        P("tp", "fsdp"),
        P("fsdp"),
        P("fsdp", "tp"),
        P("tp", "fsdp"),
        P("tp", "fsdp"),
        P("fsdp"),
        P("fsdp", "ctx", None),
    )
    shape = dict(mesh.shape)
    chip_per_latent = shape["ctx"] == 4 and shape["tp"] == 2 and shape["fsdp"] == 4
    return jax.shard_map(
        fast_body if chip_per_latent else body,
        mesh=mesh,
        in_specs=placed,
        out_specs=(
            P("fsdp", "ctx", None),
            P("fsdp", "ctx", None),
            P(("fsdp", "tp"), None),
            P(None, ("fsdp", "tp")),
            P(("fsdp", "tp")),
            P(None, "fsdp", "tp"),
            P(None, "tp", "fsdp"),
            P("tp", "fsdp"),
            P("fsdp"),
            P("fsdp", "tp"),
            P("tp", "fsdp"),
            P("tp", "fsdp"),
            P("fsdp"),
        ),
        check_vma=False,
    )
```

```python
import functools
import math

import jax
import jax.numpy as jnp
from jax import lax
from jax.experimental import pallas as pl
from jax.experimental.pallas import tpu as pltpu
from jax.sharding import PartitionSpec as P


def modulate(tok_rows, shift_row, scale_row):
    centre = tok_rows - jnp.mean(tok_rows, axis=-1, keepdims=True)
    spread = jnp.mean(centre * centre, axis=-1, keepdims=True)
    normed = centre * lax.rsqrt(spread + 1e-06)
    return normed * (1.0 + scale_row[:, None, :]) + shift_row[:, None, :]


def gelu_tanh(pre_act):
    return jax.nn.gelu(pre_act, approximate=True)


def flat_dot(left, right):
    return jnp.dot(left, right, preferred_element_type=jnp.float32)


def head_slice(source, latent, head_pair):
    row_count = source.shape[1]
    picked = lax.dynamic_slice(source, (latent, 0, head_pair * 128), (1, row_count, 128))
    return picked[0].reshape(row_count, 2, 64)


def tokens_major(stacked, latents, head_pairs):
    row_count = stacked.shape[-2]
    grouped = stacked.reshape(latents, head_pairs, row_count, 128)
    return jnp.transpose(grouped, (0, 2, 1, 3)).reshape(latents, row_count, head_pairs * 128)


def attend(queries, keys_all, values_all, head_pairs):

    def attend_per_block(block_index):
        latent = block_index // head_pairs
        head_pair = block_index % head_pairs
        query_h = head_slice(queries, latent, head_pair)
        key_h = head_slice(keys_all, latent, head_pair)
        value_h = head_slice(values_all, latent, head_pair)
        scores = (
            jnp.einsum("qhd,khd->hqk", query_h, key_h, preferred_element_type=jnp.float32) * 0.125
        )
        row_max = jnp.max(scores, axis=-1, keepdims=True)
        weights = jnp.exp(scores - row_max)
        row_total = jnp.sum(weights, axis=-1, keepdims=True)
        probs_low = (weights / row_total).astype(jnp.bfloat16)
        attended = jnp.einsum(
            "hqk,khd->qhd", probs_low, value_h, preferred_element_type=jnp.float32
        )
        return (attended.reshape(query_h.shape[0], 128), (row_max + jnp.log(row_total))[..., 0])

    return lax.map(attend_per_block, jnp.arange(queries.shape[0] * head_pairs))


def query_side(queries, keys_all, values_all, grad_rows, log_norm, head_pairs):

    def query_per_block(packed):
        block_index, norm_block = packed
        latent = block_index // head_pairs
        head_pair = block_index % head_pairs
        query_h = head_slice(queries, latent, head_pair)
        key_h = head_slice(keys_all, latent, head_pair)
        value_h = head_slice(values_all, latent, head_pair)
        grad_h = head_slice(grad_rows, latent, head_pair)
        scores = (
            jnp.einsum("qhd,khd->hqk", query_h, key_h, preferred_element_type=jnp.float32) * 0.125
        )
        probs = jnp.exp(scores - norm_block[..., None])
        dprobs = jnp.einsum("qhd,khd->hqk", grad_h, value_h, preferred_element_type=jnp.float32)
        row_delta = jnp.sum(probs * dprobs, axis=-1, keepdims=True)
        score_grad = (probs * (dprobs - row_delta)).astype(jnp.bfloat16)
        query_grad = (
            jnp.einsum("hqk,khd->qhd", score_grad, key_h, preferred_element_type=jnp.float32)
            * 0.125
        )
        query_count = query_h.shape[0]
        key_grad = (
            jnp.einsum("hqk,qhd->khd", score_grad, query_h, preferred_element_type=jnp.float32)
            * 0.125
        )
        value_grad = jnp.einsum(
            "hqk,qhd->khd", probs.astype(jnp.bfloat16), grad_h, preferred_element_type=jnp.float32
        )
        return (
            query_grad.reshape(query_count, 128),
            key_grad.reshape(-1, 128),
            value_grad.reshape(-1, 128),
        )

    return lax.map(query_per_block, (jnp.arange(queries.shape[0] * head_pairs), log_norm))


def body(
    tokens,
    condition,
    mod_weight,
    mod_bias,
    qkv_weight,
    qv_bias,
    attn_weight,
    attn_bias,
    up_weight,
    up_bias,
    down_weight,
    down_bias,
    cotangent,
):
    latents, tok_count, width = tokens.shape
    gathered = (
        lax.all_gather(condition, "fsdp", axis=0, tiled=True),
        lax.all_gather(qkv_weight, "fsdp", axis=1, tiled=True),
        lax.all_gather(qv_bias, "fsdp", axis=2, tiled=True),
        lax.all_gather(attn_weight, "fsdp", axis=1, tiled=True),
        lax.all_gather(attn_bias, "fsdp", axis=0, tiled=True),
        lax.all_gather(up_weight, "fsdp", axis=0, tiled=True),
        lax.all_gather(up_bias, "fsdp", axis=1, tiled=True),
        lax.all_gather(down_weight, "fsdp", axis=1, tiled=True),
        lax.all_gather(down_bias, "fsdp", axis=0, tiled=True),
    )
    (
        cond_all,
        qkv_full,
        qv_full,
        attn_full,
        attn_bias_full,
        up_full,
        up_bias_full,
        down_full,
        down_bias_full,
    ) = gathered
    q_bias = qv_full[0].reshape(-1).astype(jnp.float32)
    v_bias = qv_full[1].reshape(-1).astype(jnp.float32)
    hidden_bias = up_bias_full.reshape(-1).astype(jnp.float32)
    act_all = jax.nn.silu(cond_all.astype(jnp.float32)).astype(jnp.bfloat16)
    mod_piece = flat_dot(act_all, mod_weight) + mod_bias.astype(jnp.float32)
    mod_full = lax.all_gather(mod_piece, ("fsdp", "tp"), axis=1, tiled=True)
    first_latent = lax.axis_index("fsdp") * latents
    modulation = lax.dynamic_slice_in_dim(mod_full, first_latent, latents, 0).reshape(
        latents, 6, width
    )
    shift_attn, scale_attn, gate_attn = (modulation[:, 0], modulation[:, 1], modulation[:, 2])
    shift_mlp, scale_mlp, gate_mlp = (modulation[:, 3], modulation[:, 4], modulation[:, 5])
    tok_float = tokens.astype(jnp.float32)
    attn_input_f, norm_pull_attn = jax.vjp(modulate, tok_float, shift_attn, scale_attn)
    attn_input = attn_input_f.astype(jnp.bfloat16).reshape(-1, width)
    queries = (
        (flat_dot(attn_input, qkv_full[0]) + q_bias)
        .astype(jnp.bfloat16)
        .reshape(latents, tok_count, -1)
    )
    keys_own = (
        flat_dot(attn_input, qkv_full[1]).astype(jnp.bfloat16).reshape(latents, tok_count, -1)
    )
    values_own = (
        (flat_dot(attn_input, qkv_full[2]) + v_bias)
        .astype(jnp.bfloat16)
        .reshape(latents, tok_count, -1)
    )
    keys_all, values_all = (
        lax.all_gather(keys_own, "ctx", axis=1, tiled=True),
        lax.all_gather(values_own, "ctx", axis=1, tiled=True),
    )
    head_width = queries.shape[-1]
    head_pairs = head_width // 128
    attended_st, log_norm = attend(queries, keys_all, values_all, head_pairs)
    attended = (
        tokens_major(attended_st, latents, head_pairs).astype(jnp.bfloat16).reshape(-1, head_width)
    )
    attn_out = lax.psum(flat_dot(attended, attn_full), "tp") + attn_bias_full.astype(jnp.float32)
    attn_out = attn_out.reshape(latents, tok_count, width)
    middle = tok_float + gate_attn[:, None, :] * attn_out
    mlp_input_f, norm_pull_mlp = jax.vjp(modulate, middle, shift_mlp, scale_mlp)
    mlp_input = mlp_input_f.astype(jnp.bfloat16).reshape(-1, width)
    up_pre = flat_dot(mlp_input, up_full) + hidden_bias
    up_act_f, gelu_pull = jax.vjp(gelu_tanh, up_pre)
    up_act = up_act_f.astype(jnp.bfloat16)
    mlp_out = lax.psum(flat_dot(up_act, down_full), "tp") + down_bias_full.astype(jnp.float32)
    mlp_out = mlp_out.reshape(latents, tok_count, width)
    layer_out = (middle + gate_mlp[:, None, :] * mlp_out).astype(jnp.bfloat16)
    out_grad = cotangent.astype(jnp.float32)
    gate_mlp_grad = jnp.sum(out_grad * mlp_out, axis=1)
    mlp_grad = (out_grad * gate_mlp[:, None, :]).astype(jnp.bfloat16).reshape(-1, width)
    down_bgrad_part = jnp.sum(mlp_grad.astype(jnp.float32), axis=0)
    down_wgrad_part = flat_dot(up_act.T, mlp_grad)
    up_grad = gelu_pull(flat_dot(mlp_grad, down_full.T))[0].astype(jnp.bfloat16)
    up_bgrad_part = jnp.sum(up_grad.astype(jnp.float32), axis=0)
    up_wgrad_part = flat_dot(mlp_input.T, up_grad)
    mlp_input_grad = lax.psum(flat_dot(up_grad, up_full.T), "tp").reshape(latents, tok_count, width)
    middle_part, shift_mlp_grad, scale_mlp_grad = norm_pull_mlp(mlp_input_grad)
    middle_grad = out_grad + middle_part
    gate_attn_grad = jnp.sum(middle_grad * attn_out, axis=1)
    attn_grad = (middle_grad * gate_attn[:, None, :]).astype(jnp.bfloat16).reshape(-1, width)
    attn_bgrad_part = jnp.sum(attn_grad.astype(jnp.float32), axis=0)
    attn_wgrad_part = flat_dot(attended.T, attn_grad)
    attended_grad = (
        flat_dot(attn_grad, attn_full.T)
        .astype(jnp.bfloat16)
        .reshape(latents, tok_count, head_width)
    )
    query_st, key_st, value_st = query_side(
        queries, keys_all, values_all, attended_grad, log_norm, head_pairs
    )
    key_parts = key_st.reshape(latents, head_pairs, -1, 128)
    value_parts = value_st.reshape(latents, head_pairs, -1, 128)
    key_sum, value_sum = (
        lax.psum_scatter(key_parts, "ctx", scatter_dimension=2, tiled=True),
        lax.psum_scatter(value_parts, "ctx", scatter_dimension=2, tiled=True),
    )
    key_grad = tokens_major(
        key_sum.reshape(latents * head_pairs, tok_count, 128), latents, head_pairs
    )
    value_grad = tokens_major(
        value_sum.reshape(latents * head_pairs, tok_count, 128), latents, head_pairs
    )
    query_flat = (
        tokens_major(query_st, latents, head_pairs).astype(jnp.bfloat16).reshape(-1, head_width)
    )
    key_flat = key_grad.astype(jnp.bfloat16).reshape(-1, head_width)
    value_flat = value_grad.astype(jnp.bfloat16).reshape(-1, head_width)
    input_terms = (
        flat_dot(query_flat, qkv_full[0].T)
        + flat_dot(key_flat, qkv_full[1].T)
        + flat_dot(value_flat, qkv_full[2].T)
    )
    attn_input_grad = lax.psum(input_terms, "tp").reshape(latents, tok_count, width)
    qkv_wgrad_part = jnp.stack(
        [
            flat_dot(attn_input.T, query_flat),
            flat_dot(attn_input.T, key_flat),
            flat_dot(attn_input.T, value_flat),
        ]
    )
    qv_bgrad_part = jnp.stack(
        [
            jnp.sum(query_flat.astype(jnp.float32), axis=0),
            jnp.sum(value_flat.astype(jnp.float32), axis=0),
        ]
    ).reshape(2, -1, 128)
    token_part, shift_attn_grad, scale_attn_grad = norm_pull_attn(attn_input_grad)
    tokens_grad = middle_grad + token_part
    mod_grad_own = jnp.stack(
        [
            shift_attn_grad,
            scale_attn_grad,
            gate_attn_grad,
            shift_mlp_grad,
            scale_mlp_grad,
            gate_mlp_grad,
        ],
        axis=1,
    ).reshape(latents, -1)
    mod_grad_slab = lax.dynamic_update_slice_in_dim(
        jnp.zeros(mod_full.shape, jnp.float32), mod_grad_own, first_latent, 0
    )
    mod_grad_all = lax.psum(mod_grad_slab, ("fsdp", "ctx")).astype(jnp.bfloat16)
    piece = lax.axis_index("fsdp") * lax.axis_size("tp") + lax.axis_index("tp")
    piece_width = mod_weight.shape[1]
    mod_grad_piece = lax.dynamic_slice_in_dim(mod_grad_all, piece * piece_width, piece_width, 1)
    mod_wgrad = flat_dot(act_all.T, mod_grad_piece)
    mod_bgrad = jnp.sum(mod_grad_piece.astype(jnp.float32), axis=0)
    own_rows = mod_full.shape[0] // (lax.axis_size("fsdp") * lax.axis_size("tp"))
    act_grad = lax.psum_scatter(
        flat_dot(mod_grad_piece, mod_weight.T), ("fsdp", "tp"), scatter_dimension=0, tiled=True
    )
    cond_rows = lax.dynamic_slice_in_dim(cond_all, piece * own_rows, own_rows, 0).astype(
        jnp.float32
    )
    condition_grad = jax.vjp(jax.nn.silu, cond_rows)[1](act_grad)[0]
    partials = (
        qkv_wgrad_part,
        qv_bgrad_part,
        attn_wgrad_part,
        attn_bgrad_part,
        up_wgrad_part,
        up_bgrad_part.reshape(-1, 128),
        down_wgrad_part,
        down_bgrad_part,
    )
    shards = (
        lax.psum_scatter(partials[0], "fsdp", scatter_dimension=1, tiled=True),
        lax.psum_scatter(partials[1], "fsdp", scatter_dimension=2, tiled=True),
        lax.psum_scatter(partials[2], "fsdp", scatter_dimension=1, tiled=True),
        lax.psum_scatter(partials[3], "fsdp", scatter_dimension=0, tiled=True),
        lax.psum_scatter(partials[4], "fsdp", scatter_dimension=0, tiled=True),
        lax.psum_scatter(partials[5], "fsdp", scatter_dimension=1, tiled=True),
        lax.psum_scatter(partials[6], "fsdp", scatter_dimension=1, tiled=True),
        lax.psum_scatter(partials[7], "fsdp", scatter_dimension=0, tiled=True),
    )
    reduced = lax.psum(
        (shards[0], shards[1], shards[2], shards[3], shards[4], shards[5], shards[6], shards[7]),
        "ctx",
    )
    qkv_wgrad, qv_bgrad, attn_wgrad, attn_bgrad, up_wgrad, up_bgrad, down_wgrad, down_bgrad = (
        reduced
    )
    return (
        layer_out,
        tokens_grad,
        condition_grad,
        mod_wgrad,
        mod_bgrad,
        qkv_wgrad,
        qv_bgrad,
        attn_wgrad,
        attn_bgrad,
        up_wgrad,
        up_bgrad,
        down_wgrad,
        down_bgrad,
    )


X_SWAP = [(0, 2), (2, 0), (1, 3), (3, 1)]
CORE_SWAP = [(0, 1), (1, 0), (2, 3), (3, 2)]
Y_SWAP = [(0, 1), (1, 0)]


def to_x(value):
    return lax.ppermute(value, "ctx", X_SWAP)


def to_core(value):
    return lax.ppermute(value, "ctx", CORE_SWAP)


def to_y(value):
    return lax.ppermute(value, "tp", Y_SWAP)


def to_z(value, step):
    count = lax.axis_size("fsdp")
    return lax.ppermute(value, "fsdp", [(src, (src + step) % count) for src in range(count)])


def z_order(relative, z):
    count = len(relative)
    back = list(relative[::-1])
    doubled = jnp.stack(back + back[:-1])
    return lax.dynamic_slice_in_dim(doubled, count - 1 - z, count, 0)


def pick(stacked, index):
    return lax.dynamic_index_in_dim(stacked, index, 0, keepdims=False)


def gather_z(value):
    count = lax.axis_size("fsdp")
    return [value] + [to_z(value, step) for step in range(1, count)]


def normalize(rows):
    centre = rows - jnp.mean(rows, axis=-1, keepdims=True)
    spread = jnp.mean(centre * centre, axis=-1, keepdims=True)
    inverse = lax.rsqrt(spread + 1e-06)
    return centre * inverse, inverse


def normalize_back(grad, normed, inverse, scale):
    e = grad * (1.0 + scale)
    mean_e = jnp.mean(e, axis=-1, keepdims=True)
    mean_en = jnp.mean(e * normed, axis=-1, keepdims=True)
    return (e - mean_e - normed * mean_en) * inverse


def dot_nt(left, right):
    return lax.dot_general(left, right, (((1,), (1,)), ((), ())), preferred_element_type=jnp.float32)


def dot_tn(left, right):
    return lax.dot_general(left, right, (((0,), (0,)), ((), ())), preferred_element_type=jnp.float32)


MESH = pl.DeviceIdType.MESH
ANYWHERE = pl.BlockSpec(memory_space=pl.ANY)
VMEM_BYTES = 64 * 1024 * 1024 - 4 * 65536


def nt(left, right):
    return lax.dot_general(left, right, (((1,), (1,)), ((), ())), preferred_element_type=jnp.float32)


def nn(left, right):
    return lax.dot_general(left, right, (((1,), (0,)), ((), ())), preferred_element_type=jnp.float32)


def block_of(index, size):
    return pl.ds(pl.multiple_of(index * size, size), size)


def shard_of(z, step, count):
    return lax.rem(z - step + count, count)


def shard_for(z, step, count):
    return lax.rem(z + step, count)


def attn_copies(plane, pieces, wqkv, wout, sems):
    count = len(pieces)
    z = lax.axis_index("fsdp")
    result = []
    for step, piece in enumerate(pieces):
        rows = piece.shape[1]
        at = block_of(shard_of(z, step, count), rows)
        result.append(pltpu.make_async_copy(piece.at[pl.ds(0, 3)], wqkv.at[plane, :, at, :], sems.at[plane, step, 0]))
        result.append(pltpu.make_async_copy(piece.at[3], wout.at[plane, :, at], sems.at[plane, step, 1]))
    return result


def row_copies(refs, target, sems):
    half = refs[0].shape[0]
    return [
        pltpu.make_async_copy(ref, target.at[pl.ds(i * half, half)], sems.at[i]) for i, ref in enumerate(refs)
    ]


def head_mask(rows, head):
    lane = lax.broadcasted_iota(jnp.int32, (rows, 128), 1)
    return (lane >= 64 * head) & (lane < 64 * head + 64)


class Gather:
    def __init__(self, own, full, z_send, z_recv, y_send, y_recv, x_send, x_recv):
        self.own, self.full = own, full
        self.sems = (z_send, z_recv, y_send, y_recv, x_send, x_recv)
        self.count = full.shape[1]
        self.z = lax.axis_index("fsdp")
        self.x = lax.axis_index("ctx") // 2

    def shard(self, index):
        if index == 0:
            return self.z
        if index < self.count:
            return self.z - index
        return self.z + index - self.count + 1

    def present(self, index):
        at = self.shard(index)
        return (at >= 0) & (at < self.count)

    def safe(self, index):
        return lax.rem(self.shard(index) + self.count, self.count)

    def source(self, index):
        return self.own if index == 0 else self.full.at[0, self.safe(index)]

    def half(self, ref):
        rows = ref.shape[0] // 2
        return ref.at[block_of(self.x, rows)]

    def along_z(self, index, side):
        slot = index if side == 0 or index == 0 else index - self.count + 1
        target = self.z + 1 if side == 0 else self.z - 1
        return pltpu.make_async_remote_copy(
            src_ref=self.source(index),
            dst_ref=self.full.at[0, self.safe(index)],
            send_sem=self.sems[0].at[side, slot],
            recv_sem=self.sems[1].at[side, slot],
            device_id={"fsdp": target},
            device_id_type=MESH,
        )

    def can_go(self, index, side):
        ok = self.z < self.count - 1 if side == 0 else self.z > 0
        return ok & self.present(index)

    def came_z(self, index):
        side = 0 if index < self.count else 1
        slot = index - 1 if side == 0 else index - self.count
        into = self.full.at[0, self.safe(index)]
        return pltpu.make_async_remote_copy(
            src_ref=into,
            dst_ref=into,
            send_sem=self.sems[0].at[side, slot],
            recv_sem=self.sems[1].at[side, slot],
            device_id={"fsdp": self.z},
            device_id_type=MESH,
        )

    def along_y(self, index):
        return pltpu.make_async_remote_copy(
            src_ref=self.half(self.source(index)),
            dst_ref=self.half(self.full.at[1, self.safe(index)]),
            send_sem=self.sems[2].at[index],
            recv_sem=self.sems[3].at[index],
            device_id={"tp": 1 - lax.axis_index("tp")},
            device_id_type=MESH,
        )

    def along_x(self, index):
        part = self.half(self.full.at[1, self.safe(index)])
        return pltpu.make_async_remote_copy(
            src_ref=part,
            dst_ref=part,
            send_sem=self.sems[4].at[index],
            recv_sem=self.sems[5].at[index],
            device_id={"ctx": lax.rem(lax.axis_index("ctx") + 2, 4)},
            device_id_type=MESH,
        )

    def came_x(self, index):
        rows = self.full.shape[2] // 2
        part = self.full.at[1, self.safe(index), block_of(1 - self.x, rows)]
        return pltpu.make_async_remote_copy(
            src_ref=part,
            dst_ref=part,
            send_sem=self.sems[4].at[index],
            recv_sem=self.sems[5].at[index],
            device_id={"ctx": lax.rem(lax.axis_index("ctx") + 2, 4)},
            device_id_type=MESH,
        )

    def indices(self):
        order = [0]
        for away in range(1, self.count):
            order += [away, self.count + away - 1]
        return order

    def begin(self):
        for side in range(2):

            @pl.when(self.can_go(0, side))
            def _():
                self.along_z(0, side).start()

        self.along_y(0).start()

    def relay_z(self, away):
        for side, index in ((0, away), (1, self.count + away - 1)):

            @pl.when(self.present(index))
            def _():
                self.came_z(index).wait_recv()

                if away < self.count - 1:

                    @pl.when(self.can_go(index, side))
                    def _():
                        self.along_z(index, side).start()

                self.along_y(index).start()

    def relay_x(self, away):
        for index in [0] if away == 0 else [away, self.count + away - 1]:

            @pl.when(self.present(index))
            def _():
                self.along_y(index).wait_recv()
                self.along_x(index).start()

    def end(self):
        for index in self.indices():

            @pl.when(self.present(index))
            def _():
                self.came_x(index).wait_recv()
                self.along_y(index).wait_send()
                self.along_x(index).wait_send()

            for side in range(2):
                if index == 0 or ((index < self.count) == (side == 0) and index not in (self.count - 1, 2 * self.count - 2)):

                    @pl.when(self.can_go(index, side))
                    def _():
                        self.along_z(index, side).wait_send()


def greet(z_all):
    barrier = pltpu.get_barrier_semaphore()
    z, count = lax.axis_index("fsdp"), lax.axis_size("fsdp")
    pl.semaphore_signal(barrier, inc=1, device_id={"tp": 1 - lax.axis_index("tp")}, device_id_type=MESH)
    pl.semaphore_signal(barrier, inc=1, device_id={"ctx": lax.rem(lax.axis_index("ctx") + 2, 4)}, device_id_type=MESH)
    for step in range(1, count):
        pl.semaphore_signal(barrier, inc=1, device_id={"fsdp": lax.rem(z + step, count)}, device_id_type=MESH)
    pl.semaphore_wait(barrier, count + 1)


def attn_forward_kernel(count, block, *refs):
    x_own, x_oth = refs[:2]
    pieces = refs[2 : 2 + count]
    up_half, down_half, qb, vb = refs[2 + count : 6 + count]
    q_ref, k_ref, v_ref, att_ref, lse_ref, out_own, out_send, a_oth, up_full, down_full = refs[6 + count : 16 + count]
    xs, wqkv, wout, vt, acc, w_sem, x_sem, o_sem, a_sem, g_z, g_y = refs[16 + count :]
    plane = pl.program_id(0)
    rows = xs.shape[0]
    half = rows // 2
    f32, bf16 = jnp.float32, jnp.bfloat16
    z = lax.axis_index("fsdp")
    xpos = lax.axis_index("ctx") // 2
    depth = pieces[0].shape[1] // 2
    gathers = [
        Gather(own, full, *[g_z.at[i, j] for j in range(2)], *[g_y.at[i, j] for j in range(4)])
        for i, (own, full) in enumerate(((up_half, up_full), (down_half, down_full)))
    ]
    x_peer = lax.rem(lax.axis_index("ctx") + 2, 4)

    def a_by_y(step):
        at = shard_of(z, step, count)
        return pltpu.make_async_remote_copy(
            src_ref=pieces[step].at[:, block_of(xpos, depth)],
            dst_ref=a_oth.at[at, :, block_of(xpos, depth)],
            send_sem=a_sem.at[0, step],
            recv_sem=a_sem.at[1, step],
            device_id={"tp": 1 - lax.axis_index("tp")},
            device_id_type=MESH,
        )

    def a_by_x(step, side):
        part = a_oth.at[shard_of(z, step, count), :, block_of(side, depth)]
        return pltpu.make_async_remote_copy(
            src_ref=part,
            dst_ref=part,
            send_sem=a_sem.at[2, step],
            recv_sem=a_sem.at[3, step],
            device_id={"ctx": x_peer},
            device_id_type=MESH,
        )

    def native_copies():
        return attn_copies(0, pieces, wqkv, wout, w_sem)

    def other_copies():
        return attn_copies(1, [a_oth.at[shard_of(z, step, count)] for step in range(count)], wqkv, wout, w_sem)

    @pl.when(plane == 0)
    def _():
        inputs = row_copies((x_own, x_oth), xs, x_sem)
        for copy in inputs + native_copies():
            copy.start()
        greet(True)
        for step in range(count):
            a_by_y(step).start()
        for gather in gathers:
            gather.begin()
        for copy in inputs + native_copies():
            copy.wait()

    @pl.when(plane == 1)
    def _():
        for step in range(count):
            a_by_x(step, 1 - xpos).wait_recv()
        for copy in other_copies():
            copy.start()
        for copy in other_copies():
            copy.wait()

    def slot(first, second):
        for p, actions in enumerate((first, second)):
            if actions:

                @pl.when(plane == p)
                def _():
                    for action in actions:
                        action()

    def pass_a(step):
        def act():
            a_by_y(step).wait_recv()
            a_by_x(step, xpos).start()

        return act

    def project(b, _):
        at = block_of(b, block)
        xb = xs[at, :]
        q_ref[0, at, :] = (nn(xb, wqkv[plane, 0]) + qb[...]).astype(bf16)
        k_ref[0, at, :] = nn(xb, wqkv[plane, 1]).astype(bf16)
        value = (nn(xb, wqkv[plane, 2]) + vb[...]).astype(bf16)
        v_ref[0, at, :] = value
        vt[:, at] = value.T
        return 0

    lax.fori_loop(0, rows // block, project, 0)
    up, down = gathers
    relay_z = lambda gather, away: (lambda: gather.relay_z(away)) if away < count else (lambda: None)
    relay_x = lambda gather, away: (lambda: gather.relay_x(away)) if away < count else (lambda: None)
    slot([pass_a(0)], [relay_x(up, 0)])

    for pair in range(2):
        lanes = slice(128 * pair, 128 * pair + 128)

        def attend(b, _):
            at = block_of(b, block)
            qp = q_ref[0, at, lanes] * jnp.bfloat16(0.125)
            keys = k_ref[0, :, lanes]
            tops = []
            for head in range(2):
                scores = nt(keys, jnp.where(head_mask(block, head), qp, jnp.bfloat16(0)))
                top = jnp.max(scores, axis=0, keepdims=True)
                weights = jnp.exp(scores - top)
                total = jnp.sum(weights, axis=0, keepdims=True)
                probs = (weights * (1.0 / total)).astype(bf16)
                low = 128 * pair + 64 * head
                tops.append(nn(vt[low : low + 64, :], probs))
                lse_ref[0, 2 * pair + head : 2 * pair + head + 1, at] = top + jnp.log(total)
            att_ref[0, at, lanes] = jnp.concatenate(tops, axis=0).T.astype(bf16)
            return 0

        lax.fori_loop(0, rows // block, attend, 0)
        if pair == 0:
            slot([pass_a(step) for step in range(1, count - 1)], [relay_z(up, 2), relay_x(down, 0), relay_x(up, 1)])
        else:
            slot([relay_z(up, 1), pass_a(count - 1)], [relay_z(down, 2), relay_x(down, 1)])

    def finish(b, _):
        at = block_of(b, block)
        term = nn(att_ref[0, at, :], wout[plane])

        @pl.when(plane == 0)
        def _():
            acc[at, :] = term

        @pl.when(plane == 1)
        def _():
            acc[at, :] = acc[at, :] + term

        return 0

    lax.fori_loop(0, rows // block, finish, 0)
    slot([relay_z(down, 1)], [])

    @pl.when(plane == 1)
    def _():
        for i, ref in enumerate((out_own, out_send)):
            pltpu.make_async_copy(acc.at[pl.ds(i * half, half)], ref, o_sem.at[i]).start()
        for away in range(3, count):
            for gather in gathers:
                gather.relay_z(away)
        for away in range(2, count):
            for gather in gathers:
                gather.relay_x(away)
        for gather in gathers:
            gather.end()
        for step in range(count):
            a_by_y(step).wait_send()
            a_by_x(step, xpos).wait_send()
        for i, ref in enumerate((out_own, out_send)):
            pltpu.make_async_copy(acc.at[pl.ds(i * half, half)], ref, o_sem.at[i]).wait()


def attn_forward(x_own, x_oth, nat, up_half, down_half, q_bias, v_bias):
    count = len(nat)
    half, width = x_own.shape
    rows = 2 * half
    wide = nat[0].shape[2]
    bf16, f32 = jnp.bfloat16, jnp.float32
    by_plane = lambda *shape: pl.BlockSpec((1,) + shape, lambda p: (p,) + (0,) * len(shape))
    biases = [b.reshape(2, 1, wide) for b in (q_bias, v_bias)]
    squeezed = pl.BlockSpec((None, 1, wide), lambda p: (p, 0, 0))
    shape = lambda s, d: jax.ShapeDtypeStruct(s, d)
    flops = 2 * rows * width * wide * 2 * 4 + 8 * 2 * rows * rows * 64 * 2
    return pl.pallas_call(
        functools.partial(attn_forward_kernel, count, min(256, half)),
        grid=(2,),
        in_specs=[ANYWHERE] * (4 + count) + [squeezed] * 2,
        out_specs=[by_plane(rows, wide)] * 4 + [by_plane(4, rows)] + [ANYWHERE] * 5,
        out_shape=[shape((2, rows, wide), bf16)] * 4
        + [shape((2, 4, rows), f32)]
        + [shape((half, width), f32)] * 2
        + [shape((count,) + nat[0].shape, bf16)]
        + [shape((2, count) + w.shape, bf16) for w in (up_half, down_half)],
        scratch_shapes=[
            pltpu.VMEM((rows, width), bf16),
            pltpu.VMEM((2, 3, width, wide), bf16),
            pltpu.VMEM((2, wide, width), bf16),
            pltpu.VMEM((wide, rows), bf16),
            pltpu.VMEM((rows, width), f32),
            pltpu.SemaphoreType.DMA((2, count, 2)),
            pltpu.SemaphoreType.DMA((2,)),
            pltpu.SemaphoreType.DMA((2,)),
            pltpu.SemaphoreType.DMA((4, count)),
            pltpu.SemaphoreType.DMA((2, 2, 2, count)),
            pltpu.SemaphoreType.DMA((2, 4, 2 * count - 1)),
        ],
        compiler_params=pltpu.CompilerParams(
            dimension_semantics=("arbitrary",), vmem_limit_bytes=VMEM_BYTES, collective_id=0, has_side_effects=True
        ),
        cost_estimate=pl.CostEstimate(flops=flops, bytes_accessed=18 << 20, transcendentals=8 * rows * rows),
        name="attn_forward",
    )(x_own, x_oth, *nat, up_half, down_half, *biases)


def attn_backward_kernel(count, block, *refs):
    g_own, g_oth, x_own, x_oth = refs[:4]
    z = lax.axis_index("fsdp")
    a_oth = refs[4 + count]
    pieces = (refs[4 : 4 + count], [a_oth.at[shard_of(z, step, count)] for step in range(count)])
    refs = refs[5 + count :]
    q_ref, k_ref, v_ref, att_ref, lse_ref = refs[:5]
    back_own, back_send = refs[5:7]
    grads = (refs[7 : 7 + count], refs[7 + count : 7 + 2 * count])
    bias_ref = refs[7 + 2 * count]
    (gs, xs, xt, attt, wqkv, wout, d_att, dq, dk, dv, kt, dk_acc, dv_acc, acc, wg, awg, w_sem, x_sem, o_sem, g_sem) = refs[
        8 + 2 * count :
    ]
    plane = pl.program_id(0)
    rows = xs.shape[0]
    half = rows // 2
    f32, bf16 = jnp.float32, jnp.bfloat16
    blocks = rows // block

    @pl.when(plane == 0)
    def _():
        inputs = row_copies((g_own, g_oth), gs, x_sem.at[0]) + row_copies((x_own, x_oth), xs, x_sem.at[1])
        for copy in inputs:
            copy.start()
        for p in range(2):
            for copy in attn_copies(p, pieces[p], wqkv, wout, w_sem):
                copy.start()
        for copy in inputs:
            copy.wait()

        def flip(b, _):
            at = block_of(b, block)
            xt[:, at] = xs[at, :].T
            return 0

        lax.fori_loop(0, blocks, flip, 0)

    for p in range(2):

        @pl.when(plane == p)
        def _():
            for copy in attn_copies(p, pieces[p], wqkv, wout, w_sem):
                copy.wait()

    def enter(b, _):
        at = block_of(b, block)
        d_att[at, :] = nt(gs[at, :], wout[plane]).astype(bf16)
        attt[:, at] = att_ref[0, at, :].T
        kt[:, at] = k_ref[0, at, :].T
        return 0

    lax.fori_loop(0, blocks, enter, 0)

    for pair in range(2):
        lanes = slice(128 * pair, 128 * pair + 128)
        dk_acc[...] = jnp.zeros_like(dk_acc)
        dv_acc[...] = jnp.zeros_like(dv_acc)

        def step(b, _):
            at = block_of(b, block)
            qp = q_ref[0, at, lanes] * jnp.bfloat16(0.125)
            dp = d_att[at, lanes]
            keys = k_ref[0, :, lanes]
            values = v_ref[0, :, lanes]
            tops, p_all, s_all, q_all, d_all = [], [], [], [], []
            for head in range(2):
                mask = head_mask(block, head)
                qm = jnp.where(mask, qp, jnp.bfloat16(0))
                dm = jnp.where(mask, dp, jnp.bfloat16(0))
                r = 2 * pair + head
                probs = jnp.exp(nt(keys, qm) - lse_ref[0, r : r + 1, at])
                dprobs = nt(values, dm)
                delta = jnp.sum(probs * dprobs, axis=0, keepdims=True)
                ds = (probs * (dprobs - delta)).astype(bf16)
                low = 128 * pair + 64 * head
                tops.append(nn(kt[low : low + 64, :], ds))
                dv_acc[...] = dv_acc[...] + nn(probs.astype(bf16), dm)
                dk_acc[...] = dk_acc[...] + nn(ds, qm)
            dq[at, lanes] = (jnp.concatenate(tops, axis=0).T * 0.125).astype(bf16)
            return 0

        lax.fori_loop(0, blocks, step, 0)
        dk[:, lanes] = dk_acc[...].astype(bf16)
        dv[:, lanes] = dv_acc[...].astype(bf16)

    bias_ref[0, 0:1, :] = jnp.sum(dq[...].astype(f32), axis=0, keepdims=True)
    bias_ref[0, 1:2, :] = jnp.sum(dv[...].astype(f32), axis=0, keepdims=True)

    def leave(b, _):
        at = block_of(b, block)
        term = nt(dq[at, :], wqkv[plane, 0]) + nt(dk[at, :], wqkv[plane, 1]) + nt(dv[at, :], wqkv[plane, 2])

        @pl.when(plane == 0)
        def _():
            acc[at, :] = term

        @pl.when(plane == 1)
        def _():
            acc[at, :] = acc[at, :] + term

        return 0

    lax.fori_loop(0, blocks, leave, 0)

    outs = ((back_own, 0), (back_send, 1))

    @pl.when(plane == 1)
    def _():
        for ref, i in outs:
            pltpu.make_async_copy(acc.at[pl.ds(i * half, half)], ref, o_sem.at[i]).start()

    def weigh(b, _):
        at = block_of(b, block)
        xb = xt[at, :]
        for part, ref in enumerate((dq, dk, dv)):
            wg[plane, part, at, :] = nn(xb, ref[...]).astype(bf16)
        return 0

    lax.fori_loop(0, xt.shape[0] // block, weigh, 0)
    awg[plane] = nn(attt[...], gs[...]).astype(bf16)

    def sends(p):
        result = []
        for step_, ref in enumerate(grads[p]):
            depth = ref.shape[1]
            at = block_of(shard_for(z, step_, count), depth)
            result.append(pltpu.make_async_copy(wg.at[p, :, at, :], ref.at[pl.ds(0, 3)], g_sem.at[p, step_, 0]))
            result.append(pltpu.make_async_copy(awg.at[p, :, at], ref.at[3], g_sem.at[p, step_, 1]))
        return result

    for p in range(2):

        @pl.when(plane == p)
        def _():
            for copy in sends(p):
                copy.start()

    @pl.when(plane == 1)
    def _():
        for ref, i in outs:
            pltpu.make_async_copy(acc.at[pl.ds(i * half, half)], ref, o_sem.at[i]).wait()
        for p in range(2):
            for copy in sends(p):
                copy.wait()


def attn_backward(g_own, g_oth, x_own, x_oth, nat, a_oth, q, k, v, attended, log_norm):
    count = len(nat)
    half, width = x_own.shape
    rows = 2 * half
    wide = nat[0].shape[2]
    bf16, f32 = jnp.bfloat16, jnp.float32
    by_plane = lambda *shape: pl.BlockSpec((1,) + shape, lambda p: (p,) + (0,) * len(shape))
    shape = lambda s, d: jax.ShapeDtypeStruct(s, d)
    flops = 2 * rows * width * wide * 2 * 8 + 8 * 5 * rows * rows * 64 * 2
    block = min(256, half)
    results = pl.pallas_call(
        functools.partial(attn_backward_kernel, count, block),
        grid=(2,),
        in_specs=[ANYWHERE] * (5 + count) + [by_plane(rows, wide)] * 4 + [by_plane(4, rows)],
        out_specs=[ANYWHERE] * (2 + 2 * count) + [by_plane(2, wide)],
        out_shape=[shape((half, width), f32)] * 2
        + [shape(nat[0].shape, bf16)] * (2 * count)
        + [shape((2, 2, wide), f32)],
        scratch_shapes=[
            pltpu.VMEM((rows, width), bf16),
            pltpu.VMEM((rows, width), bf16),
            pltpu.VMEM((width, rows), bf16),
            pltpu.VMEM((wide, rows), bf16),
            pltpu.VMEM((2, 3, width, wide), bf16),
            pltpu.VMEM((2, wide, width), bf16),
            pltpu.VMEM((rows, wide), bf16),
            pltpu.VMEM((rows, wide), bf16),
            pltpu.VMEM((rows, wide), bf16),
            pltpu.VMEM((rows, wide), bf16),
            pltpu.VMEM((wide, rows), bf16),
            pltpu.VMEM((rows, 128), f32),
            pltpu.VMEM((rows, 128), f32),
            pltpu.VMEM((rows, width), f32),
            pltpu.VMEM((2, 3, width, wide), bf16),
            pltpu.VMEM((2, wide, width), bf16),
            pltpu.SemaphoreType.DMA((2, count, 2)),
            pltpu.SemaphoreType.DMA((2, 2)),
            pltpu.SemaphoreType.DMA((2,)),
            pltpu.SemaphoreType.DMA((2, count, 2)),
        ],
        compiler_params=pltpu.CompilerParams(dimension_semantics=("arbitrary",), vmem_limit_bytes=VMEM_BYTES),
        cost_estimate=pl.CostEstimate(flops=flops, bytes_accessed=24 << 20, transcendentals=8 * rows * rows),
        name="attn_backward",
    )(g_own, g_oth, x_own, x_oth, *nat, a_oth, q, k, v, attended, log_norm)
    back_own, back_send = results[:2]
    bias = jnp.transpose(results[-1], (1, 0, 2)).reshape(2, -1)
    return back_own, back_send, results[2 : 2 + count], results[2 + count : 2 + 2 * count], bias


GELU_A = math.sqrt(2.0 / math.pi)
GELU_B = 0.044715


def mlp_copies(plane, ups, downs, upw, downw, sems):
    count = len(ups)
    z = lax.axis_index("fsdp")
    result = []
    for step in range(count):
        at = block_of(shard_of(z, step, count), ups[step].shape[0])
        result.append(pltpu.make_async_copy(ups[step], upw.at[plane, at, :], sems.at[plane, step, 0]))
        result.append(pltpu.make_async_copy(downs[step], downw.at[plane, :, at], sems.at[plane, step, 1]))
    return result


def mlp_kernel(count, block, tile, *refs):
    m_own, m_oth, g_own, g_oth = refs[:4]
    refs = refs[4:]
    z = lax.axis_index("fsdp")
    ups, downs = [
        [[own] + [full.at[0, shard_of(z, step, count)] for step in range(1, count)]]
        + [[full.at[1, shard_of(z, step, count)] for step in range(count)]]
        for own, full in (refs[:2], refs[2:4])
    ]
    bias_ref = refs[4]
    refs = refs[5:]
    out_own, out_send, back_own, back_send = refs[:4]
    refs = refs[4:]
    up_out, down_out = (refs[:count], refs[count : 2 * count]), (refs[2 * count : 3 * count], refs[3 * count : 4 * count])
    bgrad_ref = refs[4 * count]
    (ms, mt, gs, upw, downw, out_acc, back_acc, ugs, actt, upg, downg, w_sem, x_sem, o_sem, g_sem) = refs[4 * count + 1 :]
    plane, part = pl.program_id(0), pl.program_id(1)
    parts = pl.num_programs(1)
    rows, width = ms.shape
    half = rows // 2
    f32, bf16 = jnp.float32, jnp.bfloat16
    first = (plane == 0) & (part == 0)
    final = (plane == 1) & (part == parts - 1)

    @pl.when(first)
    def _():
        inputs = row_copies((m_own, m_oth), ms, x_sem.at[0]) + row_copies((g_own, g_oth), gs, x_sem.at[1])
        for copy in inputs:
            copy.start()
        for p in range(2):
            for copy in mlp_copies(p, ups[p], downs[p], upw, downw, w_sem):
                copy.start()
        for copy in inputs:
            copy.wait()

        def flip(b, _):
            at = block_of(b, block)
            mt[:, at] = ms[at, :].T
            return 0

        lax.fori_loop(0, rows // block, flip, 0)

    for p in range(2):

        @pl.when((plane == p) & (part == 0))
        def _():
            for copy in mlp_copies(p, ups[p], downs[p], upw, downw, w_sem):
                copy.wait()

    hidden = block_of(part, tile)

    def work(b, total):
        at = block_of(b, block)
        pre = nn(ms[at, :], upw[plane, :, hidden]) + bias_ref[...]
        dact = nt(gs[at, :], downw[plane, hidden, :])
        square = pre * pre
        inner = jnp.tanh(GELU_A * (pre + GELU_B * (square * pre)))
        half_plus = 0.5 + 0.5 * inner
        act = (pre * half_plus).astype(bf16)
        slope = half_plus + (0.5 * GELU_A) * pre * (1.0 - inner * inner) * (1.0 + (3.0 * GELU_B) * square)
        ug = (dact * slope).astype(bf16)
        out_term = nn(act, downw[plane, hidden, :])
        back_term = nt(ug, upw[plane, :, hidden])

        @pl.when(first)
        def _():
            out_acc[at, :] = out_term
            back_acc[at, :] = back_term

        @pl.when(jnp.logical_not(first))
        def _():
            out_acc[at, :] = out_acc[at, :] + out_term
            back_acc[at, :] = back_acc[at, :] + back_term

        ugs[at, :] = ug
        actt[:, at] = act.T
        return total + jnp.sum(ug.astype(f32), axis=0, keepdims=True)

    bgrad_ref[...] = lax.fori_loop(0, rows // block, work, jnp.zeros((1, tile), f32))

    ends = ((out_acc, 0, out_own), (out_acc, 1, out_send), (back_acc, 0, back_own), (back_acc, 1, back_send))

    def results():
        return [
            pltpu.make_async_copy(a.at[pl.ds(i * half, half)], ref, o_sem.at[j]) for j, (a, i, ref) in enumerate(ends)
        ]

    @pl.when(final)
    def _():
        for copy in results():
            copy.start()

    def weigh_up(b, _):
        at = block_of(b, block)
        upg[plane, at, hidden] = nn(mt[at, :], ugs[...]).astype(bf16)
        return 0

    lax.fori_loop(0, width // block, weigh_up, 0)

    def weigh_down(b, _):
        at = block_of(b, block)
        to = pl.ds(pl.multiple_of(part * tile + b * block, block), block)
        downg[plane, to, :] = nn(actt[at, :], gs[...]).astype(bf16)
        return 0

    lax.fori_loop(0, tile // block, weigh_down, 0)

    def sends(p):
        result = []
        for step in range(count):
            at = block_of(shard_for(z, step, count), up_out[p][step].shape[0])
            result.append(pltpu.make_async_copy(upg.at[p, at, :], up_out[p][step], g_sem.at[p, step, 0]))
            result.append(pltpu.make_async_copy(downg.at[p, :, at], down_out[p][step], g_sem.at[p, step, 1]))
        return result

    for p in range(2):

        @pl.when((plane == p) & (part == parts - 1))
        def _():
            for copy in sends(p):
                copy.start()

    @pl.when(final)
    def _():
        for copy in results():
            copy.wait()
        for p in range(2):
            for copy in sends(p):
                copy.wait()


def mlp(m_own, m_oth, g_own, g_oth, up_half, up_full, down_half, down_full, bias):
    count = up_full.shape[1]
    half, width = m_own.shape
    rows = 2 * half
    wide = up_half.shape[1]
    tile = min(512, wide)
    parts = wide // tile
    block = min(256, half)
    bf16, f32 = jnp.bfloat16, jnp.float32
    shape = lambda s, d: jax.ShapeDtypeStruct(s, d)
    hidden_spec = pl.BlockSpec((None, None, 1, tile), lambda p, h: (p, h, 0, 0))
    results = pl.pallas_call(
        functools.partial(mlp_kernel, count, block, tile),
        grid=(2, parts),
        in_specs=[ANYWHERE] * 8 + [hidden_spec],
        out_specs=[ANYWHERE] * (4 + 4 * count) + [hidden_spec],
        out_shape=[shape((half, width), f32)] * 4
        + [shape(up_half.shape, bf16)] * (2 * count)
        + [shape(down_half.shape, bf16)] * (2 * count)
        + [shape((2, parts, 1, tile), f32)],
        scratch_shapes=[
            pltpu.VMEM((rows, width), bf16),
            pltpu.VMEM((width, rows), bf16),
            pltpu.VMEM((rows, width), bf16),
            pltpu.VMEM((2, width, wide), bf16),
            pltpu.VMEM((2, wide, width), bf16),
            pltpu.VMEM((rows, width), f32),
            pltpu.VMEM((rows, width), f32),
            pltpu.VMEM((rows, tile), bf16),
            pltpu.VMEM((tile, rows), bf16),
            pltpu.VMEM((2, width, wide), bf16),
            pltpu.VMEM((2, wide, width), bf16),
            pltpu.SemaphoreType.DMA((2, count, 2)),
            pltpu.SemaphoreType.DMA((2, 2)),
            pltpu.SemaphoreType.DMA((4,)),
            pltpu.SemaphoreType.DMA((2, count, 2)),
        ],
        compiler_params=pltpu.CompilerParams(
            dimension_semantics=("arbitrary", "arbitrary"), vmem_limit_bytes=VMEM_BYTES
        ),
        cost_estimate=pl.CostEstimate(
            flops=6 * 2 * rows * width * 2 * wide, bytes_accessed=40 << 20, transcendentals=rows * 2 * wide
        ),
        name="mlp",
    )(m_own, m_oth, g_own, g_oth, up_half, up_full, down_half, down_full, bias.reshape(2, parts, 1, tile))
    grads = results[4:-1]
    return (*results[:4], *[grads[i * count : (i + 1) * count] for i in range(4)], results[-1].reshape(-1))


def reduce_pieces(nat, oth):
    f32 = jnp.float32
    got = [to_y(piece) for piece in oth]
    summed = [(a.astype(f32) + b.astype(f32)) for a, b in zip(nat, got)]
    total = summed[0]
    for step in range(1, len(summed)):
        total = total + to_z(summed[step].astype(jnp.bfloat16), step).astype(f32)
    low = total.astype(jnp.bfloat16)
    return low.astype(f32) + to_x(low).astype(f32)


def hyper_sum(value):
    value = value + to_core(value)
    value = value + to_x(value)
    value = value + to_y(value)
    count = lax.axis_size("fsdp")
    reach = 1
    while reach < count:
        value = value + lax.ppermute(value, "fsdp", [(src, src ^ reach) for src in range(count)])
        reach *= 2
    return value


def fast_body(
    tokens, condition, mod_weight, mod_bias, qkv_weight, qv_bias, attn_weight, attn_bias,
    up_weight, up_bias, down_weight, down_bias, cotangent,
):
    f32, bf16 = jnp.float32, jnp.bfloat16
    latents, tok_count, width = tokens.shape
    count = lax.axis_size("fsdp")
    z, y = lax.axis_index("fsdp"), lax.axis_index("tp")
    place = lax.axis_index("ctx")
    x, core = place // 2, place % 2
    mine, theirs = 2 * x + y, 2 * (1 - x) + y

    small_parts = (condition, qv_bias, attn_bias, up_bias, down_bias)
    small = jnp.concatenate([a.reshape(-1) for a in small_parts])
    small_all = z_order(gather_z(small), z)
    cond_size = condition.size
    cond_all = small_all[:, :cond_size].reshape(count * latents, width)
    bias_all = small_all[:, cond_size:]
    bias_oth = to_y(bias_all)
    marks = [qv_bias.size, qv_bias.size + attn_bias.size, qv_bias.size + attn_bias.size + up_bias.size]

    def qv_plane(b):
        rows = jnp.transpose(b[:, : marks[0]].reshape((count,) + qv_bias.shape), (1, 2, 0, 3)).reshape(2, -1)
        return lax.dynamic_slice_in_dim(rows, core * (rows.shape[1] // 2), rows.shape[1] // 2, 1)

    def up_plane(b):
        rows = jnp.transpose(b[:, marks[1] : marks[2]].reshape((count,) + up_bias.shape), (1, 0, 2)).reshape(-1)
        return lax.dynamic_slice_in_dim(rows, core * (rows.shape[0] // 2), rows.shape[0] // 2, 0)

    qv = jnp.concatenate([qv_plane(bias_all), qv_plane(bias_oth)], axis=1).astype(f32)
    hidden_bias = jnp.concatenate([up_plane(bias_all), up_plane(bias_oth)]).astype(f32)
    attn_bias_full = bias_all[:, marks[0] : marks[1]].reshape(-1).astype(f32)
    down_bias_full = bias_all[:, marks[2] :].reshape(-1).astype(f32)

    act_all = jax.nn.silu(cond_all.astype(f32)).astype(bf16)
    mod_piece = flat_dot(act_all, mod_weight) + mod_bias.astype(f32)
    mod_pair = jnp.stack([mod_piece, to_y(mod_piece)], axis=1)
    mod_pair = jnp.where(y == 0, mod_pair, mod_pair[:, ::-1])
    rows_for = lambda step: lax.dynamic_slice_in_dim(mod_pair, ((z + step) % count) * latents, latents, 0)
    mod_rel = [pick(rows_for(0), mine)] + [pick(to_z(rows_for(step), step), mine) for step in range(1, count)]
    modulation = z_order(mod_rel, z).reshape(6, width)
    shift_attn, scale_attn, gate_attn, shift_mlp, scale_mlp, gate_mlp = [modulation[r] for r in range(6)]

    def enter(source):
        return jnp.concatenate([pick(source, mine), to_x(pick(source, theirs))])

    tok = enter(tokens).astype(f32)
    cot = enter(cotangent).astype(f32)

    half_of = lambda a, axis: lax.dynamic_slice_in_dim(a, core * (a.shape[axis] // 2), a.shape[axis] // 2, axis)
    own_a = jnp.concatenate([half_of(qkv_weight, 2), half_of(attn_weight, 0)[None]])
    a_nat = gather_z(own_a)
    up_half, down_half = half_of(up_weight, 1), half_of(down_weight, 0)

    norm_a, inv_a = normalize(tok)
    x_own = (norm_a * (1.0 + scale_attn) + shift_attn).astype(bf16)
    x_oth = to_core(x_own)
    q, k, v, attended, log_norm, ao_own, ao_send, a_oth, up_full, down_full = attn_forward(
        x_own, x_oth, a_nat, up_half, down_half, qv[0], qv[1]
    )
    attn_out = ao_own + to_core(ao_send).astype(f32) + attn_bias_full
    middle = tok + gate_attn * attn_out
    norm_m, inv_m = normalize(middle)
    m_own = (norm_m * (1.0 + scale_mlp) + shift_mlp).astype(bf16)
    m_oth = to_core(m_own)
    g_own = (cot * gate_mlp).astype(bf16)
    g_oth = to_core(g_own)
    (
        mo_own, mo_send, mig_own, mig_send, upg_nat, upg_oth, downg_nat, downg_oth, up_bpart,
    ) = mlp(m_own, m_oth, g_own, g_oth, up_half, up_full, down_half, down_full, hidden_bias)
    up_total = reduce_pieces(upg_nat, upg_oth)
    down_total = reduce_pieces(downg_nat, downg_oth)
    mlp_out = mo_own + to_core(mo_send).astype(f32) + down_bias_full
    out_rows = (middle + gate_mlp * mlp_out).astype(bf16)
    gate_mlp_grad = jnp.sum(cot * mlp_out, axis=0)
    down_bpart = jnp.sum(g_own.astype(f32), axis=0)
    mig = mig_own + to_core(mig_send).astype(f32)
    middle_grad = cot + normalize_back(mig, norm_m, inv_m, scale_mlp)
    shift_mlp_grad = jnp.sum(mig, axis=0)
    scale_mlp_grad = jnp.sum(mig * norm_m, axis=0)
    gate_attn_grad = jnp.sum(middle_grad * attn_out, axis=0)
    ag_own = (middle_grad * gate_attn).astype(bf16)
    attn_bpart = jnp.sum(ag_own.astype(f32), axis=0)
    ag_oth = to_core(ag_own)
    aig_own, aig_send, ag_nat, ag_othp, qv_bpart = attn_backward(
        ag_own, ag_oth, x_own, x_oth, a_nat, a_oth, q, k, v, attended, log_norm
    )
    a_half = reduce_pieces(ag_nat, ag_othp)
    aig = aig_own + to_core(aig_send).astype(f32)
    tok_grad = middle_grad + normalize_back(aig, norm_a, inv_a, scale_attn)
    shift_attn_grad = jnp.sum(aig, axis=0)
    scale_attn_grad = jnp.sum(aig * norm_a, axis=0)

    def leave(rows):
        own, other = rows[:tok_count], to_x(rows[tok_count:])
        own_y, other_y = to_y(own), to_y(other)
        result = jnp.zeros((latents, tok_count, width), rows.dtype)
        for value, where_x, where_y in ((own, x, y), (other, 1 - x, y), (own_y, x, 1 - y), (other_y, 1 - x, 1 - y)):
            result = lax.dynamic_update_slice(result, value[None], (2 * where_x + where_y, 0, 0))
        return result

    layer_out = leave(out_rows)
    tokens_grad = leave(tok_grad.astype(bf16)).astype(f32)

    mod_own = jnp.stack(
        [shift_attn_grad, scale_attn_grad, gate_attn_grad, shift_mlp_grad, scale_mlp_grad, gate_mlp_grad]
    ).reshape(-1)
    mod_own = (mod_own + to_core(mod_own)).astype(bf16)
    by_x = jnp.stack([mod_own, to_x(mod_own)])
    by_x = jnp.where(x == 0, by_x, by_x[::-1])
    by_y = jnp.stack([by_x, to_y(by_x)], axis=1)
    by_y = jnp.where(y == 0, by_y, by_y[:, ::-1]).reshape(latents, -1)
    mod_grad_all = z_order(gather_z(by_y), z).reshape(count * latents, -1)
    piece = z * 2 + y
    piece_width = mod_weight.shape[1]
    mod_grad_piece = lax.dynamic_slice_in_dim(mod_grad_all, piece * piece_width, piece_width, 1)
    mod_wgrad = dot_tn(act_all, mod_grad_piece)
    mod_bgrad = jnp.sum(mod_grad_piece.astype(f32), axis=0)
    act_part = dot_nt(mod_grad_piece, mod_weight)
    part_for = lambda step: lax.dynamic_slice_in_dim(act_part, ((z + step) % count) * latents, latents, 0)
    act_z = part_for(0)
    for step in range(1, count):
        act_z = act_z + to_z(part_for(step), step)
    own_rows = latents // 2
    act_grad = lax.dynamic_slice_in_dim(act_z, y * own_rows, own_rows, 0) + to_y(
        lax.dynamic_slice_in_dim(act_z, (1 - y) * own_rows, own_rows, 0)
    )
    cond_rows = lax.dynamic_slice_in_dim(cond_all, piece * own_rows, own_rows, 0).astype(f32)
    condition_grad = jax.vjp(jax.nn.silu, cond_rows)[1](act_grad)[0]

    def spread(part, full):
        quarter = part.shape[-1] // 2
        zero = jnp.zeros(part.shape[:-1] + (full,), f32)
        plane = full // 2
        at = [0] * (part.ndim - 1)
        zero = lax.dynamic_update_slice(zero, part[..., :quarter], (*at, y * plane + core * quarter))
        return lax.dynamic_update_slice(zero, part[..., quarter:], (*at, (1 - y) * plane + core * quarter))

    qv_spread = spread(qv_bpart, width)
    up_spread = spread(up_bpart, up_bpart.shape[0] * 2)
    packed = hyper_sum(jnp.concatenate([qv_spread.reshape(-1), up_spread, attn_bpart, down_bpart]))
    qv_sum = packed[: 2 * width].reshape(2, width // 128, 128)
    up_sum = packed[2 * width : 2 * width + up_spread.shape[0]].reshape(-1, 128)
    rest = packed[2 * width + up_spread.shape[0] :].reshape(2, width)
    lanes = 128 // count
    qv_bgrad = lax.dynamic_slice(qv_sum, (0, y * qv_bias.shape[1], z * lanes), qv_bias.shape)
    up_bgrad = lax.dynamic_slice(up_sum, (y * up_bias.shape[0], z * lanes), up_bias.shape)
    attn_bgrad = lax.dynamic_slice_in_dim(rest[0], z * (width // count), width // count, 0)
    down_bgrad = lax.dynamic_slice_in_dim(rest[1], z * (width // count), width // count, 0)

    def both(part, axis):
        other = to_core(part)
        first = jnp.where(core == 0, part, other)
        second = jnp.where(core == 0, other, part)
        return jnp.concatenate([first, second], axis=axis)

    qkv_wgrad = both(a_half[:3], 2)
    attn_wgrad = both(a_half[3], 0)
    up_wgrad = both(up_total, 1)
    down_wgrad = both(down_total, 0)
    return (
        layer_out, tokens_grad, condition_grad, mod_wgrad, mod_bgrad, qkv_wgrad, qv_bgrad,
        attn_wgrad, attn_bgrad, up_wgrad, up_bgrad, down_wgrad, down_bgrad,
    )


def solution(mesh):
    placed = (
        P("fsdp", "ctx", None),
        P("fsdp", None),
        P(None, ("fsdp", "tp")),
        P(("fsdp", "tp")),
        P(None, "fsdp", "tp"),
        P(None, "tp", "fsdp"),
        P("tp", "fsdp"),
        P("fsdp"),
        P("fsdp", "tp"),
        P("tp", "fsdp"),
        P("tp", "fsdp"),
        P("fsdp"),
        P("fsdp", "ctx", None),
    )
    shape = dict(mesh.shape)
    chip_per_latent = shape["ctx"] == 4 and shape["tp"] == 2 and shape["fsdp"] == 4
    return jax.shard_map(
        fast_body if chip_per_latent else body,
        mesh=mesh,
        in_specs=placed,
        out_specs=(
            P("fsdp", "ctx", None),
            P("fsdp", "ctx", None),
            P(("fsdp", "tp"), None),
            P(None, ("fsdp", "tp")),
            P(("fsdp", "tp")),
            P(None, "fsdp", "tp"),
            P(None, "tp", "fsdp"),
            P("tp", "fsdp"),
            P("fsdp"),
            P("fsdp", "tp"),
            P("tp", "fsdp"),
            P("tp", "fsdp"),
            P("fsdp"),
        ),
        check_vma=False,
    )
```

```python
import functools
import math

import jax
import jax.numpy as jnp
from jax import lax
from jax.experimental import pallas as pl
from jax.experimental.pallas import tpu as pltpu
from jax.sharding import PartitionSpec as P


def modulate(tok_rows, shift_row, scale_row):
    centre = tok_rows - jnp.mean(tok_rows, axis=-1, keepdims=True)
    spread = jnp.mean(centre * centre, axis=-1, keepdims=True)
    normed = centre * lax.rsqrt(spread + 1e-06)
    return normed * (1.0 + scale_row[:, None, :]) + shift_row[:, None, :]


def gelu_tanh(pre_act):
    return jax.nn.gelu(pre_act, approximate=True)


def flat_dot(left, right):
    return jnp.dot(left, right, preferred_element_type=jnp.float32)


def head_slice(source, latent, head_pair):
    row_count = source.shape[1]
    picked = lax.dynamic_slice(source, (latent, 0, head_pair * 128), (1, row_count, 128))
    return picked[0].reshape(row_count, 2, 64)


def tokens_major(stacked, latents, head_pairs):
    row_count = stacked.shape[-2]
    grouped = stacked.reshape(latents, head_pairs, row_count, 128)
    return jnp.transpose(grouped, (0, 2, 1, 3)).reshape(latents, row_count, head_pairs * 128)


def attend(queries, keys_all, values_all, head_pairs):

    def attend_per_block(block_index):
        latent = block_index // head_pairs
        head_pair = block_index % head_pairs
        query_h = head_slice(queries, latent, head_pair)
        key_h = head_slice(keys_all, latent, head_pair)
        value_h = head_slice(values_all, latent, head_pair)
        scores = (
            jnp.einsum("qhd,khd->hqk", query_h, key_h, preferred_element_type=jnp.float32) * 0.125
        )
        row_max = jnp.max(scores, axis=-1, keepdims=True)
        weights = jnp.exp(scores - row_max)
        row_total = jnp.sum(weights, axis=-1, keepdims=True)
        probs_low = (weights / row_total).astype(jnp.bfloat16)
        attended = jnp.einsum(
            "hqk,khd->qhd", probs_low, value_h, preferred_element_type=jnp.float32
        )
        return (attended.reshape(query_h.shape[0], 128), (row_max + jnp.log(row_total))[..., 0])

    return lax.map(attend_per_block, jnp.arange(queries.shape[0] * head_pairs))


def query_side(queries, keys_all, values_all, grad_rows, log_norm, head_pairs):

    def query_per_block(packed):
        block_index, norm_block = packed
        latent = block_index // head_pairs
        head_pair = block_index % head_pairs
        query_h = head_slice(queries, latent, head_pair)
        key_h = head_slice(keys_all, latent, head_pair)
        value_h = head_slice(values_all, latent, head_pair)
        grad_h = head_slice(grad_rows, latent, head_pair)
        scores = (
            jnp.einsum("qhd,khd->hqk", query_h, key_h, preferred_element_type=jnp.float32) * 0.125
        )
        probs = jnp.exp(scores - norm_block[..., None])
        dprobs = jnp.einsum("qhd,khd->hqk", grad_h, value_h, preferred_element_type=jnp.float32)
        row_delta = jnp.sum(probs * dprobs, axis=-1, keepdims=True)
        score_grad = (probs * (dprobs - row_delta)).astype(jnp.bfloat16)
        query_grad = (
            jnp.einsum("hqk,khd->qhd", score_grad, key_h, preferred_element_type=jnp.float32)
            * 0.125
        )
        query_count = query_h.shape[0]
        key_grad = (
            jnp.einsum("hqk,qhd->khd", score_grad, query_h, preferred_element_type=jnp.float32)
            * 0.125
        )
        value_grad = jnp.einsum(
            "hqk,qhd->khd", probs.astype(jnp.bfloat16), grad_h, preferred_element_type=jnp.float32
        )
        return (
            query_grad.reshape(query_count, 128),
            key_grad.reshape(-1, 128),
            value_grad.reshape(-1, 128),
        )

    return lax.map(query_per_block, (jnp.arange(queries.shape[0] * head_pairs), log_norm))


def body(
    tokens,
    condition,
    mod_weight,
    mod_bias,
    qkv_weight,
    qv_bias,
    attn_weight,
    attn_bias,
    up_weight,
    up_bias,
    down_weight,
    down_bias,
    cotangent,
):
    latents, tok_count, width = tokens.shape
    gathered = (
        lax.all_gather(condition, "fsdp", axis=0, tiled=True),
        lax.all_gather(qkv_weight, "fsdp", axis=1, tiled=True),
        lax.all_gather(qv_bias, "fsdp", axis=2, tiled=True),
        lax.all_gather(attn_weight, "fsdp", axis=1, tiled=True),
        lax.all_gather(attn_bias, "fsdp", axis=0, tiled=True),
        lax.all_gather(up_weight, "fsdp", axis=0, tiled=True),
        lax.all_gather(up_bias, "fsdp", axis=1, tiled=True),
        lax.all_gather(down_weight, "fsdp", axis=1, tiled=True),
        lax.all_gather(down_bias, "fsdp", axis=0, tiled=True),
    )
    (
        cond_all,
        qkv_full,
        qv_full,
        attn_full,
        attn_bias_full,
        up_full,
        up_bias_full,
        down_full,
        down_bias_full,
    ) = gathered
    q_bias = qv_full[0].reshape(-1).astype(jnp.float32)
    v_bias = qv_full[1].reshape(-1).astype(jnp.float32)
    hidden_bias = up_bias_full.reshape(-1).astype(jnp.float32)
    act_all = jax.nn.silu(cond_all.astype(jnp.float32)).astype(jnp.bfloat16)
    mod_piece = flat_dot(act_all, mod_weight) + mod_bias.astype(jnp.float32)
    mod_full = lax.all_gather(mod_piece, ("fsdp", "tp"), axis=1, tiled=True)
    first_latent = lax.axis_index("fsdp") * latents
    modulation = lax.dynamic_slice_in_dim(mod_full, first_latent, latents, 0).reshape(
        latents, 6, width
    )
    shift_attn, scale_attn, gate_attn = (modulation[:, 0], modulation[:, 1], modulation[:, 2])
    shift_mlp, scale_mlp, gate_mlp = (modulation[:, 3], modulation[:, 4], modulation[:, 5])
    tok_float = tokens.astype(jnp.float32)
    attn_input_f, norm_pull_attn = jax.vjp(modulate, tok_float, shift_attn, scale_attn)
    attn_input = attn_input_f.astype(jnp.bfloat16).reshape(-1, width)
    queries = (
        (flat_dot(attn_input, qkv_full[0]) + q_bias)
        .astype(jnp.bfloat16)
        .reshape(latents, tok_count, -1)
    )
    keys_own = (
        flat_dot(attn_input, qkv_full[1]).astype(jnp.bfloat16).reshape(latents, tok_count, -1)
    )
    values_own = (
        (flat_dot(attn_input, qkv_full[2]) + v_bias)
        .astype(jnp.bfloat16)
        .reshape(latents, tok_count, -1)
    )
    keys_all, values_all = (
        lax.all_gather(keys_own, "ctx", axis=1, tiled=True),
        lax.all_gather(values_own, "ctx", axis=1, tiled=True),
    )
    head_width = queries.shape[-1]
    head_pairs = head_width // 128
    attended_st, log_norm = attend(queries, keys_all, values_all, head_pairs)
    attended = (
        tokens_major(attended_st, latents, head_pairs).astype(jnp.bfloat16).reshape(-1, head_width)
    )
    attn_out = lax.psum(flat_dot(attended, attn_full), "tp") + attn_bias_full.astype(jnp.float32)
    attn_out = attn_out.reshape(latents, tok_count, width)
    middle = tok_float + gate_attn[:, None, :] * attn_out
    mlp_input_f, norm_pull_mlp = jax.vjp(modulate, middle, shift_mlp, scale_mlp)
    mlp_input = mlp_input_f.astype(jnp.bfloat16).reshape(-1, width)
    up_pre = flat_dot(mlp_input, up_full) + hidden_bias
    up_act_f, gelu_pull = jax.vjp(gelu_tanh, up_pre)
    up_act = up_act_f.astype(jnp.bfloat16)
    mlp_out = lax.psum(flat_dot(up_act, down_full), "tp") + down_bias_full.astype(jnp.float32)
    mlp_out = mlp_out.reshape(latents, tok_count, width)
    layer_out = (middle + gate_mlp[:, None, :] * mlp_out).astype(jnp.bfloat16)
    out_grad = cotangent.astype(jnp.float32)
    gate_mlp_grad = jnp.sum(out_grad * mlp_out, axis=1)
    mlp_grad = (out_grad * gate_mlp[:, None, :]).astype(jnp.bfloat16).reshape(-1, width)
    down_bgrad_part = jnp.sum(mlp_grad.astype(jnp.float32), axis=0)
    down_wgrad_part = flat_dot(up_act.T, mlp_grad)
    up_grad = gelu_pull(flat_dot(mlp_grad, down_full.T))[0].astype(jnp.bfloat16)
    up_bgrad_part = jnp.sum(up_grad.astype(jnp.float32), axis=0)
    up_wgrad_part = flat_dot(mlp_input.T, up_grad)
    mlp_input_grad = lax.psum(flat_dot(up_grad, up_full.T), "tp").reshape(latents, tok_count, width)
    middle_part, shift_mlp_grad, scale_mlp_grad = norm_pull_mlp(mlp_input_grad)
    middle_grad = out_grad + middle_part
    gate_attn_grad = jnp.sum(middle_grad * attn_out, axis=1)
    attn_grad = (middle_grad * gate_attn[:, None, :]).astype(jnp.bfloat16).reshape(-1, width)
    attn_bgrad_part = jnp.sum(attn_grad.astype(jnp.float32), axis=0)
    attn_wgrad_part = flat_dot(attended.T, attn_grad)
    attended_grad = (
        flat_dot(attn_grad, attn_full.T)
        .astype(jnp.bfloat16)
        .reshape(latents, tok_count, head_width)
    )
    query_st, key_st, value_st = query_side(
        queries, keys_all, values_all, attended_grad, log_norm, head_pairs
    )
    key_parts = key_st.reshape(latents, head_pairs, -1, 128)
    value_parts = value_st.reshape(latents, head_pairs, -1, 128)
    key_sum, value_sum = (
        lax.psum_scatter(key_parts, "ctx", scatter_dimension=2, tiled=True),
        lax.psum_scatter(value_parts, "ctx", scatter_dimension=2, tiled=True),
    )
    key_grad = tokens_major(
        key_sum.reshape(latents * head_pairs, tok_count, 128), latents, head_pairs
    )
    value_grad = tokens_major(
        value_sum.reshape(latents * head_pairs, tok_count, 128), latents, head_pairs
    )
    query_flat = (
        tokens_major(query_st, latents, head_pairs).astype(jnp.bfloat16).reshape(-1, head_width)
    )
    key_flat = key_grad.astype(jnp.bfloat16).reshape(-1, head_width)
    value_flat = value_grad.astype(jnp.bfloat16).reshape(-1, head_width)
    input_terms = (
        flat_dot(query_flat, qkv_full[0].T)
        + flat_dot(key_flat, qkv_full[1].T)
        + flat_dot(value_flat, qkv_full[2].T)
    )
    attn_input_grad = lax.psum(input_terms, "tp").reshape(latents, tok_count, width)
    qkv_wgrad_part = jnp.stack(
        [
            flat_dot(attn_input.T, query_flat),
            flat_dot(attn_input.T, key_flat),
            flat_dot(attn_input.T, value_flat),
        ]
    )
    qv_bgrad_part = jnp.stack(
        [
            jnp.sum(query_flat.astype(jnp.float32), axis=0),
            jnp.sum(value_flat.astype(jnp.float32), axis=0),
        ]
    ).reshape(2, -1, 128)
    token_part, shift_attn_grad, scale_attn_grad = norm_pull_attn(attn_input_grad)
    tokens_grad = middle_grad + token_part
    mod_grad_own = jnp.stack(
        [
            shift_attn_grad,
            scale_attn_grad,
            gate_attn_grad,
            shift_mlp_grad,
            scale_mlp_grad,
            gate_mlp_grad,
        ],
        axis=1,
    ).reshape(latents, -1)
    mod_grad_slab = lax.dynamic_update_slice_in_dim(
        jnp.zeros(mod_full.shape, jnp.float32), mod_grad_own, first_latent, 0
    )
    mod_grad_all = lax.psum(mod_grad_slab, ("fsdp", "ctx")).astype(jnp.bfloat16)
    piece = lax.axis_index("fsdp") * lax.axis_size("tp") + lax.axis_index("tp")
    piece_width = mod_weight.shape[1]
    mod_grad_piece = lax.dynamic_slice_in_dim(mod_grad_all, piece * piece_width, piece_width, 1)
    mod_wgrad = flat_dot(act_all.T, mod_grad_piece)
    mod_bgrad = jnp.sum(mod_grad_piece.astype(jnp.float32), axis=0)
    own_rows = mod_full.shape[0] // (lax.axis_size("fsdp") * lax.axis_size("tp"))
    act_grad = lax.psum_scatter(
        flat_dot(mod_grad_piece, mod_weight.T), ("fsdp", "tp"), scatter_dimension=0, tiled=True
    )
    cond_rows = lax.dynamic_slice_in_dim(cond_all, piece * own_rows, own_rows, 0).astype(
        jnp.float32
    )
    condition_grad = jax.vjp(jax.nn.silu, cond_rows)[1](act_grad)[0]
    partials = (
        qkv_wgrad_part,
        qv_bgrad_part,
        attn_wgrad_part,
        attn_bgrad_part,
        up_wgrad_part,
        up_bgrad_part.reshape(-1, 128),
        down_wgrad_part,
        down_bgrad_part,
    )
    shards = (
        lax.psum_scatter(partials[0], "fsdp", scatter_dimension=1, tiled=True),
        lax.psum_scatter(partials[1], "fsdp", scatter_dimension=2, tiled=True),
        lax.psum_scatter(partials[2], "fsdp", scatter_dimension=1, tiled=True),
        lax.psum_scatter(partials[3], "fsdp", scatter_dimension=0, tiled=True),
        lax.psum_scatter(partials[4], "fsdp", scatter_dimension=0, tiled=True),
        lax.psum_scatter(partials[5], "fsdp", scatter_dimension=1, tiled=True),
        lax.psum_scatter(partials[6], "fsdp", scatter_dimension=1, tiled=True),
        lax.psum_scatter(partials[7], "fsdp", scatter_dimension=0, tiled=True),
    )
    reduced = lax.psum(
        (shards[0], shards[1], shards[2], shards[3], shards[4], shards[5], shards[6], shards[7]),
        "ctx",
    )
    qkv_wgrad, qv_bgrad, attn_wgrad, attn_bgrad, up_wgrad, up_bgrad, down_wgrad, down_bgrad = (
        reduced
    )
    return (
        layer_out,
        tokens_grad,
        condition_grad,
        mod_wgrad,
        mod_bgrad,
        qkv_wgrad,
        qv_bgrad,
        attn_wgrad,
        attn_bgrad,
        up_wgrad,
        up_bgrad,
        down_wgrad,
        down_bgrad,
    )


X_SWAP = [(0, 2), (2, 0), (1, 3), (3, 1)]
CORE_SWAP = [(0, 1), (1, 0), (2, 3), (3, 2)]
Y_SWAP = [(0, 1), (1, 0)]


def to_x(value):
    return lax.ppermute(value, "ctx", X_SWAP)


def to_core(value):
    return lax.ppermute(value, "ctx", CORE_SWAP)


def to_y(value):
    return lax.ppermute(value, "tp", Y_SWAP)


def to_z(value, step):
    count = lax.axis_size("fsdp")
    return lax.ppermute(value, "fsdp", [(src, (src + step) % count) for src in range(count)])


def z_order(relative, z):
    count = len(relative)
    back = list(relative[::-1])
    doubled = jnp.stack(back + back[:-1])
    return lax.dynamic_slice_in_dim(doubled, count - 1 - z, count, 0)


def pick(stacked, index):
    return lax.dynamic_index_in_dim(stacked, index, 0, keepdims=False)


def gather_z(value):
    count = lax.axis_size("fsdp")
    return [value] + [to_z(value, step) for step in range(1, count)]


def normalize(rows):
    centre = rows - jnp.mean(rows, axis=-1, keepdims=True)
    spread = jnp.mean(centre * centre, axis=-1, keepdims=True)
    inverse = lax.rsqrt(spread + 1e-06)
    return centre * inverse, inverse


def normalize_back(grad, normed, inverse, scale):
    e = grad * (1.0 + scale)
    mean_e = jnp.mean(e, axis=-1, keepdims=True)
    mean_en = jnp.mean(e * normed, axis=-1, keepdims=True)
    return (e - mean_e - normed * mean_en) * inverse


def dot_nt(left, right):
    return lax.dot_general(left, right, (((1,), (1,)), ((), ())), preferred_element_type=jnp.float32)


def dot_tn(left, right):
    return lax.dot_general(left, right, (((0,), (0,)), ((), ())), preferred_element_type=jnp.float32)


MESH = pl.DeviceIdType.MESH
ANYWHERE = pl.BlockSpec(memory_space=pl.ANY)
VMEM_BYTES = 64 * 1024 * 1024 - 4 * 65536


def nt(left, right):
    return lax.dot_general(left, right, (((1,), (1,)), ((), ())), preferred_element_type=jnp.float32)


def nn(left, right):
    return lax.dot_general(left, right, (((1,), (0,)), ((), ())), preferred_element_type=jnp.float32)


def block_of(index, size):
    return pl.ds(pl.multiple_of(index * size, size), size)


def shard_of(z, step, count):
    return lax.rem(z - step + count, count)


def shard_for(z, step, count):
    return lax.rem(z + step, count)


def attn_copies(plane, pieces, wqkv, wout, sems):
    count = len(pieces)
    z = lax.axis_index("fsdp")
    result = []
    for step, piece in enumerate(pieces):
        rows = piece.shape[1]
        at = block_of(shard_of(z, step, count), rows)
        result.append(pltpu.make_async_copy(piece.at[pl.ds(0, 3)], wqkv.at[plane, :, at, :], sems.at[plane, step, 0]))
        result.append(pltpu.make_async_copy(piece.at[3], wout.at[plane, :, at], sems.at[plane, step, 1]))
    return result


def row_copies(refs, target, sems):
    half = refs[0].shape[0]
    return [
        pltpu.make_async_copy(ref, target.at[pl.ds(i * half, half)], sems.at[i]) for i, ref in enumerate(refs)
    ]


def head_mask(rows, head):
    lane = lax.broadcasted_iota(jnp.int32, (rows, 128), 1)
    return (lane >= 64 * head) & (lane < 64 * head + 64)


class Gather:
    def __init__(self, own, full, z_send, z_recv, y_send, y_recv, x_send, x_recv):
        self.own, self.full = own, full
        self.sems = (z_send, z_recv, y_send, y_recv, x_send, x_recv)
        self.count = full.shape[1]
        self.z = lax.axis_index("fsdp")
        self.x = lax.axis_index("ctx") // 2

    def shard(self, index):
        if index == 0:
            return self.z
        if index < self.count:
            return self.z - index
        return self.z + index - self.count + 1

    def present(self, index):
        at = self.shard(index)
        return (at >= 0) & (at < self.count)

    def safe(self, index):
        return lax.rem(self.shard(index) + self.count, self.count)

    def source(self, index):
        return self.own if index == 0 else self.full.at[0, self.safe(index)]

    def half(self, ref):
        rows = ref.shape[0] // 2
        return ref.at[block_of(self.x, rows)]

    def along_z(self, index, side):
        slot = index if side == 0 or index == 0 else index - self.count + 1
        target = self.z + 1 if side == 0 else self.z - 1
        return pltpu.make_async_remote_copy(
            src_ref=self.source(index),
            dst_ref=self.full.at[0, self.safe(index)],
            send_sem=self.sems[0].at[side, slot],
            recv_sem=self.sems[1].at[side, slot],
            device_id={"fsdp": target},
            device_id_type=MESH,
        )

    def can_go(self, index, side):
        ok = self.z < self.count - 1 if side == 0 else self.z > 0
        return ok & self.present(index)

    def came_z(self, index):
        side = 0 if index < self.count else 1
        slot = index - 1 if side == 0 else index - self.count
        into = self.full.at[0, self.safe(index)]
        return pltpu.make_async_remote_copy(
            src_ref=into,
            dst_ref=into,
            send_sem=self.sems[0].at[side, slot],
            recv_sem=self.sems[1].at[side, slot],
            device_id={"fsdp": self.z},
            device_id_type=MESH,
        )

    def along_y(self, index):
        return pltpu.make_async_remote_copy(
            src_ref=self.half(self.source(index)),
            dst_ref=self.half(self.full.at[1, self.safe(index)]),
            send_sem=self.sems[2].at[index],
            recv_sem=self.sems[3].at[index],
            device_id={"tp": 1 - lax.axis_index("tp")},
            device_id_type=MESH,
        )

    def along_x(self, index):
        part = self.half(self.full.at[1, self.safe(index)])
        return pltpu.make_async_remote_copy(
            src_ref=part,
            dst_ref=part,
            send_sem=self.sems[4].at[index],
            recv_sem=self.sems[5].at[index],
            device_id={"ctx": lax.rem(lax.axis_index("ctx") + 2, 4)},
            device_id_type=MESH,
        )

    def came_x(self, index):
        rows = self.full.shape[2] // 2
        part = self.full.at[1, self.safe(index), block_of(1 - self.x, rows)]
        return pltpu.make_async_remote_copy(
            src_ref=part,
            dst_ref=part,
            send_sem=self.sems[4].at[index],
            recv_sem=self.sems[5].at[index],
            device_id={"ctx": lax.rem(lax.axis_index("ctx") + 2, 4)},
            device_id_type=MESH,
        )

    def indices(self):
        order = [0]
        for away in range(1, self.count):
            order += [away, self.count + away - 1]
        return order

    def begin(self):
        for side in range(2):

            @pl.when(self.can_go(0, side))
            def _():
                self.along_z(0, side).start()

        self.along_y(0).start()

    def relay_z(self, away):
        for side, index in ((0, away), (1, self.count + away - 1)):

            @pl.when(self.present(index))
            def _():
                self.came_z(index).wait_recv()

                if away < self.count - 1:

                    @pl.when(self.can_go(index, side))
                    def _():
                        self.along_z(index, side).start()

                self.along_y(index).start()

    def relay_x(self, away):
        for index in [0] if away == 0 else [away, self.count + away - 1]:

            @pl.when(self.present(index))
            def _():
                self.along_y(index).wait_recv()
                self.along_x(index).start()

    def end(self):
        for index in self.indices():

            @pl.when(self.present(index))
            def _():
                self.came_x(index).wait_recv()
                self.along_y(index).wait_send()
                self.along_x(index).wait_send()

            for side in range(2):
                if index == 0 or ((index < self.count) == (side == 0) and index not in (self.count - 1, 2 * self.count - 2)):

                    @pl.when(self.can_go(index, side))
                    def _():
                        self.along_z(index, side).wait_send()


def greet(z_all):
    barrier = pltpu.get_barrier_semaphore()
    z, count = lax.axis_index("fsdp"), lax.axis_size("fsdp")
    pl.semaphore_signal(barrier, inc=1, device_id={"tp": 1 - lax.axis_index("tp")}, device_id_type=MESH)
    pl.semaphore_signal(barrier, inc=1, device_id={"ctx": lax.rem(lax.axis_index("ctx") + 2, 4)}, device_id_type=MESH)
    for step in range(1, count):
        pl.semaphore_signal(barrier, inc=1, device_id={"fsdp": lax.rem(z + step, count)}, device_id_type=MESH)
    pl.semaphore_wait(barrier, count + 1)


def attn_forward_kernel(count, block, *refs):
    x_own, x_oth = refs[:2]
    pieces = refs[2 : 2 + count]
    up_half, down_half, qb, vb = refs[2 + count : 6 + count]
    q_ref, k_ref, v_ref, att_ref, lse_ref, out_own, out_send, a_oth, up_full, down_full = refs[6 + count : 16 + count]
    xs, wqkv, wout, vt, acc, w_sem, x_sem, o_sem, a_sem, g_z, g_y = refs[16 + count :]
    plane = pl.program_id(0)
    rows = xs.shape[0]
    half = rows // 2
    f32, bf16 = jnp.float32, jnp.bfloat16
    z = lax.axis_index("fsdp")
    xpos = lax.axis_index("ctx") // 2
    depth = pieces[0].shape[1] // 2
    gathers = [
        Gather(own, full, *[g_z.at[i, j] for j in range(2)], *[g_y.at[i, j] for j in range(4)])
        for i, (own, full) in enumerate(((up_half, up_full), (down_half, down_full)))
    ]
    x_peer = lax.rem(lax.axis_index("ctx") + 2, 4)

    def a_by_y(step):
        at = shard_of(z, step, count)
        return pltpu.make_async_remote_copy(
            src_ref=pieces[step].at[:, block_of(xpos, depth)],
            dst_ref=a_oth.at[at, :, block_of(xpos, depth)],
            send_sem=a_sem.at[0, step],
            recv_sem=a_sem.at[1, step],
            device_id={"tp": 1 - lax.axis_index("tp")},
            device_id_type=MESH,
        )

    def a_by_x(step, side):
        part = a_oth.at[shard_of(z, step, count), :, block_of(side, depth)]
        return pltpu.make_async_remote_copy(
            src_ref=part,
            dst_ref=part,
            send_sem=a_sem.at[2, step],
            recv_sem=a_sem.at[3, step],
            device_id={"ctx": x_peer},
            device_id_type=MESH,
        )

    def native_copies():
        return attn_copies(0, pieces, wqkv, wout, w_sem)

    def other_copies():
        return attn_copies(1, [a_oth.at[shard_of(z, step, count)] for step in range(count)], wqkv, wout, w_sem)

    @pl.when(plane == 0)
    def _():
        inputs = row_copies((x_own, x_oth), xs, x_sem)
        for copy in inputs + native_copies():
            copy.start()
        greet(True)
        for step in range(count):
            a_by_y(step).start()
        for gather in gathers:
            gather.begin()
        for copy in inputs + native_copies():
            copy.wait()

    @pl.when(plane == 1)
    def _():
        for step in range(count):
            a_by_x(step, 1 - xpos).wait_recv()
        for copy in other_copies():
            copy.start()
        for copy in other_copies():
            copy.wait()

    def slot(first, second):
        for p, actions in enumerate((first, second)):
            if actions:

                @pl.when(plane == p)
                def _():
                    for action in actions:
                        action()

    def pass_a(step):
        def act():
            a_by_y(step).wait_recv()
            a_by_x(step, xpos).start()

        return act

    def project(b, _):
        at = block_of(b, block)
        xb = xs[at, :]
        q_ref[0, at, :] = (nn(xb, wqkv[plane, 0]) + qb[...]).astype(bf16)
        k_ref[0, at, :] = nn(xb, wqkv[plane, 1]).astype(bf16)
        value = (nn(xb, wqkv[plane, 2]) + vb[...]).astype(bf16)
        v_ref[0, at, :] = value
        vt[:, at] = value.T
        return 0

    lax.fori_loop(0, rows // block, project, 0)
    up, down = gathers
    relay_z = lambda gather, away: (lambda: gather.relay_z(away)) if away < count else (lambda: None)
    relay_x = lambda gather, away: (lambda: gather.relay_x(away)) if away < count else (lambda: None)
    slot([pass_a(0)], [relay_x(up, 0)])

    for pair in range(2):
        lanes = slice(128 * pair, 128 * pair + 128)

        def attend(b, _):
            at = block_of(b, block)
            qp = q_ref[0, at, lanes] * jnp.bfloat16(0.125)
            keys = k_ref[0, :, lanes]
            tops = []
            for head in range(2):
                scores = nt(keys, jnp.where(head_mask(block, head), qp, jnp.bfloat16(0)))
                top = jnp.max(scores, axis=0, keepdims=True)
                weights = jnp.exp(scores - top)
                total = jnp.sum(weights, axis=0, keepdims=True)
                probs = (weights * (1.0 / total)).astype(bf16)
                low = 128 * pair + 64 * head
                tops.append(nn(vt[low : low + 64, :], probs))
                lse_ref[0, 2 * pair + head : 2 * pair + head + 1, at] = top + jnp.log(total)
            att_ref[0, at, lanes] = jnp.concatenate(tops, axis=0).T.astype(bf16)
            return 0

        lax.fori_loop(0, rows // block, attend, 0)
        if pair == 0:
            slot([pass_a(step) for step in range(1, count - 1)], [relay_z(up, 2), relay_x(down, 0), relay_x(up, 1)])
        else:
            slot([relay_z(up, 1), pass_a(count - 1)], [relay_z(down, 2), relay_x(down, 1)])

    def finish(b, _):
        at = block_of(b, block)
        term = nn(att_ref[0, at, :], wout[plane])

        @pl.when(plane == 0)
        def _():
            acc[at, :] = term

        @pl.when(plane == 1)
        def _():
            acc[at, :] = acc[at, :] + term

        return 0

    lax.fori_loop(0, rows // block, finish, 0)
    slot([relay_z(down, 1)], [])

    @pl.when(plane == 1)
    def _():
        for i, ref in enumerate((out_own, out_send)):
            pltpu.make_async_copy(acc.at[pl.ds(i * half, half)], ref, o_sem.at[i]).start()
        for away in range(3, count):
            for gather in gathers:
                gather.relay_z(away)
        for away in range(2, count):
            for gather in gathers:
                gather.relay_x(away)
        for gather in gathers:
            gather.end()
        for step in range(count):
            a_by_y(step).wait_send()
            a_by_x(step, xpos).wait_send()
        for i, ref in enumerate((out_own, out_send)):
            pltpu.make_async_copy(acc.at[pl.ds(i * half, half)], ref, o_sem.at[i]).wait()


def attn_forward(x_own, x_oth, nat, up_half, down_half, q_bias, v_bias):
    count = len(nat)
    half, width = x_own.shape
    rows = 2 * half
    wide = nat[0].shape[2]
    bf16, f32 = jnp.bfloat16, jnp.float32
    by_plane = lambda *shape: pl.BlockSpec((1,) + shape, lambda p: (p,) + (0,) * len(shape))
    biases = [b.reshape(2, 1, wide) for b in (q_bias, v_bias)]
    squeezed = pl.BlockSpec((None, 1, wide), lambda p: (p, 0, 0))
    shape = lambda s, d: jax.ShapeDtypeStruct(s, d)
    flops = 2 * rows * width * wide * 2 * 4 + 8 * 2 * rows * rows * 64 * 2
    return pl.pallas_call(
        functools.partial(attn_forward_kernel, count, min(256, half)),
        grid=(2,),
        in_specs=[ANYWHERE] * (4 + count) + [squeezed] * 2,
        out_specs=[by_plane(rows, wide)] * 4 + [by_plane(4, rows)] + [ANYWHERE] * 5,
        out_shape=[shape((2, rows, wide), bf16)] * 4
        + [shape((2, 4, rows), f32)]
        + [shape((half, width), f32)] * 2
        + [shape((count,) + nat[0].shape, bf16)]
        + [shape((2, count) + w.shape, bf16) for w in (up_half, down_half)],
        scratch_shapes=[
            pltpu.VMEM((rows, width), bf16),
            pltpu.VMEM((2, 3, width, wide), bf16),
            pltpu.VMEM((2, wide, width), bf16),
            pltpu.VMEM((wide, rows), bf16),
            pltpu.VMEM((rows, width), f32),
            pltpu.SemaphoreType.DMA((2, count, 2)),
            pltpu.SemaphoreType.DMA((2,)),
            pltpu.SemaphoreType.DMA((2,)),
            pltpu.SemaphoreType.DMA((4, count)),
            pltpu.SemaphoreType.DMA((2, 2, 2, count)),
            pltpu.SemaphoreType.DMA((2, 4, 2 * count - 1)),
        ],
        compiler_params=pltpu.CompilerParams(
            dimension_semantics=("arbitrary",), vmem_limit_bytes=VMEM_BYTES, collective_id=0, has_side_effects=True
        ),
        cost_estimate=pl.CostEstimate(flops=flops, bytes_accessed=18 << 20, transcendentals=8 * rows * rows),
        name="attn_forward",
    )(x_own, x_oth, *nat, up_half, down_half, *biases)


class Reduce:
    def __init__(self, x_first, part, own, other, from_x, from_y, from_z, load, x_sem, y_sem, z_sem):
        self.x_first, self.part, self.own, self.other = x_first, part, own, other
        self.from_x, self.from_y, self.from_z = from_x, from_y, from_z
        self.load_sem, self.x_sem, self.y_sem, self.z_sem = load, x_sem, y_sem, z_sem
        self.count = part.shape[1]
        self.rows = part.shape[2] // 2
        self.z = lax.axis_index("fsdp")
        self.x = lax.axis_index("ctx") // 2

    def shard(self, step):
        return shard_for(self.z, step, self.count)

    def order(self):
        return list(range(1, self.count)) + [0]

    def loads(self):
        result = []
        for step in self.order():
            at = self.shard(step)
            mine = self.part.at[1, at, block_of(self.x, self.rows)]
            result.append(pltpu.make_async_copy(mine, self.other.at[at], self.load_sem.at[1, step]))
            mine = self.part.at[0, at, block_of(self.x, self.rows)] if self.x_first else self.part.at[0, at]
            result.append(pltpu.make_async_copy(mine, self.own.at[at], self.load_sem.at[0, step]))
        return result

    def to_x(self, plane, step):
        at = self.shard(step)
        return pltpu.make_async_remote_copy(
            src_ref=self.part.at[plane, at, block_of(1 - self.x, self.rows)],
            dst_ref=self.from_x.at[plane, at] if self.x_first else self.from_x.at[0, at],
            send_sem=self.x_sem.at[0, plane, step],
            recv_sem=self.x_sem.at[1, plane, step],
            device_id={"ctx": lax.rem(lax.axis_index("ctx") + 2, 4)},
            device_id_type=MESH,
        )

    def to_y(self, step):
        at = self.shard(step)
        return pltpu.make_async_remote_copy(
            src_ref=self.other.at[at],
            dst_ref=self.from_y.at[at],
            send_sem=self.y_sem.at[0, step],
            recv_sem=self.y_sem.at[1, step],
            device_id={"tp": 1 - lax.axis_index("tp")},
            device_id_type=MESH,
        )

    def to_z(self, step):
        return pltpu.make_async_remote_copy(
            src_ref=self.own.at[self.shard(step)],
            dst_ref=self.from_z.at[step - 1],
            send_sem=self.z_sem.at[0, step - 1],
            recv_sem=self.z_sem.at[1, step - 1],
            device_id={"fsdp": self.shard(step)},
            device_id_type=MESH,
        )

    def begin(self, plane):
        for step in self.order():
            self.to_x(plane, step).start()

    def begin_loads(self):
        for copy in self.loads():
            copy.start()

    def wait_loads(self):
        for copy in self.loads():
            copy.wait()

    def add_x(self, step):
        at = self.shard(step)
        self.to_x(1, step).wait_recv()
        came = self.from_x[1 if self.x_first else 0, at]
        self.other[at] = (self.other[at].astype(jnp.float32) + came.astype(jnp.float32)).astype(jnp.bfloat16)
        self.to_y(step).start()

    def add_y(self, step):
        f32 = jnp.float32
        at = self.shard(step)
        if self.x_first:
            self.to_x(0, step).wait_recv()
            self.to_y(step).wait_recv()
            total = self.own[at].astype(f32) + self.from_x[0, at].astype(f32) + self.from_y[at].astype(f32)
            self.own[at] = total.astype(jnp.bfloat16)
        else:
            self.to_y(step).wait_recv()
            rows = block_of(self.x, self.rows)
            self.own[at, rows] = (self.own[at, rows].astype(f32) + self.from_y[at].astype(f32)).astype(jnp.bfloat16)
        if step:
            self.to_z(step).start()

    def total(self):
        f32 = jnp.float32
        result = self.own[self.z].astype(f32)
        for step in range(1, self.count):
            self.to_z(step).wait_recv()
            result = result + self.from_z[step - 1].astype(f32)
        return result

    def end(self):
        for step in range(self.count):
            self.to_x(1, step).wait_send()
            if self.x_first:
                self.to_x(0, step).wait_send()
            self.to_y(step).wait_send()
            if step:
                self.to_z(step).wait_send()


def reduce_scratch(x_first, part_shape):
    count, (rows, lanes) = part_shape[1], part_shape[2:]
    bf16 = jnp.bfloat16
    own_rows = rows // 2 if x_first else rows
    planes = 2 if x_first else 1
    return [
        pltpu.VMEM((count, own_rows, lanes), bf16),
        pltpu.VMEM((count, rows // 2, lanes), bf16),
        pltpu.VMEM((planes, count, rows // 2, lanes), bf16),
        pltpu.VMEM((count, rows // 2, lanes), bf16),
        pltpu.VMEM((count - 1, own_rows, lanes), bf16),
        pltpu.SemaphoreType.DMA((2, count)),
        pltpu.SemaphoreType.DMA((2, 2, count)),
        pltpu.SemaphoreType.DMA((2, count)),
        pltpu.SemaphoreType.DMA((2, count - 1)),
    ]


def attn_backward_kernel(count, block, *refs):
    g_own, g_oth, x_own, x_oth = refs[:4]
    z = lax.axis_index("fsdp")
    a_oth = refs[4 + count]
    pieces = (refs[4 : 4 + count], [a_oth.at[shard_of(z, step, count)] for step in range(count)])
    up_part, down_part = refs[5 + count : 7 + count]
    refs = refs[7 + count :]
    q_ref, k_ref, v_ref, att_ref, lse_ref = refs[:5]
    back_own, back_send = refs[5:7]
    grads = (refs[7 : 7 + count], refs[7 + count : 7 + 2 * count])
    bias_ref, up_ref, down_ref = refs[7 + 2 * count : 10 + 2 * count]
    up = Reduce(False, up_part, *refs[-18:-9])
    down = Reduce(True, down_part, *refs[-9:])
    refs = refs[:-18]
    (gs, xs, xt, attt, wqkv, wout, d_att, dq, dk, dv, kt, dk_acc, dv_acc, acc, wg, awg, w_sem, x_sem, o_sem, g_sem) = refs[
        10 + 2 * count :
    ]
    plane = pl.program_id(0)
    rows = xs.shape[0]
    half = rows // 2
    f32, bf16 = jnp.float32, jnp.bfloat16
    blocks = rows // block

    @pl.when(plane == 0)
    def _():
        inputs = row_copies((g_own, g_oth), gs, x_sem.at[0]) + row_copies((x_own, x_oth), xs, x_sem.at[1])
        for copy in inputs:
            copy.start()
        for p in range(2):
            for copy in attn_copies(p, pieces[p], wqkv, wout, w_sem):
                copy.start()
        greet(True)
        up.begin(1)
        down.begin(1)
        down.begin(0)
        up.begin_loads()
        down.begin_loads()
        for copy in inputs:
            copy.wait()

        def flip(b, _):
            at = block_of(b, block)
            xt[:, at] = xs[at, :].T
            return 0

        lax.fori_loop(0, blocks, flip, 0)

    for p in range(2):

        @pl.when(plane == p)
        def _():
            for copy in attn_copies(p, pieces[p], wqkv, wout, w_sem):
                copy.wait()

    def slot(first, second):
        for p, actions in enumerate((first, second)):
            if actions:

                @pl.when(plane == p)
                def _():
                    for action, *given in actions:
                        action(*given)

    steps = up.order()

    def enter(b, _):
        at = block_of(b, block)
        d_att[at, :] = nt(gs[at, :], wout[plane]).astype(bf16)
        attt[:, at] = att_ref[0, at, :].T
        kt[:, at] = k_ref[0, at, :].T
        return 0

    lax.fori_loop(0, blocks, enter, 0)
    slot([(up.wait_loads,), (down.wait_loads,)], [(up.add_y, steps[3])])

    for pair in range(2):
        lanes = slice(128 * pair, 128 * pair + 128)
        dk_acc[...] = jnp.zeros_like(dk_acc)
        dv_acc[...] = jnp.zeros_like(dv_acc)

        def step(b, _):
            at = block_of(b, block)
            qp = q_ref[0, at, lanes] * jnp.bfloat16(0.125)
            dp = d_att[at, lanes]
            keys = k_ref[0, :, lanes]
            values = v_ref[0, :, lanes]
            tops, p_all, s_all, q_all, d_all = [], [], [], [], []
            for head in range(2):
                mask = head_mask(block, head)
                qm = jnp.where(mask, qp, jnp.bfloat16(0))
                dm = jnp.where(mask, dp, jnp.bfloat16(0))
                r = 2 * pair + head
                probs = jnp.exp(nt(keys, qm) - lse_ref[0, r : r + 1, at])
                dprobs = nt(values, dm)
                delta = jnp.sum(probs * dprobs, axis=0, keepdims=True)
                ds = (probs * (dprobs - delta)).astype(bf16)
                low = 128 * pair + 64 * head
                tops.append(nn(kt[low : low + 64, :], ds))
                dv_acc[...] = dv_acc[...] + nn(probs.astype(bf16), dm)
                dk_acc[...] = dk_acc[...] + nn(ds, qm)
            dq[at, lanes] = (jnp.concatenate(tops, axis=0).T * 0.125).astype(bf16)
            return 0

        lax.fori_loop(0, blocks, step, 0)
        dk[:, lanes] = dk_acc[...].astype(bf16)
        dv[:, lanes] = dv_acc[...].astype(bf16)
        if pair == 0:
            slot([(up.add_x, steps[0])], [(down.add_x, steps[1]), (down.add_x, steps[2])])
        else:
            slot([(up.add_x, steps[1]), (up.add_x, steps[2]), (up.add_y, steps[0])], [(down.add_x, steps[3])])

    bias_ref[0, 0:1, :] = jnp.sum(dq[...].astype(f32), axis=0, keepdims=True)
    bias_ref[0, 1:2, :] = jnp.sum(dv[...].astype(f32), axis=0, keepdims=True)

    def leave(b, _):
        at = block_of(b, block)
        term = nt(dq[at, :], wqkv[plane, 0]) + nt(dk[at, :], wqkv[plane, 1]) + nt(dv[at, :], wqkv[plane, 2])

        @pl.when(plane == 0)
        def _():
            acc[at, :] = term

        @pl.when(plane == 1)
        def _():
            acc[at, :] = acc[at, :] + term

        return 0

    lax.fori_loop(0, blocks, leave, 0)
    slot([(up.add_x, steps[3]), (up.add_y, steps[1])], [(down.add_y, steps[0])])

    outs = ((back_own, 0), (back_send, 1))

    @pl.when(plane == 1)
    def _():
        for ref, i in outs:
            pltpu.make_async_copy(acc.at[pl.ds(i * half, half)], ref, o_sem.at[i]).start()

    def weigh(b, _):
        at = block_of(b, block)
        xb = xt[at, :]
        for part, ref in enumerate((dq, dk, dv)):
            wg[plane, part, at, :] = nn(xb, ref[...]).astype(bf16)
        return 0

    lax.fori_loop(0, xt.shape[0] // block, weigh, 0)
    awg[plane] = nn(attt[...], gs[...]).astype(bf16)
    slot([(up.add_y, steps[2]), (down.add_x, steps[0])], [(down.add_y, steps[1])])

    def sends(p):
        result = []
        for step_, ref in enumerate(grads[p]):
            depth = ref.shape[1]
            at = block_of(shard_for(z, step_, count), depth)
            result.append(pltpu.make_async_copy(wg.at[p, :, at, :], ref.at[pl.ds(0, 3)], g_sem.at[p, step_, 0]))
            result.append(pltpu.make_async_copy(awg.at[p, :, at], ref.at[3], g_sem.at[p, step_, 1]))
        return result

    for p in range(2):

        @pl.when(plane == p)
        def _():
            for copy in sends(p):
                copy.start()

    @pl.when(plane == 1)
    def _():
        for ref, i in outs:
            pltpu.make_async_copy(acc.at[pl.ds(i * half, half)], ref, o_sem.at[i]).wait()
        for step_ in steps[2:]:
            down.add_y(step_)
        up_ref[...] = up.total().astype(bf16)
        down_ref[...] = down.total()
        up.end()
        down.end()
        for p in range(2):
            for copy in sends(p):
                copy.wait()


def attn_backward(g_own, g_oth, x_own, x_oth, nat, a_oth, up_part, down_part, q, k, v, attended, log_norm):
    count = len(nat)
    half, width = x_own.shape
    rows = 2 * half
    wide = nat[0].shape[2]
    bf16, f32 = jnp.bfloat16, jnp.float32
    by_plane = lambda *shape: pl.BlockSpec((1,) + shape, lambda p: (p,) + (0,) * len(shape))
    shape = lambda s, d: jax.ShapeDtypeStruct(s, d)
    flops = 2 * rows * width * wide * 2 * 8 + 8 * 5 * rows * rows * 64 * 2
    block = min(256, half)
    results = pl.pallas_call(
        functools.partial(attn_backward_kernel, count, block),
        grid=(2,),
        in_specs=[ANYWHERE] * (7 + count) + [by_plane(rows, wide)] * 4 + [by_plane(4, rows)],
        out_specs=[ANYWHERE] * (2 + 2 * count) + [by_plane(2, wide)] + [pl.BlockSpec(memory_space=pltpu.VMEM)] * 2,
        out_shape=[shape((half, width), f32)] * 2
        + [shape(nat[0].shape, bf16)] * (2 * count)
        + [shape((2, 2, wide), f32), shape(up_part.shape[2:], bf16), shape((down_part.shape[2] // 2, down_part.shape[3]), f32)],
        scratch_shapes=[
            pltpu.VMEM((rows, width), bf16),
            pltpu.VMEM((rows, width), bf16),
            pltpu.VMEM((width, rows), bf16),
            pltpu.VMEM((wide, rows), bf16),
            pltpu.VMEM((2, 3, width, wide), bf16),
            pltpu.VMEM((2, wide, width), bf16),
            pltpu.VMEM((rows, wide), bf16),
            pltpu.VMEM((rows, wide), bf16),
            pltpu.VMEM((rows, wide), bf16),
            pltpu.VMEM((rows, wide), bf16),
            pltpu.VMEM((wide, rows), bf16),
            pltpu.VMEM((rows, 128), f32),
            pltpu.VMEM((rows, 128), f32),
            pltpu.VMEM((rows, width), f32),
            pltpu.VMEM((2, 3, width, wide), bf16),
            pltpu.VMEM((2, wide, width), bf16),
            pltpu.SemaphoreType.DMA((2, count, 2)),
            pltpu.SemaphoreType.DMA((2, 2)),
            pltpu.SemaphoreType.DMA((2,)),
            pltpu.SemaphoreType.DMA((2, count, 2)),
        ]
        + reduce_scratch(False, up_part.shape)
        + reduce_scratch(True, down_part.shape),
        compiler_params=pltpu.CompilerParams(
            dimension_semantics=("arbitrary",), vmem_limit_bytes=VMEM_BYTES, collective_id=1, has_side_effects=True
        ),
        cost_estimate=pl.CostEstimate(flops=flops, bytes_accessed=24 << 20, transcendentals=8 * rows * rows),
        name="attn_backward",
    )(g_own, g_oth, x_own, x_oth, *nat, a_oth, up_part, down_part, q, k, v, attended, log_norm)
    back_own, back_send = results[:2]
    bias = jnp.transpose(results[-3], (1, 0, 2)).reshape(2, -1)
    return back_own, back_send, results[2 : 2 + count], results[2 + count : 2 + 2 * count], bias, *results[-2:]


GELU_A = math.sqrt(2.0 / math.pi)
GELU_B = 0.044715


def mlp_copies(plane, ups, downs, upw, downw, sems):
    count = len(ups)
    z = lax.axis_index("fsdp")
    result = []
    for step in range(count):
        at = block_of(shard_of(z, step, count), ups[step].shape[0])
        result.append(pltpu.make_async_copy(ups[step], upw.at[plane, at, :], sems.at[plane, step, 0]))
        result.append(pltpu.make_async_copy(downs[step], downw.at[plane, :, at], sems.at[plane, step, 1]))
    return result


def mlp_kernel(count, block, tile, *refs):
    m_own, m_oth, g_own, g_oth = refs[:4]
    refs = refs[4:]
    z = lax.axis_index("fsdp")
    ups, downs = [
        [[own] + [full.at[0, shard_of(z, step, count)] for step in range(1, count)]]
        + [[full.at[1, shard_of(z, step, count)] for step in range(count)]]
        for own, full in (refs[:2], refs[2:4])
    ]
    bias_ref = refs[4]
    refs = refs[5:]
    out_own, out_send, back_own, back_send = refs[:4]
    refs = refs[4:]
    up_part, down_part, bgrad_ref = refs[:3]
    (ms, mt, gs, upw, downw, out_acc, back_acc, ugs, actt, upg, downg, w_sem, x_sem, o_sem, g_sem) = refs[3:]
    plane, part = pl.program_id(0), pl.program_id(1)
    parts = pl.num_programs(1)
    rows, width = ms.shape
    half = rows // 2
    f32, bf16 = jnp.float32, jnp.bfloat16
    first = (plane == 0) & (part == 0)
    final = (plane == 1) & (part == parts - 1)

    @pl.when(first)
    def _():
        inputs = row_copies((m_own, m_oth), ms, x_sem.at[0]) + row_copies((g_own, g_oth), gs, x_sem.at[1])
        for copy in inputs:
            copy.start()
        for p in range(2):
            for copy in mlp_copies(p, ups[p], downs[p], upw, downw, w_sem):
                copy.start()
        for copy in inputs:
            copy.wait()

        def flip(b, _):
            at = block_of(b, block)
            mt[:, at] = ms[at, :].T
            return 0

        lax.fori_loop(0, rows // block, flip, 0)

    for p in range(2):

        @pl.when((plane == p) & (part == 0))
        def _():
            for copy in mlp_copies(p, ups[p], downs[p], upw, downw, w_sem):
                copy.wait()

    hidden = block_of(part, tile)

    def work(b, total):
        at = block_of(b, block)
        pre = nn(ms[at, :], upw[plane, :, hidden]) + bias_ref[...]
        dact = nt(gs[at, :], downw[plane, hidden, :])
        square = pre * pre
        inner = jnp.tanh(GELU_A * (pre + GELU_B * (square * pre)))
        half_plus = 0.5 + 0.5 * inner
        act = (pre * half_plus).astype(bf16)
        slope = half_plus + (0.5 * GELU_A) * pre * (1.0 - inner * inner) * (1.0 + (3.0 * GELU_B) * square)
        ug = (dact * slope).astype(bf16)
        out_term = nn(act, downw[plane, hidden, :])
        back_term = nt(ug, upw[plane, :, hidden])

        @pl.when(first)
        def _():
            out_acc[at, :] = out_term
            back_acc[at, :] = back_term

        @pl.when(jnp.logical_not(first))
        def _():
            out_acc[at, :] = out_acc[at, :] + out_term
            back_acc[at, :] = back_acc[at, :] + back_term

        ugs[at, :] = ug
        actt[:, at] = act.T
        return total + jnp.sum(ug.astype(f32), axis=0, keepdims=True)

    bgrad_ref[...] = lax.fori_loop(0, rows // block, work, jnp.zeros((1, tile), f32))

    ends = ((out_acc, 0, out_own), (out_acc, 1, out_send), (back_acc, 0, back_own), (back_acc, 1, back_send))

    def results():
        return [
            pltpu.make_async_copy(a.at[pl.ds(i * half, half)], ref, o_sem.at[j]) for j, (a, i, ref) in enumerate(ends)
        ]

    @pl.when(final)
    def _():
        for copy in results():
            copy.start()

    def weigh_up(b, _):
        at = block_of(b, block)
        upg[plane, at, hidden] = nn(mt[at, :], ugs[...]).astype(bf16)
        return 0

    lax.fori_loop(0, width // block, weigh_up, 0)

    def weigh_down(b, _):
        at = block_of(b, block)
        to = pl.ds(pl.multiple_of(part * tile + b * block, block), block)
        downg[plane, to, :] = nn(actt[at, :], gs[...]).astype(bf16)
        return 0

    lax.fori_loop(0, tile // block, weigh_down, 0)

    def sends(p):
        result = []
        for shard in range(count):
            at = block_of(shard, up_part.shape[2])
            result.append(pltpu.make_async_copy(upg.at[p, at, :], up_part.at[p, shard], g_sem.at[p, shard, 0]))
            result.append(pltpu.make_async_copy(downg.at[p, :, at], down_part.at[p, shard], g_sem.at[p, shard, 1]))
        return result

    for p in range(2):

        @pl.when((plane == p) & (part == parts - 1))
        def _():
            for copy in sends(p):
                copy.start()

    @pl.when(final)
    def _():
        for copy in results():
            copy.wait()
        for p in range(2):
            for copy in sends(p):
                copy.wait()


def mlp(m_own, m_oth, g_own, g_oth, up_half, up_full, down_half, down_full, bias):
    count = up_full.shape[1]
    half, width = m_own.shape
    rows = 2 * half
    wide = up_half.shape[1]
    tile = min(512, wide)
    parts = wide // tile
    block = min(256, half)
    bf16, f32 = jnp.bfloat16, jnp.float32
    shape = lambda s, d: jax.ShapeDtypeStruct(s, d)
    hidden_spec = pl.BlockSpec((None, None, 1, tile), lambda p, h: (p, h, 0, 0))
    results = pl.pallas_call(
        functools.partial(mlp_kernel, count, block, tile),
        grid=(2, parts),
        in_specs=[ANYWHERE] * 8 + [hidden_spec],
        out_specs=[ANYWHERE] * 6 + [hidden_spec],
        out_shape=[shape((half, width), f32)] * 4
        + [shape((2, count) + w.shape, bf16) for w in (up_half, down_half)]
        + [shape((2, parts, 1, tile), f32)],
        scratch_shapes=[
            pltpu.VMEM((rows, width), bf16),
            pltpu.VMEM((width, rows), bf16),
            pltpu.VMEM((rows, width), bf16),
            pltpu.VMEM((2, width, wide), bf16),
            pltpu.VMEM((2, wide, width), bf16),
            pltpu.VMEM((rows, width), f32),
            pltpu.VMEM((rows, width), f32),
            pltpu.VMEM((rows, tile), bf16),
            pltpu.VMEM((tile, rows), bf16),
            pltpu.VMEM((2, width, wide), bf16),
            pltpu.VMEM((2, wide, width), bf16),
            pltpu.SemaphoreType.DMA((2, count, 2)),
            pltpu.SemaphoreType.DMA((2, 2)),
            pltpu.SemaphoreType.DMA((4,)),
            pltpu.SemaphoreType.DMA((2, count, 2)),
        ],
        compiler_params=pltpu.CompilerParams(
            dimension_semantics=("arbitrary", "arbitrary"), vmem_limit_bytes=VMEM_BYTES
        ),
        cost_estimate=pl.CostEstimate(
            flops=6 * 2 * rows * width * 2 * wide, bytes_accessed=40 << 20, transcendentals=rows * 2 * wide
        ),
        name="mlp",
    )(m_own, m_oth, g_own, g_oth, up_half, up_full, down_half, down_full, bias.reshape(2, parts, 1, tile))
    return (*results[:-1], results[-1].reshape(-1))


def reduce_pieces(nat, oth):
    f32 = jnp.float32
    got = [to_y(piece) for piece in oth]
    summed = [(a.astype(f32) + b.astype(f32)) for a, b in zip(nat, got)]
    total = summed[0]
    for step in range(1, len(summed)):
        total = total + to_z(summed[step].astype(jnp.bfloat16), step).astype(f32)
    low = total.astype(jnp.bfloat16)
    return low.astype(f32) + to_x(low).astype(f32)


def hyper_sum(value):
    value = value + to_core(value)
    value = value + to_x(value)
    value = value + to_y(value)
    count = lax.axis_size("fsdp")
    reach = 1
    while reach < count:
        value = value + lax.ppermute(value, "fsdp", [(src, src ^ reach) for src in range(count)])
        reach *= 2
    return value


def fast_body(
    tokens, condition, mod_weight, mod_bias, qkv_weight, qv_bias, attn_weight, attn_bias,
    up_weight, up_bias, down_weight, down_bias, cotangent,
):
    f32, bf16 = jnp.float32, jnp.bfloat16
    latents, tok_count, width = tokens.shape
    count = lax.axis_size("fsdp")
    z, y = lax.axis_index("fsdp"), lax.axis_index("tp")
    place = lax.axis_index("ctx")
    x, core = place // 2, place % 2
    mine, theirs = 2 * x + y, 2 * (1 - x) + y

    small_parts = (condition, qv_bias, attn_bias, up_bias, down_bias)
    small = jnp.concatenate([a.reshape(-1) for a in small_parts])
    small_all = z_order(gather_z(small), z)
    cond_size = condition.size
    cond_all = small_all[:, :cond_size].reshape(count * latents, width)
    bias_all = small_all[:, cond_size:]
    bias_oth = to_y(bias_all)
    marks = [qv_bias.size, qv_bias.size + attn_bias.size, qv_bias.size + attn_bias.size + up_bias.size]

    def qv_plane(b):
        rows = jnp.transpose(b[:, : marks[0]].reshape((count,) + qv_bias.shape), (1, 2, 0, 3)).reshape(2, -1)
        return lax.dynamic_slice_in_dim(rows, core * (rows.shape[1] // 2), rows.shape[1] // 2, 1)

    def up_plane(b):
        rows = jnp.transpose(b[:, marks[1] : marks[2]].reshape((count,) + up_bias.shape), (1, 0, 2)).reshape(-1)
        return lax.dynamic_slice_in_dim(rows, core * (rows.shape[0] // 2), rows.shape[0] // 2, 0)

    qv = jnp.concatenate([qv_plane(bias_all), qv_plane(bias_oth)], axis=1).astype(f32)
    hidden_bias = jnp.concatenate([up_plane(bias_all), up_plane(bias_oth)]).astype(f32)
    attn_bias_full = bias_all[:, marks[0] : marks[1]].reshape(-1).astype(f32)
    down_bias_full = bias_all[:, marks[2] :].reshape(-1).astype(f32)

    act_all = jax.nn.silu(cond_all.astype(f32)).astype(bf16)
    mod_piece = flat_dot(act_all, mod_weight) + mod_bias.astype(f32)
    mod_pair = jnp.stack([mod_piece, to_y(mod_piece)], axis=1)
    mod_pair = jnp.where(y == 0, mod_pair, mod_pair[:, ::-1])
    rows_for = lambda step: lax.dynamic_slice_in_dim(mod_pair, ((z + step) % count) * latents, latents, 0)
    mod_rel = [pick(rows_for(0), mine)] + [pick(to_z(rows_for(step), step), mine) for step in range(1, count)]
    modulation = z_order(mod_rel, z).reshape(6, width)
    shift_attn, scale_attn, gate_attn, shift_mlp, scale_mlp, gate_mlp = [modulation[r] for r in range(6)]

    def enter(source):
        return jnp.concatenate([pick(source, mine), to_x(pick(source, theirs))])

    tok = enter(tokens).astype(f32)
    cot = enter(cotangent).astype(f32)

    half_of = lambda a, axis: lax.dynamic_slice_in_dim(a, core * (a.shape[axis] // 2), a.shape[axis] // 2, axis)
    own_a = jnp.concatenate([half_of(qkv_weight, 2), half_of(attn_weight, 0)[None]])
    a_nat = gather_z(own_a)
    up_half, down_half = half_of(up_weight, 1), half_of(down_weight, 0)

    norm_a, inv_a = normalize(tok)
    x_own = (norm_a * (1.0 + scale_attn) + shift_attn).astype(bf16)
    x_oth = to_core(x_own)
    q, k, v, attended, log_norm, ao_own, ao_send, a_oth, up_full, down_full = attn_forward(
        x_own, x_oth, a_nat, up_half, down_half, qv[0], qv[1]
    )
    attn_out = ao_own + to_core(ao_send).astype(f32) + attn_bias_full
    middle = tok + gate_attn * attn_out
    norm_m, inv_m = normalize(middle)
    m_own = (norm_m * (1.0 + scale_mlp) + shift_mlp).astype(bf16)
    m_oth = to_core(m_own)
    g_own = (cot * gate_mlp).astype(bf16)
    g_oth = to_core(g_own)
    (
        mo_own, mo_send, mig_own, mig_send, up_part, down_part, up_bpart,
    ) = mlp(m_own, m_oth, g_own, g_oth, up_half, up_full, down_half, down_full, hidden_bias)
    mlp_out = mo_own + to_core(mo_send).astype(f32) + down_bias_full
    out_rows = (middle + gate_mlp * mlp_out).astype(bf16)
    gate_mlp_grad = jnp.sum(cot * mlp_out, axis=0)
    down_bpart = jnp.sum(g_own.astype(f32), axis=0)
    mig = mig_own + to_core(mig_send).astype(f32)
    middle_grad = cot + normalize_back(mig, norm_m, inv_m, scale_mlp)
    shift_mlp_grad = jnp.sum(mig, axis=0)
    scale_mlp_grad = jnp.sum(mig * norm_m, axis=0)
    gate_attn_grad = jnp.sum(middle_grad * attn_out, axis=0)
    ag_own = (middle_grad * gate_attn).astype(bf16)
    attn_bpart = jnp.sum(ag_own.astype(f32), axis=0)
    ag_oth = to_core(ag_own)
    aig_own, aig_send, ag_nat, ag_othp, qv_bpart, up_low, down_part_x = attn_backward(
        ag_own, ag_oth, x_own, x_oth, a_nat, a_oth, up_part, down_part, q, k, v, attended, log_norm
    )
    up_total = up_low.astype(f32) + to_x(up_low).astype(f32)
    down_oth_x = to_x(down_part_x)
    down_total = jnp.concatenate(
        [jnp.where(x == 0, down_part_x, down_oth_x), jnp.where(x == 0, down_oth_x, down_part_x)]
    )
    a_half = reduce_pieces(ag_nat, ag_othp)
    aig = aig_own + to_core(aig_send).astype(f32)
    tok_grad = middle_grad + normalize_back(aig, norm_a, inv_a, scale_attn)
    shift_attn_grad = jnp.sum(aig, axis=0)
    scale_attn_grad = jnp.sum(aig * norm_a, axis=0)

    def leave(rows):
        own, other = rows[:tok_count], to_x(rows[tok_count:])
        own_y, other_y = to_y(own), to_y(other)
        result = jnp.zeros((latents, tok_count, width), rows.dtype)
        for value, where_x, where_y in ((own, x, y), (other, 1 - x, y), (own_y, x, 1 - y), (other_y, 1 - x, 1 - y)):
            result = lax.dynamic_update_slice(result, value[None], (2 * where_x + where_y, 0, 0))
        return result

    layer_out = leave(out_rows)
    tokens_grad = leave(tok_grad.astype(bf16)).astype(f32)

    mod_own = jnp.stack(
        [shift_attn_grad, scale_attn_grad, gate_attn_grad, shift_mlp_grad, scale_mlp_grad, gate_mlp_grad]
    ).reshape(-1)
    mod_own = (mod_own + to_core(mod_own)).astype(bf16)
    by_x = jnp.stack([mod_own, to_x(mod_own)])
    by_x = jnp.where(x == 0, by_x, by_x[::-1])
    by_y = jnp.stack([by_x, to_y(by_x)], axis=1)
    by_y = jnp.where(y == 0, by_y, by_y[:, ::-1]).reshape(latents, -1)
    mod_grad_all = z_order(gather_z(by_y), z).reshape(count * latents, -1)
    piece = z * 2 + y
    piece_width = mod_weight.shape[1]
    mod_grad_piece = lax.dynamic_slice_in_dim(mod_grad_all, piece * piece_width, piece_width, 1)
    mod_wgrad = dot_tn(act_all, mod_grad_piece)
    mod_bgrad = jnp.sum(mod_grad_piece.astype(f32), axis=0)
    act_part = dot_nt(mod_grad_piece, mod_weight)
    part_for = lambda step: lax.dynamic_slice_in_dim(act_part, ((z + step) % count) * latents, latents, 0)
    act_z = part_for(0)
    for step in range(1, count):
        act_z = act_z + to_z(part_for(step), step)
    own_rows = latents // 2
    act_grad = lax.dynamic_slice_in_dim(act_z, y * own_rows, own_rows, 0) + to_y(
        lax.dynamic_slice_in_dim(act_z, (1 - y) * own_rows, own_rows, 0)
    )
    cond_rows = lax.dynamic_slice_in_dim(cond_all, piece * own_rows, own_rows, 0).astype(f32)
    condition_grad = jax.vjp(jax.nn.silu, cond_rows)[1](act_grad)[0]

    def spread(part, full):
        quarter = part.shape[-1] // 2
        zero = jnp.zeros(part.shape[:-1] + (full,), f32)
        plane = full // 2
        at = [0] * (part.ndim - 1)
        zero = lax.dynamic_update_slice(zero, part[..., :quarter], (*at, y * plane + core * quarter))
        return lax.dynamic_update_slice(zero, part[..., quarter:], (*at, (1 - y) * plane + core * quarter))

    qv_spread = spread(qv_bpart, width)
    up_spread = spread(up_bpart, up_bpart.shape[0] * 2)
    packed = hyper_sum(jnp.concatenate([qv_spread.reshape(-1), up_spread, attn_bpart, down_bpart]))
    qv_sum = packed[: 2 * width].reshape(2, width // 128, 128)
    up_sum = packed[2 * width : 2 * width + up_spread.shape[0]].reshape(-1, 128)
    rest = packed[2 * width + up_spread.shape[0] :].reshape(2, width)
    lanes = 128 // count
    qv_bgrad = lax.dynamic_slice(qv_sum, (0, y * qv_bias.shape[1], z * lanes), qv_bias.shape)
    up_bgrad = lax.dynamic_slice(up_sum, (y * up_bias.shape[0], z * lanes), up_bias.shape)
    attn_bgrad = lax.dynamic_slice_in_dim(rest[0], z * (width // count), width // count, 0)
    down_bgrad = lax.dynamic_slice_in_dim(rest[1], z * (width // count), width // count, 0)

    def both(part, axis):
        other = to_core(part)
        first = jnp.where(core == 0, part, other)
        second = jnp.where(core == 0, other, part)
        return jnp.concatenate([first, second], axis=axis)

    qkv_wgrad = both(a_half[:3], 2)
    attn_wgrad = both(a_half[3], 0)
    up_wgrad = both(up_total, 1)
    down_wgrad = both(down_total, 0)
    return (
        layer_out, tokens_grad, condition_grad, mod_wgrad, mod_bgrad, qkv_wgrad, qv_bgrad,
        attn_wgrad, attn_bgrad, up_wgrad, up_bgrad, down_wgrad, down_bgrad,
    )


def solution(mesh):
    placed = (
        P("fsdp", "ctx", None),
        P("fsdp", None),
        P(None, ("fsdp", "tp")),
        P(("fsdp", "tp")),
        P(None, "fsdp", "tp"),
        P(None, "tp", "fsdp"),
        P("tp", "fsdp"),
        P("fsdp"),
        P("fsdp", "tp"),
        P("tp", "fsdp"),
        P("tp", "fsdp"),
        P("fsdp"),
        P("fsdp", "ctx", None),
    )
    shape = dict(mesh.shape)
    chip_per_latent = shape["ctx"] == 4 and shape["tp"] == 2 and shape["fsdp"] == 4
    return jax.shard_map(
        fast_body if chip_per_latent else body,
        mesh=mesh,
        in_specs=placed,
        out_specs=(
            P("fsdp", "ctx", None),
            P("fsdp", "ctx", None),
            P(("fsdp", "tp"), None),
            P(None, ("fsdp", "tp")),
            P(("fsdp", "tp")),
            P(None, "fsdp", "tp"),
            P(None, "tp", "fsdp"),
            P("tp", "fsdp"),
            P("fsdp"),
            P("fsdp", "tp"),
            P("tp", "fsdp"),
            P("tp", "fsdp"),
            P("fsdp"),
        ),
        check_vma=False,
    )
```
